32 devices in a mesh: dp: 8 (over y, x, core), mp: 4 (over z).
Axes of the slice: x: 2, y: 2, z: 4, core: 2. Of those that a mesh axis runs over, the one named last changes fastest.
Arguments:
- layer_in: bfloat16 [16384, 768], P(('dp', 'mp')), may hold values from -6 to 6
- query_proj: bfloat16 [768, 768], P(None, 'mp'), may hold values from -0.21875 to 0.21875
- key_proj: bfloat16 [768, 768], P(None, 'mp'), may hold values from -0.21875 to 0.21875
- value_proj: bfloat16 [768, 768], P(None, 'mp'), may hold values from -0.21875 to 0.21875
- out_proj: bfloat16 [768, 768], P('mp'), may hold values from -1.75 to 1.75
- gate_proj: bfloat16 [768, 2048], P(None, 'mp'), may hold values from -0.21875 to 0.21875
- up_proj: bfloat16 [768, 2048], P(None, 'mp'), may hold values from -0.21875 to 0.21875
- down_proj: bfloat16 [2048, 768], P('mp'), may hold values from -0.125 to 0.125
- first_gain: float32 [768], replicated, may hold values from 0.1 to 1.9
- second_gain: float32 [768], replicated, may hold values from 0.1 to 1.9
- seq_lengths: int32 [16], P('dp'), may hold values from 64 to 1024, as said below
- cotangent: bfloat16 [16384, 768], P(('dp', 'mp')), may hold values from -6 to 6
Outputs:
- layer_out: bfloat16 [16384, 768], P(('dp', 'mp'))
- input_grad: bfloat16 [16384, 768], P(('dp', 'mp'))
- query_grad: float32 [768, 768], P(None, 'mp')
- key_grad: float32 [768, 768], P(None, 'mp')
- value_grad: float32 [768, 768], P(None, 'mp')
- output_grad: float32 [768, 768], P('mp')
- gate_grad: float32 [768, 2048], P(None, 'mp')
- up_grad: float32 [768, 2048], P(None, 'mp')
- down_grad: float32 [2048, 768], P('mp')
- first_grad: float32 [768], replicated
- second_grad: float32 [768], replicated
The draws below stay inside these ranges and needn't reach their ends.
Inputs may be any that keep to these rules, and one draw needn't show every extreme that they name: Slot i holds a sequence of seq_lengths[i] tokens at its start, the rest of its 1024 rows is padding. Some slot is full in every draw.
All inputs are finite; a program needn't handle non-finite values.
Results may differ from the reference program's by a relative error of at most 0.02.
Values may be sent and summed in bfloat16 or wider, within the bound.
A program may use at most 192 MiB of HBM per device.

```python
import math
import jax
import jax.numpy as jnp
from jax import lax

D = 768
HEADS = 12
HS = 64
FF = 2048
SLOT_LEN = 1024
MIN_LEN = 64
SLOTS = 16
TOKENS = 16384
N_MP = 4


def draw_seq_lengths(key, part):
    keys = jax.random.split(key, 5)
    spread = SLOT_LEN - MIN_LEN + 1
    first = jax.random.randint(keys[0], (SLOTS,), 0, spread)
    second = jax.random.randint(keys[1], (SLOTS,), 0, spread)
    shorter = MIN_LEN + jnp.minimum(first, second)
    whole = jax.random.randint(keys[2], (SLOTS,), 0, 8) < 3
    drawn = jnp.where(whole, SLOT_LEN, shorter)
    longest = jax.random.randint(keys[3], (), 0, SLOTS)
    offset = jax.random.randint(keys[4], (), 1, SLOTS)
    drawn = drawn.at[longest].set(SLOT_LEN)
    drawn = drawn.at[(longest + offset) % SLOTS].set(MIN_LEN)
    return drawn.astype(jnp.int32)


def steps_of(stream_key, extent, cuts, least, largest):
    def one(axis_at, blocks):
        steps = jax.random.uniform(jax.random.fold_in(jax.random.fold_in(stream_key, 6), axis_at), (blocks,), jnp.float32, least / len(cuts), largest / len(cuts))
        return jnp.repeat(jnp.exp(steps), extent[axis_at] // blocks).reshape((-1,) + (1,) * (len(extent) - axis_at - 1))

    factor_of = one(*cuts[0])
    for cut in cuts[1:]:
        factor_of = factor_of * one(*cut)
    return factor_of


def centred(stream_key, shape, width, most, shards=(), held_as=jnp.bfloat16):
    loudness = steps_of(stream_key, shape, shards, -0.22, 0.18) if shards else 1.0
    entries = jax.random.normal(stream_key, shape, jnp.float32) * width * loudness
    return jnp.minimum(jnp.maximum(entries, -most), most).astype(held_as)


def setup_inputs(seed: int = 0) -> dict:
    seeds = jax.random.split(jax.random.key(seed), 13)
    return {
        "layer_in": centred(seeds[0], (TOKENS, D), 1.0, 6.0, ((0, 32),)),
        "query_proj": centred(seeds[1], (D, HEADS * HS), D ** -0.5, 0.21875, ((1, 4),)),
        "key_proj": centred(seeds[2], (D, HEADS * HS), D ** -0.5, 0.21875, ((1, 4),)),
        "value_proj": centred(seeds[3], (D, HEADS * HS), D ** -0.5, 0.21875, ((1, 4),)),
        "out_proj": centred(seeds[4], (HEADS * HS, D), (HEADS * HS // 64) ** -0.5, 1.75, ((0, 4),)),
        "gate_proj": centred(seeds[5], (D, FF), D ** -0.5, 0.21875, ((1, 4),)),
        "up_proj": centred(seeds[6], (D, FF), D ** -0.5, 0.21875, ((1, 4),)),
        "down_proj": centred(seeds[7], (FF, D), FF ** -0.5, 0.125, ((0, 4),)),
        "first_gain": jnp.clip(1.0 + 0.18 * jax.random.normal(seeds[8], (D,), jnp.float32), 0.1, 1.9),
        "second_gain": jnp.clip(1.0 + 0.18 * jax.random.normal(seeds[9], (D,), jnp.float32), 0.1, 1.9),
        "seq_lengths": draw_seq_lengths(jax.random.fold_in(seeds[12], 71), 0),
        "cotangent": centred(seeds[11], (TOKENS, D), 1.0, 6.0, ((0, 32),)),
    }


@jax.custom_vjp
def low(v):
    return lax.optimization_barrier(v.astype(jnp.bfloat16)).astype(jnp.float32)

@jax.custom_vjp
def low_back(v):
    return v

def low_keep(v):
    return (low(v), None)

def low_pass(kept, grad):
    return (grad,)

def back_keep(v):
    return (v, None)

def back_low(kept, grad):
    return (low(grad),)
low.defvjp(low_keep, low_pass)
low_back.defvjp(back_keep, back_low)

def matmul(left, right):
    return jnp.dot(left, right, precision=lax.Precision.HIGHEST, preferred_element_type=jnp.float32)

def rms_norm(resid, gain):
    return resid * lax.rsqrt(lax.optimization_barrier(jnp.mean(resid * resid, axis=-1, keepdims=True)) + 1e-05) * gain

def rotary(field, positions):
    half = field.shape[-1] // 2
    freqs = 10000.0 ** (-jnp.arange(half, dtype=jnp.float32) * 2.0 / HS)
    angles = positions.astype(jnp.float32)[:, None] * freqs[None, :]
    cosines = jnp.cos(angles)[:, None, :]
    sines = jnp.sin(angles)[:, None, :]
    first = field[..., :half]
    second = field[..., half:]
    return jnp.concatenate([first * cosines - second * sines, second * cosines + first * sines], axis=-1)

def layer(rows_in, valid_len, weights):
    query_w, key_w, value_w, out_w, gate_w, up_w, down_w, gain_one, gain_two = weights
    group_slots = valid_len.shape[0]
    group_rows = rows_in.shape[0]
    row_ids = jnp.arange(group_rows, dtype=jnp.int32)
    positions = row_ids % SLOT_LEN
    row_len = jnp.repeat(valid_len, SLOT_LEN)
    present = (positions < row_len).astype(jnp.float32)
    key_pos = jnp.arange(SLOT_LEN, dtype=jnp.int32)
    allowed = (key_pos[None, None, :] <= key_pos[None, :, None]) & (key_pos[None, None, :] < valid_len[:, None, None])
    local_heads = HEADS // N_MP
    head_width = local_heads * HS
    attn_branch = jnp.zeros((group_rows, D), jnp.float32)
    for group in range(N_MP):
        cols = slice(group * head_width, (group + 1) * head_width)
        inputs = low_back(rows_in)
        query_raw = low_back(matmul(inputs, query_w[:, cols])).reshape(group_rows, local_heads, HS)
        key_raw = low_back(matmul(inputs, key_w[:, cols])).reshape(group_rows, local_heads, HS)
        value_low = low(low_back(matmul(inputs, value_w[:, cols]))).reshape(group_slots, SLOT_LEN, local_heads, HS)
        rot_query = low(rotary(query_raw, positions)).reshape(group_slots, SLOT_LEN, local_heads, HS)
        rot_key = low(rotary(key_raw, positions)).reshape(group_slots, SLOT_LEN, local_heads, HS)
        scores = jnp.einsum('gqhd,gkhd->ghqk', rot_query, rot_key, precision=lax.Precision.HIGHEST) * 0.125
        scores = low_back(scores)
        scores = jnp.where(allowed[:, None], scores, -1e+30)
        attn_probs = low(jax.nn.softmax(scores, axis=-1))
        mixed = jnp.einsum('ghqk,gkhd->gqhd', attn_probs, value_low, precision=lax.Precision.HIGHEST)
        mixed = mixed.reshape(group_rows, head_width) * present[:, None]
        mixed = low_back(low(mixed))
        attn_branch = attn_branch + low(matmul(mixed, out_w[cols, :]))
    attn_branch = low_back(attn_branch)
    normed = rms_norm(rows_in + attn_branch, gain_one)
    normed_low = low(normed)
    hidden_width = FF // N_MP
    ffn_branch = jnp.zeros((group_rows, D), jnp.float32)
    for group in range(N_MP):
        cols = slice(group * hidden_width, (group + 1) * hidden_width)
        inputs = low_back(normed_low)
        gate_pre = low_back(matmul(inputs, gate_w[:, cols]))
        up_pre = low_back(matmul(inputs, up_w[:, cols]))
        hidden = low(jax.nn.silu(gate_pre) * up_pre)
        ffn_branch = ffn_branch + low(matmul(hidden, down_w[cols, :]))
    ffn_branch = low_back(ffn_branch)
    return rms_norm(normed + ffn_branch, gain_two)

def reference(layer_in, query_proj, key_proj, value_proj, out_proj, gate_proj, up_proj, down_proj, first_gain, second_gain, seq_lengths, cotangent):
    weights = tuple((w.astype(jnp.float32) for w in (query_proj, key_proj, value_proj, out_proj, gate_proj, up_proj, down_proj, first_gain, second_gain)))
    group_slots = math.gcd(SLOTS, max(1, 4096 // SLOT_LEN))
    group_count = SLOTS // group_slots
    group_rows = group_slots * SLOT_LEN
    inputs = layer_in.astype(jnp.float32).reshape(group_count, group_rows, D)
    cotangents = cotangent.astype(jnp.float32).reshape(group_count, group_rows, D)
    lengths_all = seq_lengths.reshape(group_count, group_slots)

    def one_group(totals, item):
        rows_in, valid_len, rows_cot = item
        result, pullback = jax.vjp(lambda rows, params: layer(rows, valid_len, params), rows_in, weights)
        d_rows, d_params = pullback(rows_cot)
        totals = jax.tree.map(lambda a, b: a + b, totals, d_params)
        return (totals, (result, d_rows))
    zeros = jax.tree.map(jnp.zeros_like, weights)
    grads, (outputs, d_inputs) = lax.scan(one_group, zeros, (inputs, lengths_all, cotangents))
    return (outputs.reshape(TOKENS, D).astype(jnp.bfloat16), d_inputs.reshape(TOKENS, D).astype(jnp.bfloat16), grads[0], grads[1], grads[2], grads[3], grads[4], grads[5], grads[6], grads[7], grads[8])
```

```python
import functools

import jax
import jax.numpy as jnp
from jax import lax
from jax.experimental import pallas as pl
from jax.experimental.pallas import tpu as pltpu
from jax.sharding import PartitionSpec as P

HS = 64
SLOT_LEN = 1024
BLOCK = 8
VMEM_LIMIT = 60 << 20
F32 = jnp.float32
BF16 = jnp.bfloat16


def rms_norm(resid, gain):
    return resid * lax.rsqrt(jnp.mean(resid * resid, axis=-1, keepdims=True) + 1e-05) * gain


def swiglu(gate_pre, up_pre):
    return jax.nn.silu(gate_pre) * up_pre


def rotary_tables(rows):
    half = HS // 2
    positions = (jnp.arange(rows, dtype=jnp.int32) % SLOT_LEN).astype(F32)
    freqs = 10000.0 ** (-jnp.arange(half, dtype=F32) * 2.0 / HS)
    angles = positions[:, None] * freqs[None, :]
    return (jnp.cos(angles)[:, None, :], jnp.sin(angles)[:, None, :])


def rotate(field, cosines, sines):
    half = HS // 2
    first = field[..., :half]
    second = field[..., half:]
    return jnp.concatenate(
        [first * cosines - second * sines, second * cosines + first * sines], axis=-1
    )


def unrotate(grads, cosines, sines):
    half = HS // 2
    first = grads[..., :half]
    second = grads[..., half:]
    return jnp.concatenate(
        [first * cosines + second * sines, second * cosines - first * sines], axis=-1
    )


def cross(left, right):
    return lax.dot_general(left, right, (((0,), (0,)), ((), ())), preferred_element_type=F32)


def against(left, right):
    return lax.dot_general(left, right, (((1,), (1,)), ((), ())), preferred_element_type=F32)


def forward(left, right):
    return jnp.dot(left, right, preferred_element_type=F32)


def block_masks(block_index, block_rows, key_span, valid_len):
    query_pos = block_index * block_rows + jnp.arange(block_rows, dtype=jnp.int32)
    key_pos = jnp.arange(key_span, dtype=jnp.int32)
    allowed = (key_pos[None, :] <= query_pos[:, None]) & (key_pos[None, :] < valid_len)
    present = query_pos < valid_len
    return (allowed, present)


def block_scores(query_block, key_block, allowed):
    scores = (
        jnp.einsum("qhd,khd->hqk", query_block, key_block, preferred_element_type=F32) * 0.125
    )
    return jnp.where(allowed[None], scores, -1e30)


def attend(rot_queries, rot_keys, values_low, valid_len):
    block_rows = 512
    mixed_parts = []
    log_norms = []
    for block_index in range(SLOT_LEN // block_rows):
        start = block_index * block_rows
        key_span = start + block_rows
        allowed, present = block_masks(block_index, block_rows, key_span, valid_len)
        scores = block_scores(
            rot_queries[start : start + block_rows], rot_keys[:key_span], allowed
        )
        top = jnp.max(scores, axis=-1, keepdims=True)
        log_norm = top + jnp.log(jnp.sum(jnp.exp(scores - top), axis=-1, keepdims=True))
        probs_low = jnp.exp(scores - log_norm).astype(BF16)
        mixed = jnp.einsum(
            "hqk,khd->qhd", probs_low, values_low[:key_span], preferred_element_type=F32
        )
        mixed_parts.append(mixed * present.astype(F32)[:, None, None])
        log_norms.append(log_norm)
    return (jnp.concatenate(mixed_parts, axis=0), log_norms)


def attend_back(rot_queries, rot_keys, values_low, d_mixed, log_norms, valid_len):
    block_rows = 512
    query_parts = []
    key_total = jnp.zeros(rot_keys.shape, F32)
    value_total = jnp.zeros(rot_keys.shape, F32)
    for block_index in range(SLOT_LEN // block_rows):
        start = block_index * block_rows
        key_span = start + block_rows
        allowed, present = block_masks(block_index, block_rows, key_span, valid_len)
        query_block = rot_queries[start : start + block_rows]
        key_block = rot_keys[:key_span]
        value_block = values_low[:key_span]
        grad_block = d_mixed[start : start + block_rows] * present.astype(BF16)[:, None, None]
        scores = block_scores(query_block, key_block, allowed)
        attn_probs = jnp.exp(scores - log_norms[block_index])
        d_probs = jnp.einsum("qhd,khd->hqk", grad_block, value_block, preferred_element_type=F32)
        d_scores = (
            attn_probs * (d_probs - jnp.sum(d_probs * attn_probs, axis=-1, keepdims=True))
        ).astype(BF16)
        query_parts.append(
            jnp.einsum("hqk,khd->qhd", d_scores, key_block, preferred_element_type=F32) * 0.125
        )
        key_step = (
            jnp.einsum("hqk,qhd->khd", d_scores, query_block, preferred_element_type=F32) * 0.125
        )
        value_step = jnp.einsum(
            "hqk,qhd->khd", attn_probs.astype(BF16), grad_block, preferred_element_type=F32
        )
        key_total = key_total.at[:key_span].add(key_step)
        value_total = value_total.at[:key_span].add(value_step)
    return (jnp.concatenate(query_parts, axis=0), key_total, value_total)


class Links:
    def __init__(self, send, recv):
        self.send, self.recv = send, recv
        self.count = 0
        self.sent = []
        self.d = lax.axis_index("dp")
        self.z = lax.axis_index("mp")
        self.core = (self.flip(1), self.z)
        self.xn = (self.flip(2), self.z)
        self.yn = (self.flip(4), self.z)
        self.c = lax.rem(self.d, 2)
        self.x = lax.rem(lax.div(self.d, 2), 2)
        self.y = lax.rem(lax.div(self.d, 4), 2)

    def flip(self, step):
        bit = lax.rem(lax.div(self.d, step), 2)
        return self.d + step * (1 - 2 * bit)

    def along(self, r):
        return (self.d, lax.rem(self.z + r + 4, 4))

    def barrier(self):
        sem = pltpu.get_barrier_semaphore()
        targets = [self.core, self.xn, self.yn] + [self.along(r) for r in (1, 2, 3)]
        for target in targets:
            pl.semaphore_signal(
                sem, inc=1, device_id=target, device_id_type=pl.DeviceIdType.MESH
            )
        pl.semaphore_wait(sem, len(targets))

    def copy(self, src, dst, target):
        copy = pltpu.make_async_remote_copy(
            src_ref=src,
            dst_ref=dst,
            send_sem=self.send.at[self.count],
            recv_sem=self.recv.at[self.count],
            device_id=target,
            device_id_type=pl.DeviceIdType.MESH,
        )
        self.count += 1
        copy.start()
        self.sent.append(copy)
        return copy

    def drain(self):
        for copy in self.sent:
            copy.wait_send()


def cut_of(rows):
    line = rows // 4
    return max(16, (line // 2 + 15) // 16 * 16)


def piece(ref, lead, line, c, part):
    rows, cols = ref.shape[-2], ref.shape[-1]
    height, width, cut = rows // 4, cols // 2, cut_of(rows)
    first, size = {"all": (0, height), "a": (0, cut), "b": (cut, height - cut)}[part]
    at_rows = pl.ds(pl.multiple_of(line * height + first, 16), size)
    at_cols = pl.ds(pl.multiple_of(c * width, 128), width)
    if lead is None:
        return ref.at[at_rows, at_cols]
    return ref.at[lead, at_rows, at_cols]


def spread(links, ref, lead, mine):
    x, y, c = links.x, links.y, links.c
    own, off_x, off_y, far = 2 * y + x, 2 * y + 1 - x, 2 * (1 - y) + x, 3 - 2 * y - x

    def put(src, line, part, target):
        dst = piece(ref, lead, line, c, part)
        return links.copy(dst if src is None else src, dst, target)

    to_x = put(mine, own, "all", links.xn)
    to_y = put(mine, own, "all", links.yn)
    put_core = [put(mine, own, "all", links.core)]

    def relay():
        to_x.wait_recv()
        far_a = put(None, off_x, "a", links.yn)
        put_core.append(put(None, off_x, "all", links.core))
        to_y.wait_recv()
        far_b = put(None, off_y, "b", links.xn)
        put_core.append(put(None, off_y, "all", links.core))

        def last():
            far_a.wait_recv()
            put_core.append(put(None, far, "a", links.core))
            far_b.wait_recv()
            put_core.append(put(None, far, "b", links.core))

            def end():
                for copy in put_core:
                    copy.wait_recv()

            return end

        return last

    return relay


def gather_kernel(rels, *refs):
    n = len(rels)
    shards, outs = refs[:n], refs[n : 2 * n]
    links = Links(refs[2 * n], refs[2 * n + 1])
    links.barrier()
    line = 2 * links.y + links.x
    jobs = []
    for shard, out, rel in zip(shards, outs, rels):
        for slot, r in enumerate(rel):
            copy = links.copy(
                piece(shard, None, line, links.c, "all"),
                piece(out, slot, line, links.c, "all"),
                links.along(-r),
            )
            jobs.append((copy, out, slot))
    live = []
    for copy, out, slot in jobs:
        copy.wait_recv()
        live = [step() for step in live if step is not None]
        live.append(spread(links, out, slot, None))
    while any(step is not None for step in live):
        live = [step() for step in live if step is not None]
    links.drain()


def gather(shards, rels):
    copies = sum(10 * len(rel) for rel in rels)
    return pl.pallas_call(
        functools.partial(gather_kernel, rels),
        out_shape=[
            jax.ShapeDtypeStruct((len(rel),) + shard.shape, shard.dtype)
            for shard, rel in zip(shards, rels)
        ],
        in_specs=[pl.BlockSpec(memory_space=pl.ANY)] * len(shards),
        out_specs=[pl.BlockSpec(memory_space=pl.ANY)] * len(shards),
        scratch_shapes=[pltpu.SemaphoreType.DMA((copies,)), pltpu.SemaphoreType.DMA((copies,))],
        compiler_params=pltpu.CompilerParams(collective_id=0, has_side_effects=True),
        name="gather_weights",
    )(*shards)


def add_into(dst, left, right):
    dst[...] = left[...] + right[...]


class Reduction:
    def __init__(self, links, rel, part, out, from_core, acc, x_one, y_one, x_two, y_two, from_z):
        self.links, self.rel, self.part, self.out = links, rel, part, out
        self.from_core, self.acc = from_core, acc
        self.x_one, self.y_one, self.x_two, self.y_two = x_one, y_one, x_two, y_two
        self.from_z = from_z
        self.rows, self.cols = part.shape[1], part.shape[2]
        self.height, self.width = self.rows // 4, self.cols // 2
        self.cut = cut_of(self.rows)
        self.a = pl.ds(0, self.cut)
        self.b = pl.ds(self.cut, self.height - self.cut)

    def start(self):
        other = pl.ds(pl.multiple_of((1 - self.links.c) * self.width, 128), self.width)
        self.core = self.links.copy(
            self.part.at[:, :, other], self.from_core, self.links.core
        )
        return self.one

    def one(self):
        links, acc = self.links, self.acc
        self.core.wait_recv()
        n = len(self.rel)
        mine = pl.ds(pl.multiple_of(links.c * self.width, 128), self.width)
        for s in range(n):
            for line in range(4):
                rows = pl.ds(line * self.height, self.height)
                acc[s, line // 2, line % 2] = (
                    self.part[s, rows, mine] + self.from_core[s, rows, :]
                )
        self.to_x = links.copy(acc.at[:, :, 1 - links.x, self.a], self.x_one, links.xn)
        self.to_y = links.copy(acc.at[:, 1 - links.y, :, self.b], self.y_one, links.yn)
        return self.two

    def two(self):
        links, acc = self.links, self.acc
        x, y = links.x, links.y
        n = len(self.rel)
        self.to_x.wait_recv()
        for s in range(n):
            for row in range(2):
                acc[s, row, x, self.a] = acc[s, row, x, self.a] + self.x_one[s, row]
        self.to_y2 = links.copy(acc.at[:, 1 - y, x, self.a], self.y_two, links.yn)
        self.to_y.wait_recv()
        for s in range(n):
            for col in range(2):
                acc[s, y, col, self.b] = acc[s, y, col, self.b] + self.y_one[s, col]
        self.to_x2 = links.copy(acc.at[:, y, 1 - x, self.b], self.x_two, links.xn)
        return self.three

    def three(self):
        links, acc = self.links, self.acc
        x, y = links.x, links.y
        self.to_y2.wait_recv()
        self.to_x2.wait_recv()
        self.to_z = []
        order = list(range(1, len(self.rel))) + [0]
        for s in order:
            acc[s, y, x, self.a] = acc[s, y, x, self.a] + self.y_two[s]
            acc[s, y, x, self.b] = acc[s, y, x, self.b] + self.x_two[s]
            if s:
                self.to_z.append(
                    links.copy(
                        acc.at[s, y, x], self.from_z.at[s - 1], links.along(self.rel[s])
                    )
                )
        return self.four

    def four(self):
        links, acc = self.links, self.acc
        for copy in self.to_z:
            copy.wait_recv()
        total = acc[0, links.y, links.x].astype(F32)
        for s in range(len(self.rel) - 1):
            total = total + self.from_z[s].astype(F32)
        line = 2 * links.y + links.x
        target = piece(self.out, None, line, links.c, "all")
        target[...] = total.astype(BF16)
        return spread(links, self.out, None, None)


def reduce_kernel(rels, *refs):
    n = len(rels)
    parts, gains = refs[:n], refs[n]
    outs, gains_out = refs[n + 1 : 2 * n + 1], refs[2 * n + 1]
    rest = refs[2 * n + 2 :]
    links = Links(rest[0], rest[1])
    gain_core, gain_x, gain_y, gain_z, gain_acc = rest[2:7]
    rest = rest[7:]
    links.barrier()
    jobs = [
        Reduction(links, rel, parts[i], outs[i], *rest[7 * i : 7 * i + 7])
        for i, rel in enumerate(rels)
    ]
    gain_hops = [(gain_core, links.core), (gain_x, links.xn), (gain_y, links.yn)]

    def gain_step(level):
        def step():
            if level == 0:
                gain_acc[0] = gains[...]
            elif level <= 3:
                gain_step.copies[0].wait_recv()
                gain_acc[level] = gain_acc[level - 1] + gain_hops[level - 1][0][...]
            else:
                for copy in gain_step.copies:
                    copy.wait_recv()
                gains_out[...] = (
                    gain_acc[3] + gain_z[0] + gain_z[1] + gain_z[2]
                )
                return None
            if level < 3:
                buffer, target = gain_hops[level]
                gain_step.copies = [links.copy(gain_acc.at[level], buffer, target)]
            else:
                gain_step.copies = [
                    links.copy(gain_acc.at[3], gain_z.at[r - 1], links.along(r))
                    for r in (1, 2, 3)
                ]
            return gain_step(level + 1)

        return step

    live = [job.start() for job in jobs] + [gain_step(0)]
    waiting, live = live, []
    while waiting or live:
        if waiting:
            live.append(waiting.pop(0))
        nexts = []
        for step in live:
            follow = step()
            if follow is not None:
                nexts.append(follow)
        live = nexts
    links.drain()


def reduce_all(parts, rels, gains):
    scratch = []
    copies = 6
    for part, rel in zip(parts, rels):
        shards, rows, cols = part.shape
        height, width, cut = rows // 4, cols // 2, cut_of(rows)
        copies += 5 + len(rel) - 1 + 9 + 2
        scratch += [
            pltpu.VMEM((shards, rows, width), BF16),
            pltpu.VMEM((shards, 2, 2, height, width), BF16),
            pltpu.VMEM((shards, 2, cut, width), BF16),
            pltpu.VMEM((shards, 2, height - cut, width), BF16),
            pltpu.VMEM((shards, height - cut, width), BF16),
            pltpu.VMEM((shards, cut, width), BF16),
            pltpu.VMEM((max(1, shards - 1), height, width), BF16),
        ]
    n = len(parts)
    vmem = pl.BlockSpec(memory_space=pltpu.VMEM)
    return pl.pallas_call(
        functools.partial(reduce_kernel, rels),
        out_shape=[jax.ShapeDtypeStruct(part.shape[1:], BF16) for part in parts]
        + [jax.ShapeDtypeStruct(gains.shape, F32)],
        in_specs=[vmem] * (n + 1),
        out_specs=[vmem] * (n + 1),
        scratch_shapes=[
            pltpu.SemaphoreType.DMA((copies,)),
            pltpu.SemaphoreType.DMA((copies,)),
            pltpu.VMEM(gains.shape, F32),
            pltpu.VMEM(gains.shape, F32),
            pltpu.VMEM(gains.shape, F32),
            pltpu.VMEM((3,) + gains.shape, F32),
            pltpu.VMEM((4,) + gains.shape, F32),
        ]
        + scratch,
        compiler_params=pltpu.CompilerParams(
            collective_id=1, has_side_effects=True, vmem_limit_bytes=VMEM_LIMIT
        ),
        name="reduce_grads",
    )(*parts, gains)


ALL = (0, 1, 2, 3)
PAIRS = ((0, 1), (1, 0), (2, 3), (3, 2))


def halves(own, other, z):
    even = lax.rem(z, 2) == 0
    return jnp.concatenate([jnp.where(even, own, other), jnp.where(even, other, own)], axis=0)


def body(
    dp_size,
    layer_in,
    query_proj,
    key_proj,
    value_proj,
    out_proj,
    gate_proj,
    up_proj,
    down_proj,
    first_gain,
    second_gain,
    seq_lengths,
    cotangent,
):
    z = lax.axis_index("mp")
    even = lax.rem(z, 2) == 0
    rows = layer_in.shape[0]
    valid_len = lax.dynamic_index_in_dim(seq_lengths, lax.div(z, 2), keepdims=False)
    width = query_proj.shape[1]

    qkv_own = jnp.concatenate([query_proj.T, key_proj.T, value_proj.T], axis=0)
    qkv_far, out_far, gate_far, up_far, down_far = gather(
        (qkv_own, out_proj, gate_proj, up_proj, down_proj),
        ((2,), (1, 2, 3), (1, 2, 3), (1, 2, 3), (1, 2, 3)),
    )
    other_in = lax.ppermute(layer_in, "mp", PAIRS)
    slot_in = halves(layer_in, other_in, z)
    cosines, sines = rotary_tables(SLOT_LEN)

    raw = [against(slot_in, qkv_own), against(slot_in, qkv_far[0])]

    def heads(index):
        both = jnp.concatenate([r[:, index * width : (index + 1) * width] for r in raw], axis=1)
        return both.reshape(SLOT_LEN, -1, HS)

    rot_queries = rotate(heads(0), cosines, sines).astype(BF16)
    rot_keys = rotate(heads(1), cosines, sines).astype(BF16)
    values_low = heads(2).astype(BF16)
    mixed, log_norms = attend(rot_queries, rot_keys, values_low, valid_len)
    mixed_low = mixed.reshape(SLOT_LEN, 2 * width).astype(BF16)
    top, bottom = mixed_low[:rows], mixed_low[rows:]
    mixed_own = jnp.where(even, top, bottom)
    mixed_out = jnp.where(even, bottom, top)

    def swap(field):
        return jnp.concatenate([field[:, width:], field[:, :width]], axis=1)

    mixed_in = lax.ppermute(jnp.where(even, swap(mixed_out), mixed_out), "mp", PAIRS)
    mixed_all = jnp.concatenate(
        [mixed_own[:, :width], mixed_in[:, :width], mixed_own[:, width:], mixed_in[:, width:]],
        axis=1,
    )
    out_all = jnp.concatenate([out_proj[None], out_far], axis=0).reshape(4 * width, -1)
    resid_one = layer_in.astype(F32) + forward(mixed_all, out_all)
    normed, first_pull = jax.vjp(rms_norm, resid_one, first_gain)
    normed_low = normed.astype(BF16)

    gates = [gate_proj] + [gate_far[i] for i in range(3)]
    ups = [up_proj] + [up_far[i] for i in range(3)]
    downs = [down_proj] + [down_far[i] for i in range(3)]
    gate_pre = [forward(normed_low, w) for w in gates]
    up_pre = [forward(normed_low, w) for w in ups]
    hidden = [swiglu(g, u).astype(BF16) for g, u in zip(gate_pre, up_pre)]
    ffn_branch = sum(forward(h, w) for h, w in zip(hidden, downs))
    resid_two = normed + ffn_branch
    result, second_pull = jax.vjp(rms_norm, resid_two, second_gain)
    layer_out = result.astype(BF16)
    d_resid_two, second_part = second_pull(cotangent.astype(F32))
    ffn_out = d_resid_two.astype(BF16)
    d_normed = d_resid_two
    down_parts, gate_parts, up_parts = [], [], []
    for r in range(4):
        down_parts.append(cross(hidden[r], ffn_out).astype(BF16))
        d_hidden = against(ffn_out, downs[r])
        unused, glu_pull = jax.vjp(swiglu, gate_pre[r], up_pre[r])
        d_gate, d_up = (d.astype(BF16) for d in glu_pull(d_hidden))
        gate_parts.append(cross(normed_low, d_gate).astype(BF16))
        up_parts.append(cross(normed_low, d_up).astype(BF16))
        d_normed = d_normed + against(d_gate, gates[r]) + against(d_up, ups[r])
    d_resid_one, first_part = first_pull(d_normed)
    attn_out = d_resid_one.astype(BF16)
    out_part = cross(mixed_all, attn_out).astype(BF16).reshape(4, width, -1)
    d_all = against(attn_out, out_all).astype(BF16)
    d_own = jnp.concatenate([d_all[:, :width], d_all[:, 2 * width : 3 * width]], axis=1)
    d_send = jnp.concatenate([d_all[:, width : 2 * width], d_all[:, 3 * width :]], axis=1)
    d_recv = lax.ppermute(jnp.where(even, d_send, swap(d_send)), "mp", PAIRS)
    d_mixed = halves(d_own, d_recv, z).reshape(SLOT_LEN, -1, HS)
    d_rot_query, d_rot_key, d_value = attend_back(
        rot_queries, rot_keys, values_low, d_mixed, log_norms, valid_len
    )
    d_query = unrotate(d_rot_query, cosines, sines).reshape(SLOT_LEN, -1).astype(BF16)
    d_key = unrotate(d_rot_key, cosines, sines).reshape(SLOT_LEN, -1).astype(BF16)
    d_value = d_value.reshape(SLOT_LEN, -1).astype(BF16)
    d_raw = [
        jnp.concatenate([d[:, k * width : (k + 1) * width] for d in (d_query, d_key, d_value)], 1)
        for k in range(2)
    ]
    qkv_part = jnp.stack([cross(d, slot_in).astype(BF16) for d in d_raw])
    d_in = forward(d_raw[0], qkv_own) + forward(d_raw[1], qkv_far[0])
    d_top, d_bottom = d_in[:rows], d_in[rows:]
    in_recv = lax.ppermute(jnp.where(even, d_bottom, d_top).astype(BF16), "mp", PAIRS)
    input_grad = (d_resid_one + jnp.where(even, d_top, d_bottom) + in_recv.astype(F32)).astype(BF16)

    gains = jnp.concatenate(
        [first_part[None], second_part[None], jnp.zeros((6, first_part.shape[0]), F32)], axis=0
    )
    down_grad, gate_grad, up_grad, out_grad, qkv_grad, gains = reduce_all(
        (jnp.stack(down_parts), jnp.stack(gate_parts), jnp.stack(up_parts), out_part, qkv_part),
        (ALL, ALL, ALL, ALL, (0, 2)),
        gains,
    )
    down_grad, gate_grad, up_grad, out_grad, qkv_grad = (
        g.astype(F32) for g in (down_grad, gate_grad, up_grad, out_grad, qkv_grad)
    )
    if dp_size > BLOCK:
        groups = [list(range(i, dp_size, BLOCK)) for i in range(BLOCK)]
        down_grad, gate_grad, up_grad, out_grad, qkv_grad, gains = lax.psum(
            (down_grad, gate_grad, up_grad, out_grad, qkv_grad, gains),
            "dp",
            axis_index_groups=groups,
        )
    qkv_grad = qkv_grad.reshape(3, width, -1)
    return (
        layer_out,
        input_grad,
        qkv_grad[0].T,
        qkv_grad[1].T,
        qkv_grad[2].T,
        out_grad,
        gate_grad,
        up_grad,
        down_grad,
        gains[0],
        gains[1],
    )


def solution(mesh):
    rows = P(("dp", "mp"), None)
    cols, first = P(None, "mp"), P("mp", None)
    return jax.shard_map(
        functools.partial(body, mesh.shape["dp"]),
        mesh=mesh,
        in_specs=(rows, cols, cols, cols, first, cols, cols, first, P(), P(), P("dp"), rows),
        out_specs=(rows, rows, cols, cols, cols, first, cols, cols, first, P(), P()),
        check_vma=False,
    )
```

```python
import functools

import jax
import jax.numpy as jnp
from jax import lax
from jax.experimental import pallas as pl
from jax.experimental.pallas import tpu as pltpu
from jax.sharding import PartitionSpec as P

HS = 64
SLOT_LEN = 1024
BLOCK = 8
VMEM_LIMIT = 60 << 20
F32 = jnp.float32
BF16 = jnp.bfloat16


def rms_norm(resid, gain):
    return resid * lax.rsqrt(jnp.mean(resid * resid, axis=-1, keepdims=True) + 1e-05) * gain


def swiglu(gate_pre, up_pre):
    return jax.nn.silu(gate_pre) * up_pre


def rotary_tables(rows):
    half = HS // 2
    positions = (jnp.arange(rows, dtype=jnp.int32) % SLOT_LEN).astype(F32)
    freqs = 10000.0 ** (-jnp.arange(half, dtype=F32) * 2.0 / HS)
    angles = positions[:, None] * freqs[None, :]
    return (jnp.cos(angles)[:, None, :], jnp.sin(angles)[:, None, :])


def rotate(field, cosines, sines):
    half = HS // 2
    first = field[..., :half]
    second = field[..., half:]
    return jnp.concatenate(
        [first * cosines - second * sines, second * cosines + first * sines], axis=-1
    )


def unrotate(grads, cosines, sines):
    half = HS // 2
    first = grads[..., :half]
    second = grads[..., half:]
    return jnp.concatenate(
        [first * cosines + second * sines, second * cosines - first * sines], axis=-1
    )


def cross(left, right):
    return lax.dot_general(left, right, (((0,), (0,)), ((), ())), preferred_element_type=F32)


def against(left, right):
    return lax.dot_general(left, right, (((1,), (1,)), ((), ())), preferred_element_type=F32)


def forward(left, right):
    return jnp.dot(left, right, preferred_element_type=F32)


def block_masks(block_index, block_rows, key_span, valid_len):
    query_pos = block_index * block_rows + jnp.arange(block_rows, dtype=jnp.int32)
    key_pos = jnp.arange(key_span, dtype=jnp.int32)
    allowed = (key_pos[None, :] <= query_pos[:, None]) & (key_pos[None, :] < valid_len)
    present = query_pos < valid_len
    return (allowed, present)


def block_scores(query_block, key_block, allowed):
    scores = (
        jnp.einsum("qhd,khd->hqk", query_block, key_block, preferred_element_type=F32) * 0.125
    )
    return jnp.where(allowed[None], scores, -1e30)


def attend_back(rot_queries, rot_keys, values_low, d_mixed, log_norms, valid_len):
    block_rows = 512
    query_parts = []
    key_total = jnp.zeros(rot_keys.shape, F32)
    value_total = jnp.zeros(rot_keys.shape, F32)
    for block_index in range(SLOT_LEN // block_rows):
        start = block_index * block_rows
        key_span = start + block_rows
        allowed, present = block_masks(block_index, block_rows, key_span, valid_len)
        query_block = rot_queries[start : start + block_rows]
        key_block = rot_keys[:key_span]
        value_block = values_low[:key_span]
        grad_block = d_mixed[start : start + block_rows] * present.astype(BF16)[:, None, None]
        scores = block_scores(query_block, key_block, allowed)
        attn_probs = jnp.exp(scores - log_norms[:, start:key_span, None])
        d_probs = jnp.einsum("qhd,khd->hqk", grad_block, value_block, preferred_element_type=F32)
        d_scores = (
            attn_probs * (d_probs - jnp.sum(d_probs * attn_probs, axis=-1, keepdims=True))
        ).astype(BF16)
        query_parts.append(
            jnp.einsum("hqk,khd->qhd", d_scores, key_block, preferred_element_type=F32) * 0.125
        )
        key_step = (
            jnp.einsum("hqk,qhd->khd", d_scores, query_block, preferred_element_type=F32) * 0.125
        )
        value_step = jnp.einsum(
            "hqk,qhd->khd", attn_probs.astype(BF16), grad_block, preferred_element_type=F32
        )
        key_total = key_total.at[:key_span].add(key_step)
        value_total = value_total.at[:key_span].add(value_step)
    return (jnp.concatenate(query_parts, axis=0), key_total, value_total)


class Links:
    def __init__(self, send, recv):
        self.send, self.recv = send, recv
        self.count = 0
        self.sent = []
        self.d = lax.axis_index("dp")
        self.z = lax.axis_index("mp")
        self.core = (self.flip(1), self.z)
        self.xn = (self.flip(2), self.z)
        self.yn = (self.flip(4), self.z)
        self.c = lax.rem(self.d, 2)
        self.x = lax.rem(lax.div(self.d, 2), 2)
        self.y = lax.rem(lax.div(self.d, 4), 2)

    def flip(self, step):
        bit = lax.rem(lax.div(self.d, step), 2)
        return self.d + step * (1 - 2 * bit)

    def along(self, r):
        low, high = lax.rem(self.z, 2), lax.div(self.z, 2)
        low = 1 - low if r % 2 else low
        high = 1 - high if r // 2 else high
        return (self.d, 2 * high + low)

    def barrier(self):
        sem = pltpu.get_barrier_semaphore()
        targets = [self.core, self.xn, self.yn] + [self.along(r) for r in (1, 2, 3)]
        for target in targets:
            pl.semaphore_signal(
                sem, inc=1, device_id=target, device_id_type=pl.DeviceIdType.MESH
            )
        pl.semaphore_wait(sem, len(targets))

    def plan(self, src, dst, target):
        copy = pltpu.make_async_remote_copy(
            src_ref=src,
            dst_ref=dst,
            send_sem=self.send.at[self.count],
            recv_sem=self.recv.at[self.count],
            device_id=target,
            device_id_type=pl.DeviceIdType.MESH,
        )
        self.count += 1
        self.sent.append(copy)
        return copy

    def copy(self, src, dst, target):
        copy = self.plan(src, dst, target)
        copy.start()
        return copy

    def drain(self):
        for copy in self.sent:
            copy.wait_send()


def cut_of(rows):
    line = rows // 4
    return max(16, (line // 2 + 15) // 16 * 16)


def piece(ref, lead, line, c, part):
    rows, cols = ref.shape[-2], ref.shape[-1]
    height, width, cut = rows // 4, cols // 2, cut_of(rows)
    first, size = {"all": (0, height), "a": (0, cut), "b": (cut, height - cut)}[part]
    at_rows = pl.ds(pl.multiple_of(line * height + first, 16), size)
    at_cols = pl.ds(pl.multiple_of(c * width, 128), width)
    if lead is None:
        return ref.at[at_rows, at_cols]
    return ref.at[lead, at_rows, at_cols]


class Spread:
    def __init__(self, links, ref, lead):
        x, y, c = links.x, links.y, links.c
        own, off_x, off_y, far = 2 * y + x, 2 * y + 1 - x, 2 * (1 - y) + x, 3 - 2 * y - x

        def put(line, part, target):
            block = piece(ref, lead, line, c, part)
            return links.plan(block, block, target)

        self.to_x = put(own, "all", links.xn)
        self.to_y = put(own, "all", links.yn)
        self.far_a = put(off_x, "a", links.yn)
        self.far_b = put(off_y, "b", links.xn)
        self.cores = [
            put(own, "all", links.core),
            put(off_x, "all", links.core),
            put(off_y, "all", links.core),
            put(far, "a", links.core),
            put(far, "b", links.core),
        ]

    def start(self):
        self.to_x.start()
        self.to_y.start()
        self.cores[0].start()

    def relay(self):
        self.to_x.wait_recv()
        self.far_a.start()
        self.cores[1].start()
        self.to_y.wait_recv()
        self.far_b.start()
        self.cores[2].start()

    def last(self):
        self.far_a.wait_recv()
        self.cores[3].start()
        self.far_b.wait_recv()
        self.cores[4].start()

    def end(self):
        for copy in self.cores:
            copy.wait_recv()


class Gather:
    def __init__(self, links, shard, out, slot0, rels):
        line = 2 * links.y + links.x
        self.from_z = [
            links.plan(
                piece(shard, None, line, links.c, "all"),
                piece(out, slot0 + i, line, links.c, "all"),
                links.along(r),
            )
            for i, r in enumerate(rels)
        ]
        self.plane = Spread(links, out, pl.ds(slot0, len(rels)))
        self.steps = [self.arrive, self.plane.relay, self.plane.last, self.plane.end]

    def send(self):
        for copy in self.from_z:
            copy.start()

    def arrive(self):
        for copy in self.from_z:
            copy.wait_recv()
        self.plane.start()

    def step(self):
        if self.steps:
            self.steps.pop(0)()

    def finish(self):
        while self.steps:
            self.step()


def dot_nt(left, right):
    return lax.dot_general(left, right, (((1,), (1,)), ((), ())), preferred_element_type=F32)


def dot_tn(left, right):
    return lax.dot_general(left, right, (((0,), (0,)), ((), ())), preferred_element_type=F32)


def dot_nn(left, right):
    return lax.dot_general(left, right, (((1,), (0,)), ((), ())), preferred_element_type=F32)


def turned(values):
    lane = lax.broadcasted_iota(jnp.int32, values.shape, 1)
    return jnp.where(
        lax.rem(lane, HS) < HS // 2,
        pltpu.roll(values, 128 - HS // 2, 1),
        pltpu.roll(values, HS // 2, 1),
    )


def head_mask(head):
    lane = lax.broadcasted_iota(jnp.int32, (1, 128), 1)
    return jnp.where(lax.div(lane, HS) == head, 1.0, 0.0).astype(BF16)


QB = 256


def attention_kernel(
    len_ref, x_ref, qkv_ref, o_ref, cos_ref, sin_ref, gate_ref, up_ref, down_ref,
    x2, w2, wo, q_ref, k_ref, v_ref, m_all, stat, resid, gate_far, up_far, down_far,
    send, recv, m_ref, bias,
):
    links = Links(send, recv)
    rows = x_ref.shape[0]
    half = lax.rem(links.z, 2)
    mine = pl.ds(pl.multiple_of(half * rows, rows), rows)
    theirs = pl.ds(pl.multiple_of((1 - half) * rows, rows), rows)
    partner = links.along(1)
    length = len_ref[0]
    links.barrier()
    g_qkv = Gather(links, qkv_ref, w2, 1, (2,))
    g_out = Gather(links, o_ref, wo, 1, (2, 1, 3))
    g_gate = Gather(links, gate_ref, gate_far, 0, (2, 1, 3))
    g_up = Gather(links, up_ref, up_far, 0, (2, 1, 3))
    g_down = Gather(links, down_ref, down_far, 0, (2, 1, 3))
    g_qkv.send()
    swap_x = links.copy(x_ref, x2.at[mine], partner)
    g_out.send()
    g_gate.send()
    g_up.send()
    x2[mine, :] = x_ref[...]
    w2[0] = qkv_ref[...]
    wo[0] = o_ref[...]
    key_at = lax.broadcasted_iota(jnp.int32, (SLOT_LEN, QB), 0)
    bias[...] = jnp.where(key_at < length, 0.0, -1e30)
    stat[...] = jnp.zeros_like(stat)
    g_qkv.finish()
    swap_x.wait_recv()
    dim = x_ref.shape[1]
    w_rows = w2.shape[0] * w2.shape[1]
    for t, dst in enumerate((q_ref, k_ref, v_ref)):
        w = w2[:, :, t * dim : (t + 1) * dim].reshape(w_rows, dim)
        for block in range(2):
            at = pl.ds(block * 512, 512)
            raw = dot_nt(x2[at, :], w)
            for p in range(3):
                part = raw[:, p * 128 : (p + 1) * 128]
                if t < 2:
                    part = part * cos_ref[at, :] + turned(part) * sin_ref[at, :]
                if t == 0:
                    part = part.astype(BF16) * 0.125
                dst[at, p * 128 : (p + 1) * 128] = part.astype(BF16)
    g_out.step()

    ticks = {
        0: [g_gate.step, g_out.step],
        1: [g_up.step, g_gate.step, g_out.step],
        2: [g_up.step, g_gate.step],
    }

    def pair_step(p, carry):
        lanes = pl.ds(pl.multiple_of(p * 128, 128), 128)
        k_pair, v_turn = k_ref[:, lanes], v_ref[:, lanes].T
        keys = [k_pair * head_mask(h) for h in range(2)]
        for qb in range(SLOT_LEN // QB):
            at = pl.ds(qb * QB, QB)
            span = (qb + 1) * QB
            query = q_ref[at, lanes]
            query_at = qb * QB + lax.broadcasted_iota(jnp.int32, (1, QB), 1)
            outs = []
            for h in range(2):
                scores = dot_nt(keys[h][:span], query) + bias[:span, :]
                causal = lax.broadcasted_iota(jnp.int32, (QB, QB), 0) <= (
                    lax.broadcasted_iota(jnp.int32, (QB, QB), 1)
                )
                diag = jnp.where(causal, scores[span - QB :], -1e30)
                if qb:
                    scores = jnp.concatenate([scores[: span - QB], diag], axis=0)
                else:
                    scores = diag
                top = jnp.max(scores, axis=0, keepdims=True)
                probs = jnp.exp(scores - top)
                total = jnp.sum(probs, axis=0, keepdims=True)
                out = dot_nn(v_turn[h * HS : (h + 1) * HS, :span], probs.astype(BF16))
                outs.append(out * jnp.where(query_at < length, 1.0 / total, 0.0))
                stat[pl.ds(2 * p + h, 1), at] = top + jnp.log(total)
            m_ref[at, lanes] = jnp.concatenate(outs, axis=0).T.astype(BF16)
        for tick, steps in ticks.items():

            @pl.when(p == tick)
            def _(steps=steps):
                for step in steps:
                    step()

        return carry

    lax.fori_loop(0, 3, pair_step, 0)
    width = m_ref.shape[1]
    swap_m = links.copy(m_ref.at[theirs], m_all.at[:, pl.ds(width, width)], partner)
    g_down.send()
    m_all[:, :width] = m_ref[mine, :]
    wo_rows = wo.shape[1]
    g_out.finish()
    first = dot_nn(m_all[:, :width], wo[0:2].reshape(2 * wo_rows, dim))
    g_gate.step()
    g_up.step()
    swap_m.wait_recv()
    second = dot_nn(m_all[:, width:], wo[2:4].reshape(2 * wo_rows, dim))
    resid[...] = x_ref[...].astype(F32) + first + second
    g_gate.finish()
    g_up.finish()
    g_down.finish()
    links.drain()


def attention(length, layer_in, qkv_own, out_proj, cosines, sines, gate_proj, up_proj, down_proj):
    rows, dim = layer_in.shape
    width = out_proj.shape[0]
    vmem, hbm = pl.BlockSpec(memory_space=pltpu.VMEM), pl.BlockSpec(memory_space=pl.ANY)
    shape = jax.ShapeDtypeStruct
    copies = 64
    heads = shape((SLOT_LEN, 2 * width), BF16)
    return pl.pallas_call(
        attention_kernel,
        out_shape=[
            shape((SLOT_LEN, dim), BF16),
            shape((2,) + qkv_own.shape, BF16),
            shape((4,) + out_proj.shape, BF16),
            heads,
            heads,
            heads,
            shape((rows, 4 * width), BF16),
            shape((8, SLOT_LEN), F32),
            shape((rows, dim), F32),
            shape((3,) + gate_proj.shape, BF16),
            shape((3,) + up_proj.shape, BF16),
            shape((3,) + down_proj.shape, BF16),
        ],
        in_specs=[pl.BlockSpec(memory_space=pltpu.SMEM)] + [vmem] * 5 + [hbm] * 3,
        out_specs=[vmem] * 9 + [hbm] * 3,
        scratch_shapes=[
            pltpu.SemaphoreType.DMA((copies,)),
            pltpu.SemaphoreType.DMA((copies,)),
            pltpu.VMEM((SLOT_LEN, 2 * width), BF16),
            pltpu.VMEM((SLOT_LEN, QB), F32),
        ],
        compiler_params=pltpu.CompilerParams(
            collective_id=0, has_side_effects=True, vmem_limit_bytes=VMEM_LIMIT
        ),
        name="attention_forward",
    )(length, layer_in, qkv_own, out_proj, cosines, sines, gate_proj, up_proj, down_proj)


class Reduction:
    def __init__(self, links, rel, part, out, from_core, acc, x_one, y_one, x_two, y_two, from_z):
        self.links, self.rel, self.part, self.out = links, rel, part, out
        self.from_core, self.acc = from_core, acc
        self.x_one, self.y_one, self.x_two, self.y_two = x_one, y_one, x_two, y_two
        self.from_z = from_z
        self.rows, self.cols = part.shape[1], part.shape[2]
        self.height, self.width = self.rows // 4, self.cols // 2
        self.cut = cut_of(self.rows)
        self.a = pl.ds(0, self.cut)
        self.b = pl.ds(self.cut, self.height - self.cut)

    def start(self):
        other = pl.ds(pl.multiple_of((1 - self.links.c) * self.width, 128), self.width)
        self.core = self.links.copy(
            self.part.at[:, :, other], self.from_core, self.links.core
        )
        return self.one

    def one(self):
        links, acc = self.links, self.acc
        self.core.wait_recv()
        n = len(self.rel)
        mine = pl.ds(pl.multiple_of(links.c * self.width, 128), self.width)
        for s in range(n):
            for line in range(4):
                rows = pl.ds(line * self.height, self.height)
                acc[s, line // 2, line % 2] = (
                    self.part[s, rows, mine] + self.from_core[s, rows, :]
                )
        self.to_x = links.copy(acc.at[:, :, 1 - links.x, self.a], self.x_one, links.xn)
        self.to_y = links.copy(acc.at[:, 1 - links.y, :, self.b], self.y_one, links.yn)
        return self.two

    def two(self):
        links, acc = self.links, self.acc
        x, y = links.x, links.y
        n = len(self.rel)
        self.to_x.wait_recv()
        for s in range(n):
            for row in range(2):
                acc[s, row, x, self.a] = acc[s, row, x, self.a] + self.x_one[s, row]
        self.to_y2 = links.copy(acc.at[:, 1 - y, x, self.a], self.y_two, links.yn)
        self.to_y.wait_recv()
        for s in range(n):
            for col in range(2):
                acc[s, y, col, self.b] = acc[s, y, col, self.b] + self.y_one[s, col]
        self.to_x2 = links.copy(acc.at[:, y, 1 - x, self.b], self.x_two, links.xn)
        return self.three

    def three(self):
        links, acc = self.links, self.acc
        x, y = links.x, links.y
        self.to_y2.wait_recv()
        self.to_x2.wait_recv()
        self.to_z = []
        order = list(range(1, len(self.rel))) + [0]
        for s in order:
            acc[s, y, x, self.a] = acc[s, y, x, self.a] + self.y_two[s]
            acc[s, y, x, self.b] = acc[s, y, x, self.b] + self.x_two[s]
            if s:
                self.to_z.append(
                    links.copy(
                        acc.at[s, y, x], self.from_z.at[s - 1], links.along(self.rel[s])
                    )
                )
        return self.four

    def four(self):
        links, acc = self.links, self.acc
        for copy in self.to_z:
            copy.wait_recv()
        total = acc[0, links.y, links.x].astype(F32)
        for s in range(len(self.rel) - 1):
            total = total + self.from_z[s].astype(F32)
        line = 2 * links.y + links.x
        target = piece(self.out, None, line, links.c, "all")
        target[...] = total.astype(BF16)
        self.plane = Spread(links, self.out, None)
        self.plane.start()
        return self.five

    def five(self):
        self.plane.relay()
        return self.six

    def six(self):
        self.plane.last()
        return self.seven

    def seven(self):
        self.plane.end()
        return None


def reduce_kernel(rels, *refs):
    n = len(rels)
    parts, gains = refs[:n], refs[n]
    outs, gains_out = refs[n + 1 : 2 * n + 1], refs[2 * n + 1]
    rest = refs[2 * n + 2 :]
    links = Links(rest[0], rest[1])
    gain_core, gain_x, gain_y, gain_z, gain_acc = rest[2:7]
    rest = rest[7:]
    links.barrier()
    jobs = [
        Reduction(links, rel, parts[i], outs[i], *rest[7 * i : 7 * i + 7])
        for i, rel in enumerate(rels)
    ]
    gain_hops = [(gain_core, links.core), (gain_x, links.xn), (gain_y, links.yn)]

    def gain_step(level):
        def step():
            if level == 0:
                gain_acc[0] = gains[...]
            elif level <= 3:
                gain_step.copies[0].wait_recv()
                gain_acc[level] = gain_acc[level - 1] + gain_hops[level - 1][0][...]
            else:
                for copy in gain_step.copies:
                    copy.wait_recv()
                gains_out[...] = (
                    gain_acc[3] + gain_z[0] + gain_z[1] + gain_z[2]
                )
                return None
            if level < 3:
                buffer, target = gain_hops[level]
                gain_step.copies = [links.copy(gain_acc.at[level], buffer, target)]
            else:
                gain_step.copies = [
                    links.copy(gain_acc.at[3], gain_z.at[r - 1], links.along(r))
                    for r in (1, 2, 3)
                ]
            return gain_step(level + 1)

        return step

    live = [job.start() for job in jobs] + [gain_step(0)]
    waiting, live = live, []
    while waiting or live:
        if waiting:
            live.append(waiting.pop(0))
        nexts = []
        for step in live:
            follow = step()
            if follow is not None:
                nexts.append(follow)
        live = nexts
    links.drain()


def reduce_all(parts, rels, gains):
    scratch = []
    copies = 6
    for part, rel in zip(parts, rels):
        shards, rows, cols = part.shape
        height, width, cut = rows // 4, cols // 2, cut_of(rows)
        copies += 5 + len(rel) - 1 + 9 + 2
        scratch += [
            pltpu.VMEM((shards, rows, width), BF16),
            pltpu.VMEM((shards, 2, 2, height, width), BF16),
            pltpu.VMEM((shards, 2, cut, width), BF16),
            pltpu.VMEM((shards, 2, height - cut, width), BF16),
            pltpu.VMEM((shards, height - cut, width), BF16),
            pltpu.VMEM((shards, cut, width), BF16),
            pltpu.VMEM((max(1, shards - 1), height, width), BF16),
        ]
    n = len(parts)
    vmem = pl.BlockSpec(memory_space=pltpu.VMEM)
    return pl.pallas_call(
        functools.partial(reduce_kernel, rels),
        out_shape=[jax.ShapeDtypeStruct(part.shape[1:], BF16) for part in parts]
        + [jax.ShapeDtypeStruct(gains.shape, F32)],
        in_specs=[vmem] * (n + 1),
        out_specs=[vmem] * (n + 1),
        scratch_shapes=[
            pltpu.SemaphoreType.DMA((copies,)),
            pltpu.SemaphoreType.DMA((copies,)),
            pltpu.VMEM(gains.shape, F32),
            pltpu.VMEM(gains.shape, F32),
            pltpu.VMEM(gains.shape, F32),
            pltpu.VMEM((3,) + gains.shape, F32),
            pltpu.VMEM((4,) + gains.shape, F32),
        ]
        + scratch,
        compiler_params=pltpu.CompilerParams(
            collective_id=1, has_side_effects=True, vmem_limit_bytes=VMEM_LIMIT
        ),
        name="reduce_grads",
    )(*parts, gains)


ALL = (0, 2, 1, 3)
PAIRS = ((0, 1), (1, 0), (2, 3), (3, 2))


def halves(own, other, z):
    even = lax.rem(z, 2) == 0
    return jnp.concatenate([jnp.where(even, own, other), jnp.where(even, other, own)], axis=0)


def body(
    dp_size,
    layer_in,
    query_proj,
    key_proj,
    value_proj,
    out_proj,
    gate_proj,
    up_proj,
    down_proj,
    first_gain,
    second_gain,
    seq_lengths,
    cotangent,
):
    z = lax.axis_index("mp")
    even = lax.rem(z, 2) == 0
    rows = layer_in.shape[0]
    valid_len = lax.dynamic_index_in_dim(seq_lengths, lax.div(z, 2), keepdims=False)
    width = query_proj.shape[1]

    qkv_own = jnp.concatenate([query_proj.T, key_proj.T, value_proj.T], axis=1)
    cosines, sines = rotary_tables(SLOT_LEN)
    cos_wide = jnp.tile(cosines[:, 0, :], (1, 4))
    sin_wide = jnp.tile(jnp.concatenate([-sines[:, 0, :], sines[:, 0, :]], axis=1), (1, 2))
    (
        slot_in, qkv_all, out_all, rot_queries, rot_keys, values_low, mixed_all, stats,
        resid_one, gate_far, up_far, down_far,
    ) = attention(
        valid_len[None], layer_in, qkv_own, out_proj, cos_wide, sin_wide,
        gate_proj, up_proj, down_proj,
    )
    out_all = out_all.reshape(4 * width, -1)
    log_norms = stats[:6]
    rot_queries = (rot_queries * 8).reshape(SLOT_LEN, -1, HS)
    rot_keys = rot_keys.reshape(SLOT_LEN, -1, HS)
    values_low = values_low.reshape(SLOT_LEN, -1, HS)
    normed, first_pull = jax.vjp(rms_norm, resid_one, first_gain)
    normed_low = normed.astype(BF16)

    gates = [gate_proj] + [gate_far[i] for i in range(3)]
    ups = [up_proj] + [up_far[i] for i in range(3)]
    downs = [down_proj] + [down_far[i] for i in range(3)]
    gate_pre = [forward(normed_low, w) for w in gates]
    up_pre = [forward(normed_low, w) for w in ups]
    hidden = [swiglu(g, u).astype(BF16) for g, u in zip(gate_pre, up_pre)]
    ffn_branch = sum(forward(h, w) for h, w in zip(hidden, downs))
    resid_two = normed + ffn_branch
    result, second_pull = jax.vjp(rms_norm, resid_two, second_gain)
    layer_out = result.astype(BF16)
    d_resid_two, second_part = second_pull(cotangent.astype(F32))
    ffn_out = d_resid_two.astype(BF16)
    d_normed = d_resid_two
    down_parts, gate_parts, up_parts = [], [], []
    for r in range(4):
        down_parts.append(cross(hidden[r], ffn_out).astype(BF16))
        d_hidden = against(ffn_out, downs[r])
        unused, glu_pull = jax.vjp(swiglu, gate_pre[r], up_pre[r])
        d_gate, d_up = (d.astype(BF16) for d in glu_pull(d_hidden))
        gate_parts.append(cross(normed_low, d_gate).astype(BF16))
        up_parts.append(cross(normed_low, d_up).astype(BF16))
        d_normed = d_normed + against(d_gate, gates[r]) + against(d_up, ups[r])
    d_resid_one, first_part = first_pull(d_normed)
    attn_out = d_resid_one.astype(BF16)
    out_part = cross(mixed_all, attn_out).astype(BF16).reshape(4, width, -1)
    d_all = against(attn_out, out_all).astype(BF16)
    d_recv = lax.ppermute(d_all[:, 2 * width :], "mp", PAIRS)
    d_mixed = halves(d_all[:, : 2 * width], d_recv, z).reshape(SLOT_LEN, -1, HS)
    d_rot_query, d_rot_key, d_value = attend_back(
        rot_queries, rot_keys, values_low, d_mixed, log_norms, valid_len
    )
    d_query = unrotate(d_rot_query, cosines, sines).reshape(SLOT_LEN, -1).astype(BF16)
    d_key = unrotate(d_rot_key, cosines, sines).reshape(SLOT_LEN, -1).astype(BF16)
    d_value = d_value.reshape(SLOT_LEN, -1).astype(BF16)
    d_raw = [
        [d[:, k * width : (k + 1) * width] for d in (d_query, d_key, d_value)]
        for k in range(2)
    ]
    dim = layer_in.shape[1]
    qkv_part = jnp.stack(
        [jnp.concatenate([cross(t, slot_in).astype(BF16) for t in d], 1) for d in d_raw]
    )
    d_in = 0.0
    for k in range(2):
        for t in range(3):
            d_in = d_in + forward(d_raw[k][t], qkv_all[k, :, t * dim : (t + 1) * dim])
    d_top, d_bottom = d_in[:rows], d_in[rows:]
    in_recv = lax.ppermute(jnp.where(even, d_bottom, d_top).astype(BF16), "mp", PAIRS)
    input_grad = (d_resid_one + jnp.where(even, d_top, d_bottom) + in_recv.astype(F32)).astype(BF16)

    gains = jnp.concatenate(
        [first_part[None], second_part[None], jnp.zeros((6, first_part.shape[0]), F32)], axis=0
    )
    down_grad, gate_grad, up_grad, out_grad, qkv_grad, gains = reduce_all(
        (jnp.stack(down_parts), jnp.stack(gate_parts), jnp.stack(up_parts), out_part, qkv_part),
        (ALL, ALL, ALL, ALL, (0, 2)),
        gains,
    )
    down_grad, gate_grad, up_grad, out_grad, qkv_grad = (
        g.astype(F32) for g in (down_grad, gate_grad, up_grad, out_grad, qkv_grad)
    )
    if dp_size > BLOCK:
        groups = [list(range(i, dp_size, BLOCK)) for i in range(BLOCK)]
        down_grad, gate_grad, up_grad, out_grad, qkv_grad, gains = lax.psum(
            (down_grad, gate_grad, up_grad, out_grad, qkv_grad, gains),
            "dp",
            axis_index_groups=groups,
        )
    qkv_grad = [qkv_grad[:, t * dim : (t + 1) * dim] for t in range(3)]
    return (
        layer_out,
        input_grad,
        qkv_grad[0].T,
        qkv_grad[1].T,
        qkv_grad[2].T,
        out_grad,
        gate_grad,
        up_grad,
        down_grad,
        gains[0],
        gains[1],
    )


def solution(mesh):
    rows = P(("dp", "mp"), None)
    cols, first = P(None, "mp"), P("mp", None)
    return jax.shard_map(
        functools.partial(body, mesh.shape["dp"]),
        mesh=mesh,
        in_specs=(rows, cols, cols, cols, first, cols, cols, first, P(), P(), P("dp"), rows),
        out_specs=(rows, rows, cols, cols, cols, first, cols, cols, first, P(), P()),
        check_vma=False,
    )
```

```python
import functools

import jax
import jax.numpy as jnp
from jax import lax
from jax.experimental import pallas as pl
from jax.experimental.pallas import tpu as pltpu
from jax.sharding import PartitionSpec as P

HS = 64
SLOT_LEN = 1024
BLOCK = 8
VMEM_LIMIT = 60 << 20
F32 = jnp.float32
BF16 = jnp.bfloat16


def rms_norm(resid, gain):
    return resid * lax.rsqrt(jnp.mean(resid * resid, axis=-1, keepdims=True) + 1e-05) * gain


def swiglu(gate_pre, up_pre):
    return jax.nn.silu(gate_pre) * up_pre


def rotary_tables(rows):
    half = HS // 2
    positions = (jnp.arange(rows, dtype=jnp.int32) % SLOT_LEN).astype(F32)
    freqs = 10000.0 ** (-jnp.arange(half, dtype=F32) * 2.0 / HS)
    angles = positions[:, None] * freqs[None, :]
    return (jnp.cos(angles)[:, None, :], jnp.sin(angles)[:, None, :])


def cross(left, right):
    return lax.dot_general(left, right, (((0,), (0,)), ((), ())), preferred_element_type=F32)


def against(left, right):
    return lax.dot_general(left, right, (((1,), (1,)), ((), ())), preferred_element_type=F32)


def forward(left, right):
    return jnp.dot(left, right, preferred_element_type=F32)


class Links:
    def __init__(self, send, recv):
        self.send, self.recv = send, recv
        self.count = 0
        self.sent = []
        self.d = lax.axis_index("dp")
        self.z = lax.axis_index("mp")
        self.core = (self.flip(1), self.z)
        self.xn = (self.flip(2), self.z)
        self.yn = (self.flip(4), self.z)
        self.c = lax.rem(self.d, 2)
        self.x = lax.rem(lax.div(self.d, 2), 2)
        self.y = lax.rem(lax.div(self.d, 4), 2)

    def flip(self, step):
        bit = lax.rem(lax.div(self.d, step), 2)
        return self.d + step * (1 - 2 * bit)

    def along(self, r):
        low, high = lax.rem(self.z, 2), lax.div(self.z, 2)
        low = 1 - low if r % 2 else low
        high = 1 - high if r // 2 else high
        return (self.d, 2 * high + low)

    def barrier(self):
        sem = pltpu.get_barrier_semaphore()
        targets = [self.core, self.xn, self.yn] + [self.along(r) for r in (1, 2, 3)]
        for target in targets:
            pl.semaphore_signal(
                sem, inc=1, device_id=target, device_id_type=pl.DeviceIdType.MESH
            )
        pl.semaphore_wait(sem, len(targets))

    def plan(self, src, dst, target):
        copy = pltpu.make_async_remote_copy(
            src_ref=src,
            dst_ref=dst,
            send_sem=self.send.at[self.count],
            recv_sem=self.recv.at[self.count],
            device_id=target,
            device_id_type=pl.DeviceIdType.MESH,
        )
        self.count += 1
        self.sent.append(copy)
        return copy

    def copy(self, src, dst, target):
        copy = self.plan(src, dst, target)
        copy.start()
        return copy

    def drain(self):
        for copy in self.sent:
            copy.wait_send()


def cut_of(rows):
    line = rows // 4
    return max(16, (line // 2 + 15) // 16 * 16)


def piece(ref, lead, line, c, part):
    rows, cols = ref.shape[-2], ref.shape[-1]
    height, width, cut = rows // 4, cols // 2, cut_of(rows)
    first, size = {"all": (0, height), "a": (0, cut), "b": (cut, height - cut)}[part]
    at_rows = pl.ds(pl.multiple_of(line * height + first, 16), size)
    at_cols = pl.ds(pl.multiple_of(c * width, 128), width)
    if lead is None:
        return ref.at[at_rows, at_cols]
    return ref.at[lead, at_rows, at_cols]


class Spread:
    def __init__(self, links, ref, lead):
        x, y, c = links.x, links.y, links.c
        own, off_x, off_y, far = 2 * y + x, 2 * y + 1 - x, 2 * (1 - y) + x, 3 - 2 * y - x

        def put(line, part, target):
            block = piece(ref, lead, line, c, part)
            return links.plan(block, block, target)

        self.to_x = put(own, "all", links.xn)
        self.to_y = put(own, "all", links.yn)
        self.far_a = put(off_x, "a", links.yn)
        self.far_b = put(off_y, "b", links.xn)
        self.cores = [
            put(own, "all", links.core),
            put(off_x, "all", links.core),
            put(off_y, "all", links.core),
            put(far, "a", links.core),
            put(far, "b", links.core),
        ]

    def start(self):
        self.to_x.start()
        self.to_y.start()
        self.cores[0].start()

    def relay(self):
        self.to_x.wait_recv()
        self.far_a.start()
        self.cores[1].start()
        self.to_y.wait_recv()
        self.far_b.start()
        self.cores[2].start()

    def last(self):
        self.far_a.wait_recv()
        self.cores[3].start()
        self.far_b.wait_recv()
        self.cores[4].start()

    def end(self):
        for copy in self.cores:
            copy.wait_recv()


class Gather:
    def __init__(self, links, shard, out, slot0, rels):
        line = 2 * links.y + links.x
        self.from_z = [
            links.plan(
                piece(shard, None, line, links.c, "all"),
                piece(out, slot0 + i, line, links.c, "all"),
                links.along(r),
            )
            for i, r in enumerate(rels)
        ]
        self.plane = Spread(links, out, pl.ds(slot0, len(rels)))
        self.steps = [self.arrive, self.plane.relay, self.plane.last, self.plane.end]

    def send(self):
        for copy in self.from_z:
            copy.start()

    def arrive(self):
        for copy in self.from_z:
            copy.wait_recv()
        self.plane.start()

    def step(self):
        if self.steps:
            self.steps.pop(0)()

    def finish(self):
        while self.steps:
            self.step()


def dot_nt(left, right):
    return lax.dot_general(left, right, (((1,), (1,)), ((), ())), preferred_element_type=F32)


def dot_tn(left, right):
    return lax.dot_general(left, right, (((0,), (0,)), ((), ())), preferred_element_type=F32)


def dot_nn(left, right):
    return lax.dot_general(left, right, (((1,), (0,)), ((), ())), preferred_element_type=F32)


def turned(values):
    lane = lax.broadcasted_iota(jnp.int32, values.shape, 1)
    return jnp.where(
        lax.rem(lane, HS) < HS // 2,
        pltpu.roll(values, 128 - HS // 2, 1),
        pltpu.roll(values, HS // 2, 1),
    )


def head_mask(head):
    lane = lax.broadcasted_iota(jnp.int32, (1, 128), 1)
    return jnp.where(lax.div(lane, HS) == head, 1.0, 0.0).astype(BF16)


QB = 256


def attention_kernel(
    len_ref, x_ref, qkv_ref, o_ref, cos_ref, sin_ref, gate_ref, up_ref, down_ref,
    x2, w2, wo, q_ref, k_ref, v_ref, m_all, stat, resid, gate_far, up_far, down_far,
    send, recv, m_ref, bias,
):
    links = Links(send, recv)
    rows = x_ref.shape[0]
    half = lax.rem(links.z, 2)
    mine = pl.ds(pl.multiple_of(half * rows, rows), rows)
    theirs = pl.ds(pl.multiple_of((1 - half) * rows, rows), rows)
    partner = links.along(1)
    length = len_ref[0]
    links.barrier()
    g_qkv = Gather(links, qkv_ref, w2, 1, (2,))
    g_out = Gather(links, o_ref, wo, 1, (2, 1, 3))
    g_gate = Gather(links, gate_ref, gate_far, 0, (2, 1, 3))
    g_up = Gather(links, up_ref, up_far, 0, (2, 1, 3))
    g_down = Gather(links, down_ref, down_far, 0, (2, 1, 3))
    g_qkv.send()
    swap_x = links.copy(x_ref, x2.at[mine], partner)
    g_out.send()
    g_gate.send()
    g_up.send()
    x2[mine, :] = x_ref[...]
    w2[0] = qkv_ref[...]
    wo[0] = o_ref[...]
    key_at = lax.broadcasted_iota(jnp.int32, (SLOT_LEN, QB), 0)
    bias[...] = jnp.where(key_at < length, 0.0, -1e30)
    stat[...] = jnp.zeros_like(stat)
    g_qkv.finish()
    swap_x.wait_recv()
    dim = x_ref.shape[1]
    w_rows = w2.shape[0] * w2.shape[1]
    for t, dst in enumerate((q_ref, k_ref, v_ref)):
        w = w2[:, :, t * dim : (t + 1) * dim].reshape(w_rows, dim)
        for block in range(2):
            at = pl.ds(block * 512, 512)
            raw = dot_nt(x2[at, :], w)
            for p in range(3):
                part = raw[:, p * 128 : (p + 1) * 128]
                if t < 2:
                    part = part * cos_ref[at, :] + turned(part) * sin_ref[at, :]
                if t == 0:
                    part = part.astype(BF16) * 0.125
                dst[at, p * 128 : (p + 1) * 128] = part.astype(BF16)
    g_out.step()

    ticks = {
        0: [g_gate.step, g_out.step],
        1: [g_up.step, g_gate.step, g_out.step],
        2: [g_up.step, g_gate.step],
    }

    def pair_step(p, carry):
        lanes = pl.ds(pl.multiple_of(p * 128, 128), 128)
        k_pair, v_turn = k_ref[:, lanes], v_ref[:, lanes].T
        keys = [k_pair * head_mask(h) for h in range(2)]
        for qb in range(SLOT_LEN // QB):
            at = pl.ds(qb * QB, QB)
            span = (qb + 1) * QB
            query = q_ref[at, lanes]
            query_at = qb * QB + lax.broadcasted_iota(jnp.int32, (1, QB), 1)
            outs = []
            for h in range(2):
                scores = dot_nt(keys[h][:span], query) + bias[:span, :]
                causal = lax.broadcasted_iota(jnp.int32, (QB, QB), 0) <= (
                    lax.broadcasted_iota(jnp.int32, (QB, QB), 1)
                )
                diag = jnp.where(causal, scores[span - QB :], -1e30)
                if qb:
                    scores = jnp.concatenate([scores[: span - QB], diag], axis=0)
                else:
                    scores = diag
                top = jnp.max(scores, axis=0, keepdims=True)
                probs = jnp.exp(scores - top)
                total = jnp.sum(probs, axis=0, keepdims=True)
                out = dot_nn(v_turn[h * HS : (h + 1) * HS, :span], probs.astype(BF16))
                outs.append(out * jnp.where(query_at < length, 1.0 / total, 0.0))
                stat[pl.ds(2 * p + h, 1), at] = top + jnp.log(total)
            m_ref[at, lanes] = jnp.concatenate(outs, axis=0).T.astype(BF16)
        for tick, steps in ticks.items():

            @pl.when(p == tick)
            def _(steps=steps):
                for step in steps:
                    step()

        return carry

    lax.fori_loop(0, 3, pair_step, 0)
    width = m_ref.shape[1]
    swap_m = links.copy(m_ref.at[theirs], m_all.at[:, pl.ds(width, width)], partner)
    g_down.send()
    m_all[:, :width] = m_ref[mine, :]
    wo_rows = wo.shape[1]
    g_out.finish()
    first = dot_nn(m_all[:, :width], wo[0:2].reshape(2 * wo_rows, dim))
    g_gate.step()
    g_up.step()
    swap_m.wait_recv()
    second = dot_nn(m_all[:, width:], wo[2:4].reshape(2 * wo_rows, dim))
    resid[...] = x_ref[...].astype(F32) + first + second
    g_gate.finish()
    g_up.finish()
    g_down.finish()
    links.drain()


def attention(length, layer_in, qkv_own, out_proj, cosines, sines, gate_proj, up_proj, down_proj):
    rows, dim = layer_in.shape
    width = out_proj.shape[0]
    vmem, hbm = pl.BlockSpec(memory_space=pltpu.VMEM), pl.BlockSpec(memory_space=pl.ANY)
    shape = jax.ShapeDtypeStruct
    copies = 64
    heads = shape((SLOT_LEN, 2 * width), BF16)
    return pl.pallas_call(
        attention_kernel,
        out_shape=[
            shape((SLOT_LEN, dim), BF16),
            shape((2,) + qkv_own.shape, BF16),
            shape((4,) + out_proj.shape, BF16),
            heads,
            heads,
            heads,
            shape((rows, 4 * width), BF16),
            shape((8, SLOT_LEN), F32),
            shape((rows, dim), F32),
            shape((3,) + gate_proj.shape, BF16),
            shape((3,) + up_proj.shape, BF16),
            shape((3,) + down_proj.shape, BF16),
        ],
        in_specs=[pl.BlockSpec(memory_space=pltpu.SMEM)] + [vmem] * 5 + [hbm] * 3,
        out_specs=[vmem] * 9 + [hbm] * 3,
        scratch_shapes=[
            pltpu.SemaphoreType.DMA((copies,)),
            pltpu.SemaphoreType.DMA((copies,)),
            pltpu.VMEM((SLOT_LEN, 2 * width), BF16),
            pltpu.VMEM((SLOT_LEN, QB), F32),
        ],
        compiler_params=pltpu.CompilerParams(
            collective_id=0, has_side_effects=True, vmem_limit_bytes=VMEM_LIMIT
        ),
        name="attention_forward",
    )(length, layer_in, qkv_own, out_proj, cosines, sines, gate_proj, up_proj, down_proj)


class Steps:
    def step(self):
        if self.steps:
            self.steps.pop(0)()


class Reduction(Steps):
    def __init__(self, links, rel, parts, out, acc, x_one, y_one, x_two, y_two, from_z):
        self.links, self.parts, self.out, self.acc = links, parts, out, acc
        self.x_one, self.y_one, self.x_two, self.y_two = x_one, y_one, x_two, y_two
        self.from_z = from_z
        x, y, c = links.x, links.y, links.c
        height, width = acc.shape[3], acc.shape[4]
        cut = cut_of(4 * height)
        self.a, self.b = pl.ds(0, cut), pl.ds(cut, height - cut)
        self.mine = pl.ds(pl.multiple_of(c * width, 128), width)
        other = pl.ds(pl.multiple_of((1 - c) * width, 128), width)
        self.n = len(rel)
        self.core = [
            links.plan(parts[s].at[:, :, :, other], acc.at[s], links.core) for s in range(self.n)
        ]
        self.to_x = links.plan(acc.at[:, :, 1 - x, self.a], x_one, links.xn)
        self.to_y = links.plan(acc.at[:, 1 - y, :, self.b], y_one, links.yn)
        self.to_y2 = links.plan(acc.at[:, 1 - y, x, self.a], y_two, links.yn)
        self.to_x2 = links.plan(acc.at[:, y, 1 - x, self.b], x_two, links.xn)
        self.to_z = [
            links.plan(acc.at[s, y, x], from_z.at[s - 1], links.along(rel[s]))
            for s in range(1, self.n)
        ]
        self.plane = Spread(links, out, None)
        self.total = piece(out, None, 2 * y + x, c, "all")
        self.steps = [
            self.start, self.one, self.two, self.three, self.four,
            self.plane.relay, self.plane.last, self.plane.end,
        ]

    def start(self):
        for copy in self.core:
            copy.start()

    def one(self):
        acc = self.acc
        for s in range(self.n):
            self.core[s].wait_recv()
            acc[s] = acc[s] + self.parts[s][:, :, :, self.mine]
        self.to_x.start()
        self.to_y.start()

    def two(self):
        acc, x, y = self.acc, self.links.x, self.links.y
        self.to_x.wait_recv()
        for s in range(self.n):
            for row in range(2):
                acc[s, row, x, self.a] = acc[s, row, x, self.a] + self.x_one[s, row]
        self.to_y2.start()
        self.to_y.wait_recv()
        for s in range(self.n):
            for col in range(2):
                acc[s, y, col, self.b] = acc[s, y, col, self.b] + self.y_one[s, col]
        self.to_x2.start()

    def three(self):
        acc, x, y = self.acc, self.links.x, self.links.y
        self.to_y2.wait_recv()
        self.to_x2.wait_recv()
        for s in list(range(1, self.n)) + [0]:
            acc[s, y, x, self.a] = acc[s, y, x, self.a] + self.y_two[s]
            acc[s, y, x, self.b] = acc[s, y, x, self.b] + self.x_two[s]
            if s:
                self.to_z[s - 1].start()

    def four(self):
        for copy in self.to_z:
            copy.wait_recv()
        total = self.acc[0, self.links.y, self.links.x].astype(F32)
        for s in range(self.n - 1):
            total = total + self.from_z[s].astype(F32)
        self.total[...] = total.astype(BF16)
        self.plane.start()


class GainSum(Steps):
    def __init__(self, links, gains, out, from_core, from_x, from_y, from_z, acc):
        self.gains, self.out, self.from_z, self.acc = gains, out, from_z, acc
        self.hops = [
            (from_core, links.plan(acc.at[0], from_core, links.core)),
            (from_x, links.plan(acc.at[1], from_x, links.xn)),
            (from_y, links.plan(acc.at[2], from_y, links.yn)),
        ]
        self.to_z = [links.plan(acc.at[3], from_z.at[r - 1], links.along(r)) for r in (1, 2, 3)]
        self.steps = [self.start] + [functools.partial(self.hop, i) for i in range(3)] + [self.end]

    def start(self):
        self.acc[0] = self.gains[...]
        self.hops[0][1].start()

    def hop(self, i):
        self.hops[i][1].wait_recv()
        self.acc[i + 1] = self.acc[i] + self.hops[i][0][...]
        for copy in [self.hops[i + 1][1]] if i < 2 else self.to_z:
            copy.start()

    def end(self):
        for copy in self.to_z:
            copy.wait_recv()
        self.out[...] = self.acc[3] + self.from_z[0] + self.from_z[1] + self.from_z[2]


def backward_kernel(
    len_ref, d_ref, x2, w2, q_ref, k_ref, v_ref, stat, cos_ref, sin_ref, resid, gains, out_part,
    *refs,
):
    down_parts, gate_parts, up_parts = refs[0:4], refs[4:8], refs[8:12]
    in_grad, down_out, gate_out, up_out, out_out, qkv_out, gains_out = refs[12:19]
    send, recv, d2, bias, d_raw, dk_acc, dv_acc, qkv_part, in_send, in_recv = refs[19:29]
    gain_refs, rest = refs[29:34], refs[34:]
    links = Links(send, recv)
    rows, dim = resid.shape
    width = d2.shape[1]
    half = lax.rem(links.z, 2)
    mine = pl.ds(pl.multiple_of(half * rows, rows), rows)
    theirs = pl.ds(pl.multiple_of((1 - half) * rows, rows), rows)
    partner = links.along(1)
    length = len_ref[0]
    links.barrier()
    swaps = [
        links.plan(
            d_ref.at[:, pl.ds(width + p * 128, 128)], d2.at[mine, pl.ds(p * 128, 128)], partner
        )
        for p in range(3)
    ]
    swap_in = links.plan(in_send, in_recv, partner)
    qkv_parts = [qkv_part.at[s] for s in range(2)]
    out_parts = [out_part.at[s] for s in range(4)]
    down, gate, up, out = (
        Reduction(links, ALL, parts, result, *rest[6 * i : 6 * i + 6])
        for i, (parts, result) in enumerate(
            [(down_parts, down_out), (gate_parts, gate_out), (up_parts, up_out),
             (out_parts, out_out)]
        )
    )
    qkv = Reduction(links, (0, 2), qkv_parts, qkv_out, *rest[24:30])
    gain = GainSum(links, gains, gains_out, *gain_refs)
    for copy in swaps:
        copy.start()
    for job in (down, gate, up, out, gain):
        job.step()
    d2[mine, :] = d_ref[:, :width]
    key_at = lax.broadcasted_iota(jnp.int32, (SLOT_LEN, QB), 0)
    bias[...] = jnp.where(key_at < length, 0.0, -1e30)
    down.step()

    plan = [
        [], [gate], [gain], [down], [up], [gain],
        [gate], [down], [gain], [up, out], [gate], [gain],
    ]
    plan = [[job.steps.pop(0) for job in jobs] for jobs in plan]

    def pair_step(p, carry):
        lanes = pl.ds(pl.multiple_of(p * 128, 128), 128)
        for i in range(3):

            @pl.when(p == i)
            def _(i=i):
                swaps[i].wait_recv()

        k_pair, v_pair = k_ref[:, lanes], v_ref[:, lanes]
        k_turn = k_pair.T
        keys = [k_pair * head_mask(h) for h in range(2)]
        values = [v_pair * head_mask(h) for h in range(2)]
        for turn, qb in enumerate(reversed(range(SLOT_LEN // QB))):
            at = pl.ds(qb * QB, QB)
            span = (qb + 1) * QB
            query = q_ref[at, lanes]
            query_at = qb * QB + lax.broadcasted_iota(jnp.int32, (QB, 128), 0)
            present = jnp.where(query_at < length, 1.0, 0.0).astype(BF16)
            grad = d2[at, lanes] * present
            d_scores, probs_low, d_query = [], [], []
            for h in range(2):
                scores = dot_nt(keys[h][:span], query) + bias[:span, :]
                causal = lax.broadcasted_iota(jnp.int32, (QB, QB), 0) <= (
                    lax.broadcasted_iota(jnp.int32, (QB, QB), 1)
                )
                diag = jnp.where(causal, scores[span - QB :], -1e30)
                if qb:
                    scores = jnp.concatenate([scores[: span - QB], diag], axis=0)
                else:
                    scores = diag
                probs = jnp.exp(scores - stat[pl.ds(2 * p + h, 1), at])
                d_probs = dot_nt(values[h][:span], grad)
                total = jnp.sum(d_probs * probs, axis=0, keepdims=True)
                d_score = (probs * (d_probs - total)).astype(BF16)
                d_query.append(dot_nn(k_turn[h * HS : (h + 1) * HS, :span], d_score))
                d_scores.append(d_score)
                probs_low.append(probs.astype(BF16))
            d_key = dot_nn(
                jnp.concatenate(d_scores, axis=1),
                jnp.concatenate([query * head_mask(h) for h in range(2)], axis=0),
            )
            d_value = dot_nn(
                jnp.concatenate(probs_low, axis=1),
                jnp.concatenate([grad * head_mask(h) for h in range(2)], axis=0),
            )
            if turn == 0:
                dk_acc[...] = d_key
                dv_acc[...] = d_value
            else:
                dk_acc[:span, :] = dk_acc[:span, :] + d_key
                dv_acc[:span, :] = dv_acc[:span, :] + d_value
            part = jnp.concatenate(d_query, axis=0).T * 0.125
            part = part * cos_ref[at, :] - turned(part) * sin_ref[at, :]
            d_raw[at, lanes] = part.astype(BF16)
            for i in range(3):
                steps = plan[4 * i + turn]
                if steps:

                    @pl.when(p == i)
                    def _(steps=steps):
                        for step in steps:
                            step()

        part = dk_acc[...]
        part = part * cos_ref[...] - turned(part) * sin_ref[...]
        d_raw[:, pl.ds(pl.multiple_of(width + p * 128, 128), 128)] = part.astype(BF16)
        d_raw[:, pl.ds(pl.multiple_of(2 * width + p * 128, 128), 128)] = dv_acc[...].astype(BF16)
        return carry

    lax.fori_loop(0, 3, pair_step, 0)
    for t in range(3):
        grads = dot_nn(d_raw[:, t * width : (t + 1) * width].T, x2[...]).astype(BF16)
        qkv_part[:, :, :, :, t * dim : (t + 1) * dim] = grads.reshape(qkv_part.shape[:4] + (dim,))
    qkv.step()
    weights = [w2[:, :, t * dim : (t + 1) * dim].reshape(width, dim) for t in range(3)]

    def project(at):
        return sum(
            dot_nn(d_raw[at, t * width : (t + 1) * width], weights[t]) for t in range(3)
        )

    in_send[...] = project(theirs).astype(BF16)
    swap_in.start()
    qkv.step()
    jobs = [down, gate, up, out, qkv, gain]
    own = resid[...] + project(mine)
    for job in jobs:
        job.step()
    swap_in.wait_recv()
    in_grad[...] = (own + in_recv[...].astype(F32)).astype(BF16)
    while any(job.steps for job in jobs):
        for job in jobs:
            job.step()
    links.drain()


def backward(
    length, d_all, slot_in, qkv_all, queries, keys, values, stats, cosines, sines, d_resid, gains,
    out_part, down_parts, gate_parts, up_parts,
):
    rows, dim = d_resid.shape
    width = queries.shape[1]
    shape = jax.ShapeDtypeStruct
    parts = [down_parts, gate_parts, up_parts, [out_part[s] for s in range(4)]]
    shards = [(4,) + p[0].shape for p in parts]
    shards.append((2, 2, 2, width // 8, qkv_all.shape[2]))
    scratch = []
    copies = 4 + 6
    for n, _, _, height, cols in shards:
        half, cut = cols // 2, cut_of(4 * height)
        copies += 2 * n + 3 + 9
        scratch += [
            pltpu.VMEM((n, 2, 2, height, half), BF16),
            pltpu.VMEM((n, 2, cut, half), BF16),
            pltpu.VMEM((n, 2, height - cut, half), BF16),
            pltpu.VMEM((n, height - cut, half), BF16),
            pltpu.VMEM((n, cut, half), BF16),
            pltpu.VMEM((n - 1, height, half), BF16),
        ]
    vmem = pl.BlockSpec(memory_space=pltpu.VMEM)
    return pl.pallas_call(
        backward_kernel,
        out_shape=[shape((rows, dim), BF16)]
        + [shape((4 * s[3], s[4]), BF16) for s in shards]
        + [shape(gains.shape, F32)],
        in_specs=[pl.BlockSpec(memory_space=pltpu.SMEM)] + [vmem] * 24,
        out_specs=[vmem] * 7,
        scratch_shapes=[
            pltpu.SemaphoreType.DMA((copies,)),
            pltpu.SemaphoreType.DMA((copies,)),
            pltpu.VMEM((SLOT_LEN, width), BF16),
            pltpu.VMEM((SLOT_LEN, QB), F32),
            pltpu.VMEM((SLOT_LEN, 3 * width), BF16),
            pltpu.VMEM((SLOT_LEN, 128), F32),
            pltpu.VMEM((SLOT_LEN, 128), F32),
            pltpu.VMEM(shards[4], BF16),
            pltpu.VMEM((rows, dim), BF16),
            pltpu.VMEM((rows, dim), BF16),
            pltpu.VMEM(gains.shape, F32),
            pltpu.VMEM(gains.shape, F32),
            pltpu.VMEM(gains.shape, F32),
            pltpu.VMEM((3,) + gains.shape, F32),
            pltpu.VMEM((4,) + gains.shape, F32),
        ]
        + scratch,
        compiler_params=pltpu.CompilerParams(
            collective_id=1, has_side_effects=True, vmem_limit_bytes=VMEM_LIMIT
        ),
        name="attention_backward",
    )(
        length, d_all, slot_in, qkv_all, queries, keys, values, stats, cosines, sines, d_resid,
        gains, out_part, *down_parts, *gate_parts, *up_parts,
    )


ALL = (0, 2, 1, 3)


def quarters(part):
    return part.astype(BF16).reshape(2, 2, part.shape[0] // 4, part.shape[1])


def body(
    dp_size,
    layer_in,
    query_proj,
    key_proj,
    value_proj,
    out_proj,
    gate_proj,
    up_proj,
    down_proj,
    first_gain,
    second_gain,
    seq_lengths,
    cotangent,
):
    z = lax.axis_index("mp")
    valid_len = lax.dynamic_index_in_dim(seq_lengths, lax.div(z, 2), keepdims=False)
    width = query_proj.shape[1]

    qkv_own = jnp.concatenate([query_proj.T, key_proj.T, value_proj.T], axis=1)
    cosines, sines = rotary_tables(SLOT_LEN)
    cos_wide = jnp.tile(cosines[:, 0, :], (1, 4))
    sin_wide = jnp.tile(jnp.concatenate([-sines[:, 0, :], sines[:, 0, :]], axis=1), (1, 2))
    (
        slot_in, qkv_all, out_all, rot_queries, rot_keys, values_low, mixed_all, stats,
        resid_one, gate_far, up_far, down_far,
    ) = attention(
        valid_len[None], layer_in, qkv_own, out_proj, cos_wide, sin_wide,
        gate_proj, up_proj, down_proj,
    )
    out_all = out_all.reshape(4 * width, -1)
    normed, first_pull = jax.vjp(rms_norm, resid_one, first_gain)
    normed_low = normed.astype(BF16)

    gates = [gate_proj] + [gate_far[i] for i in range(3)]
    ups = [up_proj] + [up_far[i] for i in range(3)]
    downs = [down_proj] + [down_far[i] for i in range(3)]
    gate_pre = [forward(normed_low, w) for w in gates]
    up_pre = [forward(normed_low, w) for w in ups]
    hidden = [swiglu(g, u).astype(BF16) for g, u in zip(gate_pre, up_pre)]
    ffn_branch = sum(forward(h, w) for h, w in zip(hidden, downs))
    resid_two = normed + ffn_branch
    result, second_pull = jax.vjp(rms_norm, resid_two, second_gain)
    layer_out = result.astype(BF16)
    d_resid_two, second_part = second_pull(cotangent.astype(F32))
    ffn_out = d_resid_two.astype(BF16)
    d_normed = d_resid_two
    down_parts, gate_parts, up_parts = [], [], []
    for r in range(4):
        down_parts.append(quarters(cross(hidden[r], ffn_out)))
        d_hidden = against(ffn_out, downs[r])
        unused, glu_pull = jax.vjp(swiglu, gate_pre[r], up_pre[r])
        d_gate, d_up = (d.astype(BF16) for d in glu_pull(d_hidden))
        gate_parts.append(quarters(cross(normed_low, d_gate)))
        up_parts.append(quarters(cross(normed_low, d_up)))
        d_normed = d_normed + against(d_gate, gates[r]) + against(d_up, ups[r])
    d_resid_one, first_part = first_pull(d_normed)
    attn_out = d_resid_one.astype(BF16)
    out_part = cross(mixed_all, attn_out).astype(BF16).reshape(4, 2, 2, width // 4, -1)
    d_all = against(attn_out, out_all).astype(BF16)
    gains = jnp.concatenate(
        [first_part[None], second_part[None], jnp.zeros((6, first_part.shape[0]), F32)], axis=0
    )
    input_grad, down_grad, gate_grad, up_grad, out_grad, qkv_grad, gains = backward(
        valid_len[None], d_all, slot_in, qkv_all, rot_queries, rot_keys, values_low, stats,
        cos_wide, sin_wide, d_resid_one, gains, out_part, down_parts, gate_parts, up_parts,
    )
    dim = layer_in.shape[1]
    down_grad, gate_grad, up_grad, out_grad, qkv_grad = (
        g.astype(F32) for g in (down_grad, gate_grad, up_grad, out_grad, qkv_grad)
    )
    if dp_size > BLOCK:
        groups = [list(range(i, dp_size, BLOCK)) for i in range(BLOCK)]
        down_grad, gate_grad, up_grad, out_grad, qkv_grad, gains = lax.psum(
            (down_grad, gate_grad, up_grad, out_grad, qkv_grad, gains),
            "dp",
            axis_index_groups=groups,
        )
    qkv_grad = [qkv_grad[:, t * dim : (t + 1) * dim] for t in range(3)]
    return (
        layer_out,
        input_grad,
        qkv_grad[0].T,
        qkv_grad[1].T,
        qkv_grad[2].T,
        out_grad,
        gate_grad,
        up_grad,
        down_grad,
        gains[0],
        gains[1],
    )


def solution(mesh):
    rows = P(("dp", "mp"), None)
    cols, first = P(None, "mp"), P("mp", None)
    return jax.shard_map(
        functools.partial(body, mesh.shape["dp"]),
        mesh=mesh,
        in_specs=(rows, cols, cols, cols, first, cols, cols, first, P(), P(), P("dp"), rows),
        out_specs=(rows, rows, cols, cols, cols, first, cols, cols, first, P(), P()),
        check_vma=False,
    )
```

```python
import functools

import jax
import jax.numpy as jnp
from jax import lax
from jax.experimental import pallas as pl
from jax.experimental.pallas import tpu as pltpu
from jax.sharding import PartitionSpec as P

HS = 64
SLOT_LEN = 1024
BLOCK = 8
VMEM_LIMIT = 60 << 20
F32 = jnp.float32
BF16 = jnp.bfloat16


def rms_norm(resid, gain):
    return resid * lax.rsqrt(jnp.mean(resid * resid, axis=-1, keepdims=True) + 1e-05) * gain


def swiglu(gate_pre, up_pre):
    return jax.nn.silu(gate_pre) * up_pre


def rotary_tables(rows):
    half = HS // 2
    positions = (jnp.arange(rows, dtype=jnp.int32) % SLOT_LEN).astype(F32)
    freqs = 10000.0 ** (-jnp.arange(half, dtype=F32) * 2.0 / HS)
    angles = positions[:, None] * freqs[None, :]
    return (jnp.cos(angles)[:, None, :], jnp.sin(angles)[:, None, :])


def cross(left, right):
    return lax.dot_general(left, right, (((0,), (0,)), ((), ())), preferred_element_type=F32)


def against(left, right):
    return lax.dot_general(left, right, (((1,), (1,)), ((), ())), preferred_element_type=F32)


def forward(left, right):
    return jnp.dot(left, right, preferred_element_type=F32)


class Links:
    def __init__(self, send, recv):
        self.send, self.recv = send, recv
        self.count = 0
        self.sent = []
        self.d = lax.axis_index("dp")
        self.z = lax.axis_index("mp")
        self.core = (self.flip(1), self.z)
        self.xn = (self.flip(2), self.z)
        self.yn = (self.flip(4), self.z)
        self.c = lax.rem(self.d, 2)
        self.x = lax.rem(lax.div(self.d, 2), 2)
        self.y = lax.rem(lax.div(self.d, 4), 2)

    def flip(self, step):
        bit = lax.rem(lax.div(self.d, step), 2)
        return self.d + step * (1 - 2 * bit)

    def along(self, r):
        low, high = lax.rem(self.z, 2), lax.div(self.z, 2)
        low = 1 - low if r % 2 else low
        high = 1 - high if r // 2 else high
        return (self.d, 2 * high + low)

    def barrier(self):
        sem = pltpu.get_barrier_semaphore()
        targets = [self.core, self.xn, self.yn] + [self.along(r) for r in (1, 2, 3)]
        for target in targets:
            pl.semaphore_signal(
                sem, inc=1, device_id=target, device_id_type=pl.DeviceIdType.MESH
            )
        pl.semaphore_wait(sem, len(targets))

    def plan(self, src, dst, target):
        copy = pltpu.make_async_remote_copy(
            src_ref=src,
            dst_ref=dst,
            send_sem=self.send.at[self.count],
            recv_sem=self.recv.at[self.count],
            device_id=target,
            device_id_type=pl.DeviceIdType.MESH,
        )
        self.count += 1
        self.sent.append(copy)
        return copy

    def copy(self, src, dst, target):
        copy = self.plan(src, dst, target)
        copy.start()
        return copy

    def drain(self):
        for copy in self.sent:
            copy.wait_send()


def cut_of(rows):
    line = rows // 4
    return max(16, (line // 2 + 15) // 16 * 16)


def piece(ref, lead, line, c, part):
    rows, cols = ref.shape[-2], ref.shape[-1]
    height, width, cut = rows // 4, cols // 2, cut_of(rows)
    first, size = {"all": (0, height), "a": (0, cut), "b": (cut, height - cut)}[part]
    at_rows = pl.ds(pl.multiple_of(line * height + first, 16), size)
    at_cols = pl.ds(pl.multiple_of(c * width, 128), width)
    if lead is None:
        return ref.at[at_rows, at_cols]
    return ref.at[lead, at_rows, at_cols]


class Spread:
    def __init__(self, links, ref, lead):
        x, y, c = links.x, links.y, links.c
        own, off_x, off_y, far = 2 * y + x, 2 * y + 1 - x, 2 * (1 - y) + x, 3 - 2 * y - x

        def put(line, part, target):
            block = piece(ref, lead, line, c, part)
            return links.plan(block, block, target)

        self.to_x = put(own, "all", links.xn)
        self.to_y = put(own, "all", links.yn)
        self.far_a = put(off_x, "a", links.yn)
        self.far_b = put(off_y, "b", links.xn)
        self.cores = [
            put(own, "all", links.core),
            put(off_x, "all", links.core),
            put(off_y, "all", links.core),
            put(far, "a", links.core),
            put(far, "b", links.core),
        ]

    def start(self):
        self.to_x.start()
        self.to_y.start()
        self.cores[0].start()

    def relay(self):
        self.to_x.wait_recv()
        self.far_a.start()
        self.cores[1].start()
        self.to_y.wait_recv()
        self.far_b.start()
        self.cores[2].start()

    def last(self):
        self.far_a.wait_recv()
        self.cores[3].start()
        self.far_b.wait_recv()
        self.cores[4].start()

    def end(self):
        for copy in self.cores:
            copy.wait_recv()


class Gather:
    def __init__(self, links, shard, out, slot0, rels):
        line = 2 * links.y + links.x
        self.from_z = [
            links.plan(
                piece(shard, None, line, links.c, "all"),
                piece(out, slot0 + i, line, links.c, "all"),
                links.along(r),
            )
            for i, r in enumerate(rels)
        ]
        self.plane = Spread(links, out, pl.ds(slot0, len(rels)))
        self.steps = [self.arrive, self.plane.relay, self.plane.last, self.plane.end]

    def send(self):
        for copy in self.from_z:
            copy.start()

    def arrive(self):
        for copy in self.from_z:
            copy.wait_recv()
        self.plane.start()

    def step(self):
        if self.steps:
            self.steps.pop(0)()

    def finish(self):
        while self.steps:
            self.step()


def dot_nt(left, right):
    return lax.dot_general(left, right, (((1,), (1,)), ((), ())), preferred_element_type=F32)


def dot_tn(left, right):
    return lax.dot_general(left, right, (((0,), (0,)), ((), ())), preferred_element_type=F32)


def dot_nn(left, right):
    return lax.dot_general(left, right, (((1,), (0,)), ((), ())), preferred_element_type=F32)


def turned(values):
    lane = lax.broadcasted_iota(jnp.int32, values.shape, 1)
    return jnp.where(
        lax.rem(lane, HS) < HS // 2,
        pltpu.roll(values, 128 - HS // 2, 1),
        pltpu.roll(values, HS // 2, 1),
    )


def head_mask(head):
    lane = lax.broadcasted_iota(jnp.int32, (1, 128), 1)
    return jnp.where(lax.div(lane, HS) == head, 1.0, 0.0).astype(BF16)


QB = 256
FORWARD_PLAN = ["o", "", "o", "g", "o", "g", "u", "o", "g", "u", "", "d"]


def attention_kernel(
    len_ref, x_ref, qkv_ref, o_ref, cos_ref, sin_ref, gate_ref, up_ref, down_ref,
    x2, w2, wo, q_ref, k_ref, v_ref, m_all, stat, resid, gate_far, up_far, down_far,
    send, recv, m_ref, bias,
):
    links = Links(send, recv)
    rows = x_ref.shape[0]
    half = lax.rem(links.z, 2)
    mine = pl.ds(pl.multiple_of(half * rows, rows), rows)
    theirs = pl.ds(pl.multiple_of((1 - half) * rows, rows), rows)
    partner = links.along(1)
    length = len_ref[0]
    links.barrier()
    g_qkv = Gather(links, qkv_ref, w2, 1, (2,))
    g_out = Gather(links, o_ref, wo, 1, (2, 1, 3))
    g_gate = Gather(links, gate_ref, gate_far, 0, (2, 1, 3))
    g_up = Gather(links, up_ref, up_far, 0, (2, 1, 3))
    g_down = Gather(links, down_ref, down_far, 0, (2, 1, 3))
    swap_x = links.plan(x_ref, x2.at[mine], partner)
    width = m_ref.shape[1]
    swap_m = [
        links.plan(
            m_ref.at[theirs, pl.ds(p * 128, 128)], m_all.at[:, pl.ds(width + p * 128, 128)], partner
        )
        for p in range(3)
    ]
    g_qkv.send()
    swap_x.start()
    g_out.send()
    g_gate.send()
    g_up.send()
    x2[mine, :] = x_ref[...]
    w2[0] = qkv_ref[...]
    wo[0] = o_ref[...]
    key_at = lax.broadcasted_iota(jnp.int32, (SLOT_LEN, QB), 0)
    bias[...] = jnp.where(key_at < length, 0.0, -1e30)
    stat[...] = jnp.zeros_like(stat)
    g_qkv.finish()
    dim = x_ref.shape[1]
    w_rows = w2.shape[0] * w2.shape[1]
    for at in (mine, theirs):
        if at is theirs:
            swap_x.wait_recv()
        for t, dst in enumerate((q_ref, k_ref, v_ref)):
            w = w2[:, :, t * dim : (t + 1) * dim].reshape(w_rows, dim)
            raw = dot_nt(x2[at, :], w)
            for p in range(3):
                part = raw[:, p * 128 : (p + 1) * 128]
                if t < 2:
                    part = part * cos_ref[at, :] + turned(part) * sin_ref[at, :]
                if t == 0:
                    part = part.astype(BF16) * 0.125
                dst[at, p * 128 : (p + 1) * 128] = part.astype(BF16)

    plan = FORWARD_PLAN
    named = {"o": g_out, "g": g_gate, "u": g_up, "d": g_down}
    plan = [[named[name].steps.pop(0) for name in names] for names in plan]

    def pair_step(p, carry):
        lanes = pl.ds(pl.multiple_of(p * 128, 128), 128)
        k_pair, v_turn = k_ref[:, lanes], v_ref[:, lanes].T
        keys = [k_pair * head_mask(h) for h in range(2)]
        for qb in range(SLOT_LEN // QB):
            at = pl.ds(qb * QB, QB)
            span = (qb + 1) * QB
            query = q_ref[at, lanes]
            query_at = qb * QB + lax.broadcasted_iota(jnp.int32, (1, QB), 1)
            outs = []
            for h in range(2):
                scores = dot_nt(keys[h][:span], query) + bias[:span, :]
                causal = lax.broadcasted_iota(jnp.int32, (QB, QB), 0) <= (
                    lax.broadcasted_iota(jnp.int32, (QB, QB), 1)
                )
                diag = jnp.where(causal, scores[span - QB :], -1e30)
                if qb:
                    scores = jnp.concatenate([scores[: span - QB], diag], axis=0)
                else:
                    scores = diag
                top = jnp.max(scores, axis=0, keepdims=True)
                probs = jnp.exp(scores - top)
                total = jnp.sum(probs, axis=0, keepdims=True)
                out = dot_nn(v_turn[h * HS : (h + 1) * HS, :span], probs.astype(BF16))
                outs.append(out * jnp.where(query_at < length, 1.0 / total, 0.0))
                stat[pl.ds(2 * p + h, 1), at] = top + jnp.log(total)
            m_ref[at, lanes] = jnp.concatenate(outs, axis=0).T.astype(BF16)
            for i in range(3):
                steps = list(plan[4 * i + qb])
                if qb == 3:
                    steps.append(swap_m[i].start)
                    if i == 0:
                        steps.append(g_down.send)
                if steps:

                    @pl.when(p == i)
                    def _(steps=steps):
                        for step in steps:
                            step()

        return carry

    lax.fori_loop(0, 3, pair_step, 0)
    m_all[:, :width] = m_ref[mine, :]
    wo_rows = wo.shape[1]
    g_out.finish()
    g_up.step()
    first = dot_nn(m_all[:, :width], wo[0:2].reshape(2 * wo_rows, dim))
    g_down.step()
    for copy in swap_m:
        copy.wait_recv()
    g_gate.step()
    second = dot_nn(m_all[:, width:], wo[2:4].reshape(2 * wo_rows, dim))
    resid[...] = x_ref[...].astype(F32) + first + second
    gathers = [g_gate, g_up, g_down]
    while any(g.steps for g in gathers):
        for g in gathers:
            g.step()
    links.drain()


def attention(length, layer_in, qkv_own, out_proj, cosines, sines, gate_proj, up_proj, down_proj):
    rows, dim = layer_in.shape
    width = out_proj.shape[0]
    vmem, hbm = pl.BlockSpec(memory_space=pltpu.VMEM), pl.BlockSpec(memory_space=pl.ANY)
    shape = jax.ShapeDtypeStruct
    copies = 64
    heads = shape((SLOT_LEN, 2 * width), BF16)
    return pl.pallas_call(
        attention_kernel,
        out_shape=[
            shape((SLOT_LEN, dim), BF16),
            shape((2,) + qkv_own.shape, BF16),
            shape((4,) + out_proj.shape, BF16),
            heads,
            heads,
            heads,
            shape((rows, 4 * width), BF16),
            shape((8, SLOT_LEN), F32),
            shape((rows, dim), F32),
            shape((3,) + gate_proj.shape, BF16),
            shape((3,) + up_proj.shape, BF16),
            shape((3,) + down_proj.shape, BF16),
        ],
        in_specs=[pl.BlockSpec(memory_space=pltpu.SMEM)] + [vmem] * 5 + [hbm] * 3,
        out_specs=[vmem] * 9 + [hbm] * 3,
        scratch_shapes=[
            pltpu.SemaphoreType.DMA((copies,)),
            pltpu.SemaphoreType.DMA((copies,)),
            pltpu.VMEM((SLOT_LEN, 2 * width), BF16),
            pltpu.VMEM((SLOT_LEN, QB), F32),
        ],
        compiler_params=pltpu.CompilerParams(
            collective_id=0, has_side_effects=True, vmem_limit_bytes=VMEM_LIMIT
        ),
        name="attention_forward",
    )(length, layer_in, qkv_own, out_proj, cosines, sines, gate_proj, up_proj, down_proj)


class Steps:
    def step(self):
        if self.steps:
            self.steps.pop(0)()


class Reduction(Steps):
    def __init__(self, links, rel, parts, out, acc, x_one, y_one, x_two, y_two, from_z):
        self.links, self.parts, self.out, self.acc = links, parts, out, acc
        self.x_one, self.y_one, self.x_two, self.y_two = x_one, y_one, x_two, y_two
        self.from_z = from_z
        x, y, c = links.x, links.y, links.c
        height, width = acc.shape[3], acc.shape[4]
        cut = cut_of(4 * height)
        self.a, self.b = pl.ds(0, cut), pl.ds(cut, height - cut)
        self.mine = pl.ds(pl.multiple_of(c * width, 128), width)
        other = pl.ds(pl.multiple_of((1 - c) * width, 128), width)
        self.n = len(rel)
        self.core = [
            links.plan(parts[s].at[:, :, :, other], acc.at[s], links.core) for s in range(self.n)
        ]
        self.to_x = links.plan(acc.at[:, :, 1 - x, self.a], x_one, links.xn)
        self.to_y = links.plan(acc.at[:, 1 - y, :, self.b], y_one, links.yn)
        self.to_y2 = links.plan(acc.at[:, 1 - y, x, self.a], y_two, links.yn)
        self.to_x2 = links.plan(acc.at[:, y, 1 - x, self.b], x_two, links.xn)
        self.to_z = [
            links.plan(acc.at[s, y, x], from_z.at[s - 1], links.along(rel[s]))
            for s in range(1, self.n)
        ]
        self.plane = Spread(links, out, None)
        self.total = piece(out, None, 2 * y + x, c, "all")
        self.steps = [
            self.start, self.one, self.two, self.three, self.four,
            self.plane.relay, self.plane.last, self.plane.end,
        ]

    def start(self):
        for copy in self.core:
            copy.start()

    def one(self):
        acc = self.acc
        for s in range(self.n):
            self.core[s].wait_recv()
            acc[s] = acc[s] + self.parts[s][:, :, :, self.mine]
        self.to_x.start()
        self.to_y.start()

    def two(self):
        acc, x, y = self.acc, self.links.x, self.links.y
        self.to_x.wait_recv()
        for s in range(self.n):
            for row in range(2):
                acc[s, row, x, self.a] = acc[s, row, x, self.a] + self.x_one[s, row]
        self.to_y2.start()
        self.to_y.wait_recv()
        for s in range(self.n):
            for col in range(2):
                acc[s, y, col, self.b] = acc[s, y, col, self.b] + self.y_one[s, col]
        self.to_x2.start()

    def three(self):
        acc, x, y = self.acc, self.links.x, self.links.y
        self.to_y2.wait_recv()
        self.to_x2.wait_recv()
        for s in list(range(1, self.n)) + [0]:
            acc[s, y, x, self.a] = acc[s, y, x, self.a] + self.y_two[s]
            acc[s, y, x, self.b] = acc[s, y, x, self.b] + self.x_two[s]
            if s:
                self.to_z[s - 1].start()

    def four(self):
        for copy in self.to_z:
            copy.wait_recv()
        total = self.acc[0, self.links.y, self.links.x].astype(F32)
        for s in range(self.n - 1):
            total = total + self.from_z[s].astype(F32)
        self.total[...] = total.astype(BF16)
        self.plane.start()


class GainSum(Steps):
    def __init__(self, links, gains, out, from_core, from_x, from_y, from_z, acc):
        self.gains, self.out, self.from_z, self.acc = gains, out, from_z, acc
        self.hops = [
            (from_core, links.plan(acc.at[0], from_core, links.core)),
            (from_x, links.plan(acc.at[1], from_x, links.xn)),
            (from_y, links.plan(acc.at[2], from_y, links.yn)),
        ]
        self.to_z = [links.plan(acc.at[3], from_z.at[r - 1], links.along(r)) for r in (1, 2, 3)]
        self.steps = [self.start] + [functools.partial(self.hop, i) for i in range(3)] + [self.end]

    def start(self):
        self.acc[0] = self.gains[...]
        self.hops[0][1].start()

    def hop(self, i):
        self.hops[i][1].wait_recv()
        self.acc[i + 1] = self.acc[i] + self.hops[i][0][...]
        for copy in [self.hops[i + 1][1]] if i < 2 else self.to_z:
            copy.start()

    def end(self):
        for copy in self.to_z:
            copy.wait_recv()
        self.out[...] = self.acc[3] + self.from_z[0] + self.from_z[1] + self.from_z[2]


def backward_kernel(
    len_ref, d_ref, x2, w2, q_ref, k_ref, v_ref, stat, cos_ref, sin_ref, resid, gains, out_part,
    *refs,
):
    down_parts, gate_parts, up_parts = refs[0:4], refs[4:8], refs[8:12]
    in_grad, down_out, gate_out, up_out, out_out, qkv_out, gains_out = refs[12:19]
    send, recv, d2, bias, d_raw, dk_acc, dv_acc, qkv_part, in_send, in_recv = refs[19:29]
    gain_refs, rest = refs[29:34], refs[34:]
    links = Links(send, recv)
    rows, dim = resid.shape
    width = d2.shape[1]
    half = lax.rem(links.z, 2)
    mine = pl.ds(pl.multiple_of(half * rows, rows), rows)
    theirs = pl.ds(pl.multiple_of((1 - half) * rows, rows), rows)
    partner = links.along(1)
    length = len_ref[0]
    links.barrier()
    swaps = [
        links.plan(
            d_ref.at[:, pl.ds(width + p * 128, 128)], d2.at[mine, pl.ds(p * 128, 128)], partner
        )
        for p in range(3)
    ]
    swap_in = links.plan(in_send, in_recv, partner)
    qkv_parts = [qkv_part.at[s] for s in range(2)]
    out_parts = [out_part.at[s] for s in range(4)]
    down, gate, up, out = (
        Reduction(links, ALL, parts, result, *rest[6 * i : 6 * i + 6])
        for i, (parts, result) in enumerate(
            [(down_parts, down_out), (gate_parts, gate_out), (up_parts, up_out),
             (out_parts, out_out)]
        )
    )
    qkv = Reduction(links, (0, 2), qkv_parts, qkv_out, *rest[24:30])
    gain = GainSum(links, gains, gains_out, *gain_refs)
    for copy in swaps:
        copy.start()
    for job in (down, gate, up, out, gain):
        job.step()
    d2[mine, :] = d_ref[:, :width]
    key_at = lax.broadcasted_iota(jnp.int32, (SLOT_LEN, QB), 0)
    bias[...] = jnp.where(key_at < length, 0.0, -1e30)
    down.step()

    plan = [
        [], [gate], [gain], [down], [up], [gain],
        [gate], [down], [gain], [up, out], [gate], [gain],
    ]
    plan = [[job.steps.pop(0) for job in jobs] for jobs in plan]

    def pair_step(p, carry):
        lanes = pl.ds(pl.multiple_of(p * 128, 128), 128)
        for i in range(3):

            @pl.when(p == i)
            def _(i=i):
                swaps[i].wait_recv()

        k_pair, v_pair = k_ref[:, lanes], v_ref[:, lanes]
        k_turn = k_pair.T
        keys = [k_pair * head_mask(h) for h in range(2)]
        values = [v_pair * head_mask(h) for h in range(2)]
        for turn, qb in enumerate(reversed(range(SLOT_LEN // QB))):
            at = pl.ds(qb * QB, QB)
            span = (qb + 1) * QB
            query = q_ref[at, lanes]
            query_at = qb * QB + lax.broadcasted_iota(jnp.int32, (QB, 128), 0)
            present = jnp.where(query_at < length, 1.0, 0.0).astype(BF16)
            grad = d2[at, lanes] * present
            d_scores, probs_low, d_query = [], [], []
            for h in range(2):
                scores = dot_nt(keys[h][:span], query) + bias[:span, :]
                causal = lax.broadcasted_iota(jnp.int32, (QB, QB), 0) <= (
                    lax.broadcasted_iota(jnp.int32, (QB, QB), 1)
                )
                diag = jnp.where(causal, scores[span - QB :], -1e30)
                if qb:
                    scores = jnp.concatenate([scores[: span - QB], diag], axis=0)
                else:
                    scores = diag
                probs = jnp.exp(scores - stat[pl.ds(2 * p + h, 1), at])
                d_probs = dot_nt(values[h][:span], grad)
                total = jnp.sum(d_probs * probs, axis=0, keepdims=True)
                d_score = (probs * (d_probs - total)).astype(BF16)
                d_query.append(dot_nn(k_turn[h * HS : (h + 1) * HS, :span], d_score))
                d_scores.append(d_score)
                probs_low.append(probs.astype(BF16))
            d_key = dot_nn(
                jnp.concatenate(d_scores, axis=1),
                jnp.concatenate([query * head_mask(h) for h in range(2)], axis=0),
            )
            d_value = dot_nn(
                jnp.concatenate(probs_low, axis=1),
                jnp.concatenate([grad * head_mask(h) for h in range(2)], axis=0),
            )
            if turn == 0:
                dk_acc[...] = d_key
                dv_acc[...] = d_value
            else:
                dk_acc[:span, :] = dk_acc[:span, :] + d_key
                dv_acc[:span, :] = dv_acc[:span, :] + d_value
            part = jnp.concatenate(d_query, axis=0).T * 0.125
            part = part * cos_ref[at, :] - turned(part) * sin_ref[at, :]
            d_raw[at, lanes] = part.astype(BF16)
            for i in range(3):
                steps = plan[4 * i + turn]
                if steps:

                    @pl.when(p == i)
                    def _(steps=steps):
                        for step in steps:
                            step()

        part = dk_acc[...]
        part = part * cos_ref[...] - turned(part) * sin_ref[...]
        d_raw[:, pl.ds(pl.multiple_of(width + p * 128, 128), 128)] = part.astype(BF16)
        d_raw[:, pl.ds(pl.multiple_of(2 * width + p * 128, 128), 128)] = dv_acc[...].astype(BF16)
        return carry

    lax.fori_loop(0, 3, pair_step, 0)
    for t in range(3):
        grads = dot_nn(d_raw[:, t * width : (t + 1) * width].T, x2[...]).astype(BF16)
        qkv_part[:, :, :, :, t * dim : (t + 1) * dim] = grads.reshape(qkv_part.shape[:4] + (dim,))
    qkv.step()
    weights = [w2[:, :, t * dim : (t + 1) * dim].reshape(width, dim) for t in range(3)]

    def project(at):
        return sum(
            dot_nn(d_raw[at, t * width : (t + 1) * width], weights[t]) for t in range(3)
        )

    in_send[...] = project(theirs).astype(BF16)
    swap_in.start()
    qkv.step()
    jobs = [down, gate, up, out, qkv, gain]
    own = resid[...] + project(mine)
    for job in jobs:
        job.step()
    swap_in.wait_recv()
    in_grad[...] = (own + in_recv[...].astype(F32)).astype(BF16)
    while any(job.steps for job in jobs):
        for job in jobs:
            job.step()
    links.drain()


def backward(
    length, d_all, slot_in, qkv_all, queries, keys, values, stats, cosines, sines, d_resid, gains,
    out_part, down_parts, gate_parts, up_parts,
):
    rows, dim = d_resid.shape
    width = queries.shape[1]
    shape = jax.ShapeDtypeStruct
    parts = [down_parts, gate_parts, up_parts, [out_part[s] for s in range(4)]]
    shards = [(4,) + p[0].shape for p in parts]
    shards.append((2, 2, 2, width // 8, qkv_all.shape[2]))
    scratch = []
    copies = 4 + 6
    for n, _, _, height, cols in shards:
        half, cut = cols // 2, cut_of(4 * height)
        copies += 2 * n + 3 + 9
        scratch += [
            pltpu.VMEM((n, 2, 2, height, half), BF16),
            pltpu.VMEM((n, 2, cut, half), BF16),
            pltpu.VMEM((n, 2, height - cut, half), BF16),
            pltpu.VMEM((n, height - cut, half), BF16),
            pltpu.VMEM((n, cut, half), BF16),
            pltpu.VMEM((n - 1, height, half), BF16),
        ]
    vmem = pl.BlockSpec(memory_space=pltpu.VMEM)
    return pl.pallas_call(
        backward_kernel,
        out_shape=[shape((rows, dim), BF16)]
        + [shape((4 * s[3], s[4]), BF16) for s in shards]
        + [shape(gains.shape, F32)],
        in_specs=[pl.BlockSpec(memory_space=pltpu.SMEM)] + [vmem] * 24,
        out_specs=[vmem] * 7,
        scratch_shapes=[
            pltpu.SemaphoreType.DMA((copies,)),
            pltpu.SemaphoreType.DMA((copies,)),
            pltpu.VMEM((SLOT_LEN, width), BF16),
            pltpu.VMEM((SLOT_LEN, QB), F32),
            pltpu.VMEM((SLOT_LEN, 3 * width), BF16),
            pltpu.VMEM((SLOT_LEN, 128), F32),
            pltpu.VMEM((SLOT_LEN, 128), F32),
            pltpu.VMEM(shards[4], BF16),
            pltpu.VMEM((rows, dim), BF16),
            pltpu.VMEM((rows, dim), BF16),
            pltpu.VMEM(gains.shape, F32),
            pltpu.VMEM(gains.shape, F32),
            pltpu.VMEM(gains.shape, F32),
            pltpu.VMEM((3,) + gains.shape, F32),
            pltpu.VMEM((4,) + gains.shape, F32),
        ]
        + scratch,
        compiler_params=pltpu.CompilerParams(
            collective_id=1, has_side_effects=True, vmem_limit_bytes=VMEM_LIMIT
        ),
        name="attention_backward",
    )(
        length, d_all, slot_in, qkv_all, queries, keys, values, stats, cosines, sines, d_resid,
        gains, out_part, *down_parts, *gate_parts, *up_parts,
    )


ALL = (0, 2, 1, 3)


def quarters(part):
    return part.astype(BF16).reshape(2, 2, part.shape[0] // 4, part.shape[1])


def body(
    dp_size,
    layer_in,
    query_proj,
    key_proj,
    value_proj,
    out_proj,
    gate_proj,
    up_proj,
    down_proj,
    first_gain,
    second_gain,
    seq_lengths,
    cotangent,
):
    z = lax.axis_index("mp")
    valid_len = lax.dynamic_index_in_dim(seq_lengths, lax.div(z, 2), keepdims=False)
    width = query_proj.shape[1]

    qkv_own = jnp.concatenate([query_proj.T, key_proj.T, value_proj.T], axis=1)
    cosines, sines = rotary_tables(SLOT_LEN)
    cos_wide = jnp.tile(cosines[:, 0, :], (1, 4))
    sin_wide = jnp.tile(jnp.concatenate([-sines[:, 0, :], sines[:, 0, :]], axis=1), (1, 2))
    (
        slot_in, qkv_all, out_all, rot_queries, rot_keys, values_low, mixed_all, stats,
        resid_one, gate_far, up_far, down_far,
    ) = attention(
        valid_len[None], layer_in, qkv_own, out_proj, cos_wide, sin_wide,
        gate_proj, up_proj, down_proj,
    )
    out_all = out_all.reshape(4 * width, -1)
    normed, first_pull = jax.vjp(rms_norm, resid_one, first_gain)
    normed_low = normed.astype(BF16)

    gates = [gate_proj] + [gate_far[i] for i in range(3)]
    ups = [up_proj] + [up_far[i] for i in range(3)]
    downs = [down_proj] + [down_far[i] for i in range(3)]
    gate_pre = [forward(normed_low, w) for w in gates]
    up_pre = [forward(normed_low, w) for w in ups]
    hidden = [swiglu(g, u).astype(BF16) for g, u in zip(gate_pre, up_pre)]
    ffn_branch = sum(forward(h, w) for h, w in zip(hidden, downs))
    resid_two = normed + ffn_branch
    result, second_pull = jax.vjp(rms_norm, resid_two, second_gain)
    layer_out = result.astype(BF16)
    d_resid_two, second_part = second_pull(cotangent.astype(F32))
    ffn_out = d_resid_two.astype(BF16)
    d_normed = d_resid_two
    down_parts, gate_parts, up_parts = [], [], []
    for r in range(4):
        down_parts.append(quarters(cross(hidden[r], ffn_out)))
        d_hidden = against(ffn_out, downs[r])
        unused, glu_pull = jax.vjp(swiglu, gate_pre[r], up_pre[r])
        d_gate, d_up = (d.astype(BF16) for d in glu_pull(d_hidden))
        gate_parts.append(quarters(cross(normed_low, d_gate)))
        up_parts.append(quarters(cross(normed_low, d_up)))
        d_normed = d_normed + against(d_gate, gates[r]) + against(d_up, ups[r])
    d_resid_one, first_part = first_pull(d_normed)
    attn_out = d_resid_one.astype(BF16)
    out_part = cross(mixed_all, attn_out).astype(BF16).reshape(4, 2, 2, width // 4, -1)
    d_all = against(attn_out, out_all).astype(BF16)
    gains = jnp.concatenate(
        [first_part[None], second_part[None], jnp.zeros((6, first_part.shape[0]), F32)], axis=0
    )
    input_grad, down_grad, gate_grad, up_grad, out_grad, qkv_grad, gains = backward(
        valid_len[None], d_all, slot_in, qkv_all, rot_queries, rot_keys, values_low, stats,
        cos_wide, sin_wide, d_resid_one, gains, out_part, down_parts, gate_parts, up_parts,
    )
    dim = layer_in.shape[1]
    down_grad, gate_grad, up_grad, out_grad, qkv_grad = (
        g.astype(F32) for g in (down_grad, gate_grad, up_grad, out_grad, qkv_grad)
    )
    if dp_size > BLOCK:
        groups = [list(range(i, dp_size, BLOCK)) for i in range(BLOCK)]
        down_grad, gate_grad, up_grad, out_grad, qkv_grad, gains = lax.psum(
            (down_grad, gate_grad, up_grad, out_grad, qkv_grad, gains),
            "dp",
            axis_index_groups=groups,
        )
    qkv_grad = [qkv_grad[:, t * dim : (t + 1) * dim] for t in range(3)]
    return (
        layer_out,
        input_grad,
        qkv_grad[0].T,
        qkv_grad[1].T,
        qkv_grad[2].T,
        out_grad,
        gate_grad,
        up_grad,
        down_grad,
        gains[0],
        gains[1],
    )


def solution(mesh):
    rows = P(("dp", "mp"), None)
    cols, first = P(None, "mp"), P("mp", None)
    return jax.shard_map(
        functools.partial(body, mesh.shape["dp"]),
        mesh=mesh,
        in_specs=(rows, cols, cols, cols, first, cols, cols, first, P(), P(), P("dp"), rows),
        out_specs=(rows, rows, cols, cols, cols, first, cols, cols, first, P(), P()),
        check_vma=False,
    )
```

```python
import functools

import jax
import jax.numpy as jnp
from jax import lax
from jax.experimental import pallas as pl
from jax.experimental.pallas import tpu as pltpu
from jax.sharding import PartitionSpec as P

HS = 64
SLOT_LEN = 1024
BLOCK = 8
VMEM_LIMIT = 63 << 20
F32 = jnp.float32
BF16 = jnp.bfloat16


def rms_norm(resid, gain):
    return resid * lax.rsqrt(jnp.mean(resid * resid, axis=-1, keepdims=True) + 1e-05) * gain


def swiglu(gate_pre, up_pre):
    return jax.nn.silu(gate_pre) * up_pre


def rotary_tables(rows):
    half = HS // 2
    positions = (jnp.arange(rows, dtype=jnp.int32) % SLOT_LEN).astype(F32)
    freqs = 10000.0 ** (-jnp.arange(half, dtype=F32) * 2.0 / HS)
    angles = positions[:, None] * freqs[None, :]
    return (jnp.cos(angles)[:, None, :], jnp.sin(angles)[:, None, :])


def cross(left, right):
    return lax.dot_general(left, right, (((0,), (0,)), ((), ())), preferred_element_type=F32)


def against(left, right):
    return lax.dot_general(left, right, (((1,), (1,)), ((), ())), preferred_element_type=F32)


def forward(left, right):
    return jnp.dot(left, right, preferred_element_type=F32)


class Links:
    def __init__(self, send, recv):
        self.send, self.recv = send, recv
        self.count = 0
        self.sent = []
        self.d = lax.axis_index("dp")
        self.z = lax.axis_index("mp")
        self.core = (self.flip(1), self.z)
        self.xn = (self.flip(2), self.z)
        self.yn = (self.flip(4), self.z)
        self.c = lax.rem(self.d, 2)
        self.x = lax.rem(lax.div(self.d, 2), 2)
        self.y = lax.rem(lax.div(self.d, 4), 2)

    def flip(self, step):
        bit = lax.rem(lax.div(self.d, step), 2)
        return self.d + step * (1 - 2 * bit)

    def along(self, r):
        low, high = lax.rem(self.z, 2), lax.div(self.z, 2)
        low = 1 - low if r % 2 else low
        high = 1 - high if r // 2 else high
        return (self.d, 2 * high + low)

    def barrier(self):
        sem = pltpu.get_barrier_semaphore()
        targets = [self.core, self.xn, self.yn] + [self.along(r) for r in (1, 2, 3)]
        for target in targets:
            pl.semaphore_signal(
                sem, inc=1, device_id=target, device_id_type=pl.DeviceIdType.MESH
            )
        pl.semaphore_wait(sem, len(targets))

    def plan(self, src, dst, target):
        copy = pltpu.make_async_remote_copy(
            src_ref=src,
            dst_ref=dst,
            send_sem=self.send.at[self.count],
            recv_sem=self.recv.at[self.count],
            device_id=target,
            device_id_type=pl.DeviceIdType.MESH,
        )
        self.count += 1
        self.sent.append(copy)
        return copy

    def copy(self, src, dst, target):
        copy = self.plan(src, dst, target)
        copy.start()
        return copy

    def drain(self):
        for copy in self.sent:
            copy.wait_send()


def cut_of(rows):
    line = rows // 4
    return max(16, (line // 2 + 15) // 16 * 16)


def piece(ref, lead, line, c, part):
    rows, cols = ref.shape[-2], ref.shape[-1]
    height, width, cut = rows // 4, cols // 2, cut_of(rows)
    first, size = {"all": (0, height), "a": (0, cut), "b": (cut, height - cut)}[part]
    at_rows = pl.ds(pl.multiple_of(line * height + first, 16), size)
    at_cols = pl.ds(pl.multiple_of(c * width, 128), width)
    if lead is None:
        return ref.at[at_rows, at_cols]
    return ref.at[lead, at_rows, at_cols]


class Spread:
    def __init__(self, links, ref, lead):
        x, y, c = links.x, links.y, links.c
        own, off_x, off_y, far = 2 * y + x, 2 * y + 1 - x, 2 * (1 - y) + x, 3 - 2 * y - x

        def put(line, part, target):
            block = piece(ref, lead, line, c, part)
            return links.plan(block, block, target)

        self.to_x = put(own, "all", links.xn)
        self.to_y = put(own, "all", links.yn)
        self.far_a = put(off_x, "a", links.yn)
        self.far_b = put(off_y, "b", links.xn)
        self.cores = [
            put(own, "all", links.core),
            put(off_x, "all", links.core),
            put(off_y, "all", links.core),
            put(far, "a", links.core),
            put(far, "b", links.core),
        ]

    def start(self):
        self.to_x.start()
        self.to_y.start()
        self.cores[0].start()

    def relay(self):
        self.to_x.wait_recv()
        self.far_a.start()
        self.cores[1].start()
        self.to_y.wait_recv()
        self.far_b.start()
        self.cores[2].start()

    def last(self):
        self.far_a.wait_recv()
        self.cores[3].start()
        self.far_b.wait_recv()
        self.cores[4].start()

    def end(self):
        for copy in self.cores:
            copy.wait_recv()


class Gather:
    def __init__(self, links, shard, out, slot0, rels):
        line = 2 * links.y + links.x
        self.from_z = [
            links.plan(
                piece(shard, None, line, links.c, "all"),
                piece(out, slot0 + i, line, links.c, "all"),
                links.along(r),
            )
            for i, r in enumerate(rels)
        ]
        self.plane = Spread(links, out, pl.ds(slot0, len(rels)))
        self.steps = [self.arrive, self.plane.relay, self.plane.last, self.plane.end]

    def send(self):
        for copy in self.from_z:
            copy.start()

    def arrive(self):
        for copy in self.from_z:
            copy.wait_recv()
        self.plane.start()

    def step(self):
        if self.steps:
            self.steps.pop(0)()

    def finish(self):
        while self.steps:
            self.step()


def dot_nt(left, right):
    return lax.dot_general(left, right, (((1,), (1,)), ((), ())), preferred_element_type=F32)


def dot_tn(left, right):
    return lax.dot_general(left, right, (((0,), (0,)), ((), ())), preferred_element_type=F32)


def dot_nn(left, right):
    return lax.dot_general(left, right, (((1,), (0,)), ((), ())), preferred_element_type=F32)


def turned(values):
    lane = lax.broadcasted_iota(jnp.int32, values.shape, 1)
    return jnp.where(
        lax.rem(lane, HS) < HS // 2,
        pltpu.roll(values, 128 - HS // 2, 1),
        pltpu.roll(values, HS // 2, 1),
    )


def head_mask(head):
    lane = lax.broadcasted_iota(jnp.int32, (1, 128), 1)
    return jnp.where(lax.div(lane, HS) == head, 1.0, 0.0).astype(BF16)


QB = 256
FORWARD_PLAN = ["o", "", "o", "g", "o", "g", "u", "o", "g", "u", "", "d"]


def attention_kernel(
    len_ref, x_ref, qkv_ref, o_ref, cos_ref, sin_ref, gate_ref, up_ref, down_ref,
    x2, w2, wo, q_ref, k_ref, v_ref, m_all, stat, resid, gate_far, up_far, down_far,
    send, recv, m_ref, bias,
):
    links = Links(send, recv)
    rows = x_ref.shape[0]
    half = lax.rem(links.z, 2)
    mine = pl.ds(pl.multiple_of(half * rows, rows), rows)
    theirs = pl.ds(pl.multiple_of((1 - half) * rows, rows), rows)
    partner = links.along(1)
    length = len_ref[0]
    links.barrier()
    g_qkv = Gather(links, qkv_ref, w2, 1, (2,))
    g_out = Gather(links, o_ref, wo, 1, (2, 1, 3))
    g_gate = Gather(links, gate_ref, gate_far, 0, (2, 1, 3))
    g_up = Gather(links, up_ref, up_far, 0, (2, 1, 3))
    g_down = Gather(links, down_ref, down_far, 0, (2, 1, 3))
    swap_x = links.plan(x_ref, x2.at[mine], partner)
    width = m_ref.shape[1]
    swap_m = [
        links.plan(
            m_ref.at[theirs, pl.ds(p * 128, 128)], m_all.at[:, pl.ds(width + p * 128, 128)], partner
        )
        for p in range(3)
    ]
    g_qkv.send()
    swap_x.start()
    g_out.send()
    g_gate.send()
    g_up.send()
    x2[mine, :] = x_ref[...]
    w2[0] = qkv_ref[...]
    wo[0] = o_ref[...]
    key_at = lax.broadcasted_iota(jnp.int32, (SLOT_LEN, QB), 0)
    bias[...] = jnp.where(key_at < length, 0.0, -1e30)
    stat[...] = jnp.zeros_like(stat)
    g_qkv.finish()
    dim = x_ref.shape[1]
    w_rows = w2.shape[0] * w2.shape[1]
    for at in (mine, theirs):
        if at is theirs:
            swap_x.wait_recv()
        for t, dst in enumerate((q_ref, k_ref, v_ref)):
            w = w2[:, :, t * dim : (t + 1) * dim].reshape(w_rows, dim)
            raw = dot_nt(x2[at, :], w)
            for p in range(3):
                part = raw[:, p * 128 : (p + 1) * 128]
                if t < 2:
                    part = part * cos_ref[at, :] + turned(part) * sin_ref[at, :]
                if t == 0:
                    part = part.astype(BF16) * 0.125
                dst[at, p * 128 : (p + 1) * 128] = part.astype(BF16)

    plan = FORWARD_PLAN
    named = {"o": g_out, "g": g_gate, "u": g_up, "d": g_down}
    plan = [[named[name].steps.pop(0) for name in names] for names in plan]

    def pair_step(p, carry):
        lanes = pl.ds(pl.multiple_of(p * 128, 128), 128)
        k_pair, v_turn = k_ref[:, lanes], v_ref[:, lanes].T
        keys = [k_pair * head_mask(h) for h in range(2)]
        for qb in range(SLOT_LEN // QB):
            at = pl.ds(qb * QB, QB)
            span = (qb + 1) * QB
            query = q_ref[at, lanes]
            query_at = qb * QB + lax.broadcasted_iota(jnp.int32, (1, QB), 1)
            outs = []
            for h in range(2):
                scores = dot_nt(keys[h][:span], query) + bias[:span, :]
                causal = lax.broadcasted_iota(jnp.int32, (QB, QB), 0) <= (
                    lax.broadcasted_iota(jnp.int32, (QB, QB), 1)
                )
                diag = jnp.where(causal, scores[span - QB :], -1e30)
                if qb:
                    scores = jnp.concatenate([scores[: span - QB], diag], axis=0)
                else:
                    scores = diag
                top = jnp.max(scores, axis=0, keepdims=True)
                probs = jnp.exp(scores - top)
                total = jnp.sum(probs, axis=0, keepdims=True)
                out = dot_nn(v_turn[h * HS : (h + 1) * HS, :span], probs.astype(BF16))
                outs.append(out * jnp.where(query_at < length, 1.0 / total, 0.0))
                stat[pl.ds(2 * p + h, 1), at] = top + jnp.log(total)
            m_ref[at, lanes] = jnp.concatenate(outs, axis=0).T.astype(BF16)
            for i in range(3):
                steps = list(plan[4 * i + qb])
                if qb == 3:
                    steps.append(swap_m[i].start)
                    if i == 0:
                        steps.append(g_down.send)
                if steps:

                    @pl.when(p == i)
                    def _(steps=steps):
                        for step in steps:
                            step()

        return carry

    lax.fori_loop(0, 3, pair_step, 0)
    m_all[:, :width] = m_ref[mine, :]
    wo_rows = wo.shape[1]
    g_out.finish()
    g_up.step()
    first = dot_nn(m_all[:, :width], wo[0:2].reshape(2 * wo_rows, dim))
    g_down.step()
    for copy in swap_m:
        copy.wait_recv()
    g_gate.step()
    second = dot_nn(m_all[:, width:], wo[2:4].reshape(2 * wo_rows, dim))
    resid[...] = x_ref[...].astype(F32) + first + second
    gathers = [g_gate, g_up, g_down]
    while any(g.steps for g in gathers):
        for g in gathers:
            g.step()
    links.drain()


def attention(length, layer_in, qkv_own, out_proj, cosines, sines, gate_proj, up_proj, down_proj):
    rows, dim = layer_in.shape
    width = out_proj.shape[0]
    vmem, hbm = pl.BlockSpec(memory_space=pltpu.VMEM), pl.BlockSpec(memory_space=pl.ANY)
    shape = jax.ShapeDtypeStruct
    copies = 64
    heads = shape((SLOT_LEN, 2 * width), BF16)
    return pl.pallas_call(
        attention_kernel,
        out_shape=[
            shape((SLOT_LEN, dim), BF16),
            shape((2,) + qkv_own.shape, BF16),
            shape((4,) + out_proj.shape, BF16),
            heads,
            heads,
            heads,
            shape((rows, 4 * width), BF16),
            shape((8, SLOT_LEN), F32),
            shape((rows, dim), F32),
            shape((3,) + gate_proj.shape, BF16),
            shape((3,) + up_proj.shape, BF16),
            shape((3,) + down_proj.shape, BF16),
        ],
        in_specs=[pl.BlockSpec(memory_space=pltpu.SMEM)] + [vmem] * 5 + [hbm] * 3,
        out_specs=[vmem] * 9 + [hbm] * 3,
        scratch_shapes=[
            pltpu.SemaphoreType.DMA((copies,)),
            pltpu.SemaphoreType.DMA((copies,)),
            pltpu.VMEM((SLOT_LEN, 2 * width), BF16),
            pltpu.VMEM((SLOT_LEN, QB), F32),
        ],
        compiler_params=pltpu.CompilerParams(
            collective_id=0, has_side_effects=True, vmem_limit_bytes=VMEM_LIMIT
        ),
        name="attention_forward",
    )(length, layer_in, qkv_own, out_proj, cosines, sines, gate_proj, up_proj, down_proj)


class Steps:
    def step(self):
        if self.steps:
            self.steps.pop(0)()


class Reduction(Steps):
    def __init__(self, links, rel, parts, out, acc, x_one, y_one, x_two, y_two, from_z):
        self.links, self.parts, self.out, self.acc = links, parts, out, acc
        self.x_one, self.y_one, self.x_two, self.y_two = x_one, y_one, x_two, y_two
        self.from_z = from_z
        x, y, c = links.x, links.y, links.c
        height, width = acc.shape[3], acc.shape[4]
        cut = cut_of(4 * height)
        self.a, self.b = pl.ds(0, cut), pl.ds(cut, height - cut)
        self.mine = pl.ds(pl.multiple_of(c * width, 128), width)
        other = pl.ds(pl.multiple_of((1 - c) * width, 128), width)
        self.n = len(rel)
        self.core = [
            links.plan(parts[s].at[:, :, :, other], acc.at[s], links.core) for s in range(self.n)
        ]
        self.to_x = links.plan(acc.at[:, :, 1 - x, self.a], x_one, links.xn)
        self.to_y = links.plan(acc.at[:, 1 - y, :, self.b], y_one, links.yn)
        self.to_y2 = links.plan(acc.at[:, 1 - y, x, self.a], y_two, links.yn)
        self.to_x2 = links.plan(acc.at[:, y, 1 - x, self.b], x_two, links.xn)
        self.to_z = [
            links.plan(acc.at[s, y, x], from_z.at[s - 1], links.along(rel[s]))
            for s in range(1, self.n)
        ]
        self.plane = Spread(links, out, None)
        self.total = piece(out, None, 2 * y + x, c, "all")
        self.steps = [
            self.start, self.one, self.two, self.three, self.four,
            self.plane.relay, self.plane.last, self.plane.end,
        ]

    def start(self):
        for copy in self.core:
            copy.start()

    def one(self):
        acc = self.acc
        for s in range(self.n):
            self.core[s].wait_recv()
            acc[s] = acc[s] + self.parts[s][:, :, :, self.mine]
        self.to_x.start()
        self.to_y.start()

    def two(self):
        acc, x, y = self.acc, self.links.x, self.links.y
        self.to_x.wait_recv()
        for s in range(self.n):
            for row in range(2):
                acc[s, row, x, self.a] = acc[s, row, x, self.a] + self.x_one[s, row]
        self.to_y2.start()
        self.to_y.wait_recv()
        for s in range(self.n):
            for col in range(2):
                acc[s, y, col, self.b] = acc[s, y, col, self.b] + self.y_one[s, col]
        self.to_x2.start()

    def three(self):
        acc, x, y = self.acc, self.links.x, self.links.y
        self.to_y2.wait_recv()
        self.to_x2.wait_recv()
        for s in list(range(1, self.n)) + [0]:
            acc[s, y, x, self.a] = acc[s, y, x, self.a] + self.y_two[s]
            acc[s, y, x, self.b] = acc[s, y, x, self.b] + self.x_two[s]
            if s:
                self.to_z[s - 1].start()

    def four(self):
        for copy in self.to_z:
            copy.wait_recv()
        total = self.acc[0, self.links.y, self.links.x].astype(F32)
        for s in range(self.n - 1):
            total = total + self.from_z[s].astype(F32)
        self.total[...] = total.astype(BF16)
        self.plane.start()


class GainSum(Steps):
    def __init__(self, links, gains, out, from_core, from_x, from_y, from_z, acc):
        self.gains, self.out, self.from_z, self.acc = gains, out, from_z, acc
        self.hops = [
            (from_core, links.plan(acc.at[0], from_core, links.core)),
            (from_x, links.plan(acc.at[1], from_x, links.xn)),
            (from_y, links.plan(acc.at[2], from_y, links.yn)),
        ]
        self.to_z = [links.plan(acc.at[3], from_z.at[r - 1], links.along(r)) for r in (1, 2, 3)]
        self.steps = [self.start] + [functools.partial(self.hop, i) for i in range(3)] + [self.end]

    def start(self):
        self.acc[0] = self.gains[...]
        self.hops[0][1].start()

    def hop(self, i):
        self.hops[i][1].wait_recv()
        self.acc[i + 1] = self.acc[i] + self.hops[i][0][...]
        for copy in [self.hops[i + 1][1]] if i < 2 else self.to_z:
            copy.start()

    def end(self):
        for copy in self.to_z:
            copy.wait_recv()
        self.out[...] = self.acc[3] + self.from_z[0] + self.from_z[1] + self.from_z[2]


def backward_kernel(
    len_ref, d_ref, x2, w2, q_ref, k_ref, v_ref, stat, cos_ref, sin_ref, resid, gains, out_part,
    normed, ffn_out, *refs,
):
    hidden, d_gates, d_ups = refs[0:4], refs[4:8], refs[8:12]
    in_grad, down_out, gate_out, up_out, out_out, qkv_out, gains_out = refs[12:19]
    send, recv, d2, bias, d_raw, dk_acc, dv_acc, qkv_part, in_send, in_recv = refs[19:29]
    down_part, gate_part, up_part = refs[29:32]
    gain_refs, rest = refs[32:37], refs[37:]
    links = Links(send, recv)
    rows, dim = resid.shape
    width = d2.shape[1]
    half = lax.rem(links.z, 2)
    mine = pl.ds(pl.multiple_of(half * rows, rows), rows)
    theirs = pl.ds(pl.multiple_of((1 - half) * rows, rows), rows)
    partner = links.along(1)
    length = len_ref[0]
    links.barrier()
    swaps = [
        links.plan(
            d_ref.at[:, pl.ds(width + p * 128, 128)], d2.at[mine, pl.ds(p * 128, 128)], partner
        )
        for p in range(3)
    ]
    swap_in = links.plan(in_send, in_recv, partner)
    qkv_parts = [qkv_part.at[s] for s in range(2)]
    down_parts, gate_parts, up_parts, out_parts = (
        [part.at[s] for s in range(4)] for part in (down_part, gate_part, up_part, out_part)
    )
    down, gate, up, out = (
        Reduction(links, ALL, parts, result, *rest[6 * i : 6 * i + 6])
        for i, (parts, result) in enumerate(
            [(down_parts, down_out), (gate_parts, gate_out), (up_parts, up_out),
             (out_parts, out_out)]
        )
    )
    qkv = Reduction(links, (0, 2), qkv_parts, qkv_out, *rest[24:30])
    gain = GainSum(links, gains, gains_out, *gain_refs)
    for copy in swaps:
        copy.start()

    def produce(job, part, left, right):
        for s in range(4):
            part[s] = dot_nn(left(s), right(s)).astype(BF16).reshape(part.shape[1:])
            job.core[s].start()
        job.steps.pop(0)

    turned_rows = normed[...].T
    produce(down, down_part, lambda s: hidden[s][...].T, lambda s: ffn_out[...])
    for job in (out, gain):
        job.step()
    produce(gate, gate_part, lambda s: turned_rows, lambda s: d_gates[s][...])
    down.step()
    produce(up, up_part, lambda s: turned_rows, lambda s: d_ups[s][...])
    gate.step()
    d2[mine, :] = d_ref[:, :width]
    key_at = lax.broadcasted_iota(jnp.int32, (SLOT_LEN, QB), 0)
    bias[...] = jnp.where(key_at < length, 0.0, -1e30)

    plan = [
        [gain], [down], [up], [gain], [gate], [out],
        [gain], [down], [up], [gain], [gate], [out],
    ]
    plan = [[job.steps.pop(0) for job in jobs] for jobs in plan]

    def pair_step(p, carry):
        lanes = pl.ds(pl.multiple_of(p * 128, 128), 128)
        for i in range(3):

            @pl.when(p == i)
            def _(i=i):
                swaps[i].wait_recv()

        k_pair, v_pair = k_ref[:, lanes], v_ref[:, lanes]
        k_turn = k_pair.T
        keys = [k_pair * head_mask(h) for h in range(2)]
        values = [v_pair * head_mask(h) for h in range(2)]
        for turn, qb in enumerate(reversed(range(SLOT_LEN // QB))):
            at = pl.ds(qb * QB, QB)
            span = (qb + 1) * QB
            query = q_ref[at, lanes]
            query_at = qb * QB + lax.broadcasted_iota(jnp.int32, (QB, 128), 0)
            present = jnp.where(query_at < length, 1.0, 0.0).astype(BF16)
            grad = d2[at, lanes] * present
            d_scores, probs_low, d_query = [], [], []
            for h in range(2):
                scores = dot_nt(keys[h][:span], query) + bias[:span, :]
                causal = lax.broadcasted_iota(jnp.int32, (QB, QB), 0) <= (
                    lax.broadcasted_iota(jnp.int32, (QB, QB), 1)
                )
                diag = jnp.where(causal, scores[span - QB :], -1e30)
                if qb:
                    scores = jnp.concatenate([scores[: span - QB], diag], axis=0)
                else:
                    scores = diag
                probs = jnp.exp(scores - stat[pl.ds(2 * p + h, 1), at])
                d_probs = dot_nt(values[h][:span], grad)
                total = jnp.sum(d_probs * probs, axis=0, keepdims=True)
                d_score = (probs * (d_probs - total)).astype(BF16)
                d_query.append(dot_nn(k_turn[h * HS : (h + 1) * HS, :span], d_score))
                d_scores.append(d_score)
                probs_low.append(probs.astype(BF16))
            d_key = dot_nn(
                jnp.concatenate(d_scores, axis=1),
                jnp.concatenate([query * head_mask(h) for h in range(2)], axis=0),
            )
            d_value = dot_nn(
                jnp.concatenate(probs_low, axis=1),
                jnp.concatenate([grad * head_mask(h) for h in range(2)], axis=0),
            )
            if turn == 0:
                dk_acc[...] = d_key
                dv_acc[...] = d_value
            else:
                dk_acc[:span, :] = dk_acc[:span, :] + d_key
                dv_acc[:span, :] = dv_acc[:span, :] + d_value
            part = jnp.concatenate(d_query, axis=0).T * 0.125
            part = part * cos_ref[at, :] - turned(part) * sin_ref[at, :]
            d_raw[at, lanes] = part.astype(BF16)
            for i in range(3):
                steps = plan[4 * i + turn]
                if steps:

                    @pl.when(p == i)
                    def _(steps=steps):
                        for step in steps:
                            step()

        part = dk_acc[...]
        part = part * cos_ref[...] - turned(part) * sin_ref[...]
        d_raw[:, pl.ds(pl.multiple_of(width + p * 128, 128), 128)] = part.astype(BF16)
        d_raw[:, pl.ds(pl.multiple_of(2 * width + p * 128, 128), 128)] = dv_acc[...].astype(BF16)
        return carry

    lax.fori_loop(0, 3, pair_step, 0)
    for t in range(3):
        grads = dot_nn(d_raw[:, t * width : (t + 1) * width].T, x2[...]).astype(BF16)
        qkv_part[:, :, :, :, t * dim : (t + 1) * dim] = grads.reshape(qkv_part.shape[:4] + (dim,))
    qkv.step()
    weights = [w2[:, :, t * dim : (t + 1) * dim].reshape(width, dim) for t in range(3)]

    def project(at):
        return sum(
            dot_nn(d_raw[at, t * width : (t + 1) * width], weights[t]) for t in range(3)
        )

    in_send[...] = project(theirs).astype(BF16)
    swap_in.start()
    qkv.step()
    jobs = [down, gate, up, out, qkv, gain]
    own = resid[...] + project(mine)
    for job in jobs:
        job.step()
    swap_in.wait_recv()
    in_grad[...] = (own + in_recv[...].astype(F32)).astype(BF16)
    while any(job.steps for job in jobs):
        for job in jobs:
            job.step()
    links.drain()


def backward(
    length, d_all, slot_in, qkv_all, queries, keys, values, stats, cosines, sines, d_resid, gains,
    out_part, normed, ffn_out, hidden, d_gates, d_ups,
):
    rows, dim = d_resid.shape
    width = queries.shape[1]
    units = hidden[0].shape[1]
    shape = jax.ShapeDtypeStruct
    shards = [(4, 2, 2, units // 4, dim)] + [(4, 2, 2, dim // 4, units)] * 2 + [out_part.shape]
    shards.append((2, 2, 2, width // 8, qkv_all.shape[2]))
    scratch = []
    copies = 4 + 6
    for n, _, _, height, cols in shards:
        half, cut = cols // 2, cut_of(4 * height)
        copies += 2 * n + 3 + 9
        scratch += [
            pltpu.VMEM((n, 2, 2, height, half), BF16),
            pltpu.VMEM((n, 2, cut, half), BF16),
            pltpu.VMEM((n, 2, height - cut, half), BF16),
            pltpu.VMEM((n, height - cut, half), BF16),
            pltpu.VMEM((n, cut, half), BF16),
            pltpu.VMEM((n - 1, height, half), BF16),
        ]
    vmem = pl.BlockSpec(memory_space=pltpu.VMEM)
    return pl.pallas_call(
        backward_kernel,
        out_shape=[shape((rows, dim), BF16)]
        + [shape((4 * s[3], s[4]), BF16) for s in shards]
        + [shape(gains.shape, F32)],
        in_specs=[pl.BlockSpec(memory_space=pltpu.SMEM)] + [vmem] * 26,
        out_specs=[vmem] * 7,
        scratch_shapes=[
            pltpu.SemaphoreType.DMA((copies,)),
            pltpu.SemaphoreType.DMA((copies,)),
            pltpu.VMEM((SLOT_LEN, width), BF16),
            pltpu.VMEM((SLOT_LEN, QB), F32),
            pltpu.VMEM((SLOT_LEN, 3 * width), BF16),
            pltpu.VMEM((SLOT_LEN, 128), F32),
            pltpu.VMEM((SLOT_LEN, 128), F32),
            pltpu.VMEM(shards[4], BF16),
            pltpu.VMEM((rows, dim), BF16),
            pltpu.VMEM((rows, dim), BF16),
            pltpu.VMEM(shards[0], BF16),
            pltpu.VMEM(shards[1], BF16),
            pltpu.VMEM(shards[2], BF16),
            pltpu.VMEM(gains.shape, F32),
            pltpu.VMEM(gains.shape, F32),
            pltpu.VMEM(gains.shape, F32),
            pltpu.VMEM((3,) + gains.shape, F32),
            pltpu.VMEM((4,) + gains.shape, F32),
        ]
        + scratch,
        compiler_params=pltpu.CompilerParams(
            collective_id=1, has_side_effects=True, vmem_limit_bytes=VMEM_LIMIT
        ),
        name="attention_backward",
    )(
        length, d_all, slot_in, qkv_all, queries, keys, values, stats, cosines, sines, d_resid,
        gains, out_part, normed, ffn_out, *hidden, *d_gates, *d_ups,
    )


ALL = (0, 2, 1, 3)


def body(
    dp_size,
    layer_in,
    query_proj,
    key_proj,
    value_proj,
    out_proj,
    gate_proj,
    up_proj,
    down_proj,
    first_gain,
    second_gain,
    seq_lengths,
    cotangent,
):
    z = lax.axis_index("mp")
    valid_len = lax.dynamic_index_in_dim(seq_lengths, lax.div(z, 2), keepdims=False)
    width = query_proj.shape[1]

    qkv_own = jnp.concatenate([query_proj.T, key_proj.T, value_proj.T], axis=1)
    cosines, sines = rotary_tables(SLOT_LEN)
    cos_wide = jnp.tile(cosines[:, 0, :], (1, 4))
    sin_wide = jnp.tile(jnp.concatenate([-sines[:, 0, :], sines[:, 0, :]], axis=1), (1, 2))
    (
        slot_in, qkv_all, out_all, rot_queries, rot_keys, values_low, mixed_all, stats,
        resid_one, gate_far, up_far, down_far,
    ) = attention(
        valid_len[None], layer_in, qkv_own, out_proj, cos_wide, sin_wide,
        gate_proj, up_proj, down_proj,
    )
    out_all = out_all.reshape(4 * width, -1)
    normed, first_pull = jax.vjp(rms_norm, resid_one, first_gain)
    normed_low = normed.astype(BF16)

    gates = [gate_proj] + [gate_far[i] for i in range(3)]
    ups = [up_proj] + [up_far[i] for i in range(3)]
    downs = [down_proj] + [down_far[i] for i in range(3)]
    gate_pre = [forward(normed_low, w) for w in gates]
    up_pre = [forward(normed_low, w) for w in ups]
    hidden = [swiglu(g, u).astype(BF16) for g, u in zip(gate_pre, up_pre)]
    ffn_branch = sum(forward(h, w) for h, w in zip(hidden, downs))
    resid_two = normed + ffn_branch
    result, second_pull = jax.vjp(rms_norm, resid_two, second_gain)
    layer_out = result.astype(BF16)
    d_resid_two, second_part = second_pull(cotangent.astype(F32))
    ffn_out = d_resid_two.astype(BF16)
    d_normed = d_resid_two
    d_gates, d_ups = [], []
    for r in range(4):
        d_hidden = against(ffn_out, downs[r])
        unused, glu_pull = jax.vjp(swiglu, gate_pre[r], up_pre[r])
        d_gate, d_up = (d.astype(BF16) for d in glu_pull(d_hidden))
        d_gates.append(d_gate)
        d_ups.append(d_up)
        d_normed = d_normed + against(d_gate, gates[r]) + against(d_up, ups[r])
    d_resid_one, first_part = first_pull(d_normed)
    attn_out = d_resid_one.astype(BF16)
    out_part = cross(mixed_all, attn_out).astype(BF16).reshape(4, 2, 2, width // 4, -1)
    d_all = against(attn_out, out_all).astype(BF16)
    gains = jnp.concatenate(
        [first_part[None], second_part[None], jnp.zeros((6, first_part.shape[0]), F32)], axis=0
    )
    input_grad, down_grad, gate_grad, up_grad, out_grad, qkv_grad, gains = backward(
        valid_len[None], d_all, slot_in, qkv_all, rot_queries, rot_keys, values_low, stats,
        cos_wide, sin_wide, d_resid_one, gains, out_part, normed_low, ffn_out, hidden, d_gates,
        d_ups,
    )
    dim = layer_in.shape[1]
    down_grad, gate_grad, up_grad, out_grad, qkv_grad = (
        g.astype(F32) for g in (down_grad, gate_grad, up_grad, out_grad, qkv_grad)
    )
    if dp_size > BLOCK:
        groups = [list(range(i, dp_size, BLOCK)) for i in range(BLOCK)]
        down_grad, gate_grad, up_grad, out_grad, qkv_grad, gains = lax.psum(
            (down_grad, gate_grad, up_grad, out_grad, qkv_grad, gains),
            "dp",
            axis_index_groups=groups,
        )
    qkv_grad = [qkv_grad[:, t * dim : (t + 1) * dim] for t in range(3)]
    return (
        layer_out,
        input_grad,
        qkv_grad[0].T,
        qkv_grad[1].T,
        qkv_grad[2].T,
        out_grad,
        gate_grad,
        up_grad,
        down_grad,
        gains[0],
        gains[1],
    )


def solution(mesh):
    rows = P(("dp", "mp"), None)
    cols, first = P(None, "mp"), P("mp", None)
    return jax.shard_map(
        functools.partial(body, mesh.shape["dp"]),
        mesh=mesh,
        in_specs=(rows, cols, cols, cols, first, cols, cols, first, P(), P(), P("dp"), rows),
        out_specs=(rows, rows, cols, cols, cols, first, cols, cols, first, P(), P()),
        check_vma=False,
    )
```

```python
import functools

import jax
import jax.numpy as jnp
from jax import lax
from jax.experimental import pallas as pl
from jax.experimental.pallas import tpu as pltpu
from jax.sharding import PartitionSpec as P

HS = 64
SLOT_LEN = 1024
BLOCK = 8
VMEM_LIMIT = 63 << 20
F32 = jnp.float32
BF16 = jnp.bfloat16


def rms_norm(resid, gain):
    return resid * lax.rsqrt(jnp.mean(resid * resid, axis=-1, keepdims=True) + 1e-05) * gain


def swiglu(gate_pre, up_pre):
    return jax.nn.silu(gate_pre) * up_pre


def rotary_tables(rows):
    half = HS // 2
    positions = (jnp.arange(rows, dtype=jnp.int32) % SLOT_LEN).astype(F32)
    freqs = 10000.0 ** (-jnp.arange(half, dtype=F32) * 2.0 / HS)
    angles = positions[:, None] * freqs[None, :]
    return (jnp.cos(angles)[:, None, :], jnp.sin(angles)[:, None, :])


def cross(left, right):
    return lax.dot_general(left, right, (((0,), (0,)), ((), ())), preferred_element_type=F32)


def against(left, right):
    return lax.dot_general(left, right, (((1,), (1,)), ((), ())), preferred_element_type=F32)


def forward(left, right):
    return jnp.dot(left, right, preferred_element_type=F32)


class Links:
    def __init__(self, send, recv):
        self.send, self.recv = send, recv
        self.count = 0
        self.sent = []
        self.d = lax.axis_index("dp")
        self.z = lax.axis_index("mp")
        self.core = (self.flip(1), self.z)
        self.xn = (self.flip(2), self.z)
        self.yn = (self.flip(4), self.z)
        self.c = lax.rem(self.d, 2)
        self.x = lax.rem(lax.div(self.d, 2), 2)
        self.y = lax.rem(lax.div(self.d, 4), 2)

    def flip(self, step):
        bit = lax.rem(lax.div(self.d, step), 2)
        return self.d + step * (1 - 2 * bit)

    def along(self, r):
        low, high = lax.rem(self.z, 2), lax.div(self.z, 2)
        low = 1 - low if r % 2 else low
        high = 1 - high if r // 2 else high
        return (self.d, 2 * high + low)

    def barrier(self):
        sem = pltpu.get_barrier_semaphore()
        targets = [self.core, self.xn, self.yn] + [self.along(r) for r in (1, 2, 3)]
        for target in targets:
            pl.semaphore_signal(
                sem, inc=1, device_id=target, device_id_type=pl.DeviceIdType.MESH
            )
        pl.semaphore_wait(sem, len(targets))

    def plan(self, src, dst, target):
        copy = pltpu.make_async_remote_copy(
            src_ref=src,
            dst_ref=dst,
            send_sem=self.send.at[self.count],
            recv_sem=self.recv.at[self.count],
            device_id=target,
            device_id_type=pl.DeviceIdType.MESH,
        )
        self.count += 1
        self.sent.append(copy)
        return copy

    def copy(self, src, dst, target):
        copy = self.plan(src, dst, target)
        copy.start()
        return copy

    def drain(self):
        for copy in self.sent:
            copy.wait_send()


def cut_of(rows):
    line = rows // 4
    return max(16, (line // 2 + 15) // 16 * 16)


def piece(ref, lead, line, c, part):
    rows, cols = ref.shape[-2], ref.shape[-1]
    height, width, cut = rows // 4, cols // 2, cut_of(rows)
    first, size = {"all": (0, height), "a": (0, cut), "b": (cut, height - cut)}[part]
    at_rows = pl.ds(pl.multiple_of(line * height + first, 16), size)
    at_cols = pl.ds(pl.multiple_of(c * width, 128), width)
    if lead is None:
        return ref.at[at_rows, at_cols]
    return ref.at[lead, at_rows, at_cols]


class Spread:
    def __init__(self, links, ref, lead):
        x, y, c = links.x, links.y, links.c
        own, off_x, off_y, far = 2 * y + x, 2 * y + 1 - x, 2 * (1 - y) + x, 3 - 2 * y - x

        def put(line, part, target):
            block = piece(ref, lead, line, c, part)
            return links.plan(block, block, target)

        self.to_x = put(own, "all", links.xn)
        self.to_y = put(own, "all", links.yn)
        self.far_a = put(off_x, "a", links.yn)
        self.far_b = put(off_y, "b", links.xn)
        self.cores = [
            put(own, "all", links.core),
            put(off_x, "all", links.core),
            put(off_y, "all", links.core),
            put(far, "a", links.core),
            put(far, "b", links.core),
        ]

    def start(self):
        self.to_x.start()
        self.to_y.start()
        self.cores[0].start()

    def relay(self):
        self.to_x.wait_recv()
        self.far_a.start()
        self.cores[1].start()
        self.to_y.wait_recv()
        self.far_b.start()
        self.cores[2].start()

    def last(self):
        self.far_a.wait_recv()
        self.cores[3].start()
        self.far_b.wait_recv()
        self.cores[4].start()

    def end(self):
        for copy in self.cores:
            copy.wait_recv()


class Gather:
    def __init__(self, links, shard, out, slot0, rels):
        line = 2 * links.y + links.x
        self.from_z = [
            links.plan(
                piece(shard, None, line, links.c, "all"),
                piece(out, slot0 + i, line, links.c, "all"),
                links.along(r),
            )
            for i, r in enumerate(rels)
        ]
        self.plane = Spread(links, out, pl.ds(slot0, len(rels)))
        self.steps = [self.arrive, self.plane.relay, self.plane.last, self.plane.end]

    def send(self):
        for copy in self.from_z:
            copy.start()

    def arrive(self):
        for copy in self.from_z:
            copy.wait_recv()
        self.plane.start()

    def step(self):
        if self.steps:
            self.steps.pop(0)()

    def finish(self):
        while self.steps:
            self.step()


def dot_nt(left, right):
    return lax.dot_general(left, right, (((1,), (1,)), ((), ())), preferred_element_type=F32)


def dot_tn(left, right):
    return lax.dot_general(left, right, (((0,), (0,)), ((), ())), preferred_element_type=F32)


def dot_nn(left, right):
    return lax.dot_general(left, right, (((1,), (0,)), ((), ())), preferred_element_type=F32)


def turned(values):
    lane = lax.broadcasted_iota(jnp.int32, values.shape, 1)
    return jnp.where(
        lax.rem(lane, HS) < HS // 2,
        pltpu.roll(values, 128 - HS // 2, 1),
        pltpu.roll(values, HS // 2, 1),
    )


def head_mask(head):
    lane = lax.broadcasted_iota(jnp.int32, (1, 128), 1)
    return jnp.where(lax.div(lane, HS) == head, 1.0, 0.0).astype(BF16)


QB = 256
FORWARD_PLAN = ["o", "", "o", "g", "o", "g", "u", "o", "g", "u", "", "d"]
BACKWARD_PLAN = [
    "o", "do", "go",
    "n", "d", "u", "n", "g", "o", "d", "n", "u", "o", "gn", "d",
    "quo", "qdg", "qdq",
]


def attention_kernel(
    len_ref, x_ref, qkv_ref, o_ref, cos_ref, sin_ref, gate_ref, up_ref, down_ref,
    x2, w2, wo, q_ref, k_ref, v_ref, m_all, stat, resid, gate_far, up_far, down_far,
    send, recv, m_ref, bias,
):
    links = Links(send, recv)
    rows = x_ref.shape[0]
    half = lax.rem(links.z, 2)
    mine = pl.ds(pl.multiple_of(half * rows, rows), rows)
    theirs = pl.ds(pl.multiple_of((1 - half) * rows, rows), rows)
    partner = links.along(1)
    length = len_ref[0]
    links.barrier()
    g_qkv = Gather(links, qkv_ref, w2, 1, (2,))
    g_out = Gather(links, o_ref, wo, 1, (2, 1, 3))
    g_gate = Gather(links, gate_ref, gate_far, 0, (2, 1, 3))
    g_up = Gather(links, up_ref, up_far, 0, (2, 1, 3))
    g_down = Gather(links, down_ref, down_far, 0, (2, 1, 3))
    swap_x = links.plan(x_ref, x2.at[mine], partner)
    width = m_ref.shape[1]
    swap_m = [
        links.plan(
            m_ref.at[theirs, pl.ds(p * 128, 128)], m_all.at[:, pl.ds(width + p * 128, 128)], partner
        )
        for p in range(3)
    ]
    g_qkv.send()
    swap_x.start()
    g_out.send()
    g_gate.send()
    g_up.send()
    x2[mine, :] = x_ref[...]
    w2[0] = qkv_ref[...]
    wo[0] = o_ref[...]
    key_at = lax.broadcasted_iota(jnp.int32, (SLOT_LEN, QB), 0)
    bias[...] = jnp.where(key_at < length, 0.0, -1e30)
    stat[...] = jnp.zeros_like(stat)
    g_qkv.finish()
    dim = x_ref.shape[1]
    w_rows = w2.shape[0] * w2.shape[1]
    for at in (mine, theirs):
        if at is theirs:
            swap_x.wait_recv()
        for t, dst in enumerate((q_ref, k_ref, v_ref)):
            w = w2[:, :, t * dim : (t + 1) * dim].reshape(w_rows, dim)
            raw = dot_nt(x2[at, :], w)
            for p in range(3):
                part = raw[:, p * 128 : (p + 1) * 128]
                if t < 2:
                    part = part * cos_ref[at, :] + turned(part) * sin_ref[at, :]
                if t == 0:
                    part = part.astype(BF16) * 0.125
                dst[at, p * 128 : (p + 1) * 128] = part.astype(BF16)

    plan = FORWARD_PLAN
    named = {"o": g_out, "g": g_gate, "u": g_up, "d": g_down}
    plan = [[named[name].steps.pop(0) for name in names] for names in plan]

    def pair_step(p, carry):
        lanes = pl.ds(pl.multiple_of(p * 128, 128), 128)
        k_pair, v_turn = k_ref[:, lanes], v_ref[:, lanes].T
        keys = [k_pair * head_mask(h) for h in range(2)]
        for qb in range(SLOT_LEN // QB):
            at = pl.ds(qb * QB, QB)
            span = (qb + 1) * QB
            query = q_ref[at, lanes]
            query_at = qb * QB + lax.broadcasted_iota(jnp.int32, (1, QB), 1)
            outs = []
            for h in range(2):
                scores = dot_nt(keys[h][:span], query) + bias[:span, :]
                causal = lax.broadcasted_iota(jnp.int32, (QB, QB), 0) <= (
                    lax.broadcasted_iota(jnp.int32, (QB, QB), 1)
                )
                diag = jnp.where(causal, scores[span - QB :], -1e30)
                if qb:
                    scores = jnp.concatenate([scores[: span - QB], diag], axis=0)
                else:
                    scores = diag
                top = jnp.max(scores, axis=0, keepdims=True)
                probs = jnp.exp(scores - top)
                total = jnp.sum(probs, axis=0, keepdims=True)
                out = dot_nn(v_turn[h * HS : (h + 1) * HS, :span], probs.astype(BF16))
                outs.append(out * jnp.where(query_at < length, 1.0 / total, 0.0))
                stat[pl.ds(2 * p + h, 1), at] = top + jnp.log(total)
            m_ref[at, lanes] = jnp.concatenate(outs, axis=0).T.astype(BF16)
            for i in range(3):
                steps = list(plan[4 * i + qb])
                if qb == 3:
                    steps.append(swap_m[i].start)
                    if i == 0:
                        steps.append(g_down.send)
                if steps:

                    @pl.when(p == i)
                    def _(steps=steps):
                        for step in steps:
                            step()

        return carry

    lax.fori_loop(0, 3, pair_step, 0)
    m_all[:, :width] = m_ref[mine, :]
    wo_rows = wo.shape[1]
    g_out.finish()
    g_up.step()
    first = dot_nn(m_all[:, :width], wo[0:2].reshape(2 * wo_rows, dim))
    g_down.step()
    for copy in swap_m:
        copy.wait_recv()
    g_gate.step()
    second = dot_nn(m_all[:, width:], wo[2:4].reshape(2 * wo_rows, dim))
    resid[...] = x_ref[...].astype(F32) + first + second
    gathers = [g_gate, g_up, g_down]
    while any(g.steps for g in gathers):
        for g in gathers:
            g.step()
    links.drain()


def attention(length, layer_in, qkv_own, out_proj, cosines, sines, gate_proj, up_proj, down_proj):
    rows, dim = layer_in.shape
    width = out_proj.shape[0]
    vmem, hbm = pl.BlockSpec(memory_space=pltpu.VMEM), pl.BlockSpec(memory_space=pl.ANY)
    shape = jax.ShapeDtypeStruct
    copies = 64
    heads = shape((SLOT_LEN, 2 * width), BF16)
    return pl.pallas_call(
        attention_kernel,
        out_shape=[
            shape((SLOT_LEN, dim), BF16),
            shape((2,) + qkv_own.shape, BF16),
            shape((4,) + out_proj.shape, BF16),
            heads,
            heads,
            heads,
            shape((rows, 4 * width), BF16),
            shape((8, SLOT_LEN), F32),
            shape((rows, dim), F32),
            shape((3,) + gate_proj.shape, BF16),
            shape((3,) + up_proj.shape, BF16),
            shape((3,) + down_proj.shape, BF16),
        ],
        in_specs=[pl.BlockSpec(memory_space=pltpu.SMEM)] + [vmem] * 5 + [hbm] * 3,
        out_specs=[vmem] * 9 + [hbm] * 3,
        scratch_shapes=[
            pltpu.SemaphoreType.DMA((copies,)),
            pltpu.SemaphoreType.DMA((copies,)),
            pltpu.VMEM((SLOT_LEN, 2 * width), BF16),
            pltpu.VMEM((SLOT_LEN, QB), F32),
        ],
        compiler_params=pltpu.CompilerParams(
            collective_id=0, has_side_effects=True, vmem_limit_bytes=VMEM_LIMIT
        ),
        name="attention_forward",
    )(length, layer_in, qkv_own, out_proj, cosines, sines, gate_proj, up_proj, down_proj)


class Steps:
    def step(self):
        if self.steps:
            self.steps.pop(0)()


class Reduction(Steps):
    def __init__(self, links, rel, parts, out, acc, x_one, y_one, x_two, y_two, from_z):
        self.links, self.parts, self.out, self.acc = links, parts, out, acc
        self.x_one, self.y_one, self.x_two, self.y_two = x_one, y_one, x_two, y_two
        self.from_z = from_z
        x, y, c = links.x, links.y, links.c
        height, width = acc.shape[3], acc.shape[4]
        cut = cut_of(4 * height)
        self.a, self.b = pl.ds(0, cut), pl.ds(cut, height - cut)
        self.mine = pl.ds(pl.multiple_of(c * width, 128), width)
        other = pl.ds(pl.multiple_of((1 - c) * width, 128), width)
        self.n = len(rel)
        self.core = [
            links.plan(parts[s].at[:, :, :, other], acc.at[s], links.core) for s in range(self.n)
        ]
        self.to_x = links.plan(acc.at[:, :, 1 - x, self.a], x_one, links.xn)
        self.to_y = links.plan(acc.at[:, 1 - y, :, self.b], y_one, links.yn)
        self.to_y2 = links.plan(acc.at[:, 1 - y, x, self.a], y_two, links.yn)
        self.to_x2 = links.plan(acc.at[:, y, 1 - x, self.b], x_two, links.xn)
        self.to_z = [
            links.plan(acc.at[s, y, x], from_z.at[s - 1], links.along(rel[s]))
            for s in range(1, self.n)
        ]
        self.plane = Spread(links, out, None)
        self.total = piece(out, None, 2 * y + x, c, "all")
        self.steps = [
            self.start, self.one, self.two, self.three, self.four,
            self.plane.relay, self.plane.last, self.plane.end,
        ]

    def start(self):
        for copy in self.core:
            copy.start()

    def one(self):
        acc = self.acc
        for s in range(self.n):
            self.core[s].wait_recv()
            acc[s] = acc[s] + self.parts[s][:, :, :, self.mine]
        self.to_x.start()
        self.to_y.start()

    def two(self):
        acc, x, y = self.acc, self.links.x, self.links.y
        self.to_x.wait_recv()
        for s in range(self.n):
            for row in range(2):
                acc[s, row, x, self.a] = acc[s, row, x, self.a] + self.x_one[s, row]
        self.to_y2.start()
        self.to_y.wait_recv()
        for s in range(self.n):
            for col in range(2):
                acc[s, y, col, self.b] = acc[s, y, col, self.b] + self.y_one[s, col]
        self.to_x2.start()

    def three(self):
        acc, x, y = self.acc, self.links.x, self.links.y
        self.to_y2.wait_recv()
        self.to_x2.wait_recv()
        for s in list(range(1, self.n)) + [0]:
            acc[s, y, x, self.a] = acc[s, y, x, self.a] + self.y_two[s]
            acc[s, y, x, self.b] = acc[s, y, x, self.b] + self.x_two[s]
            if s:
                self.to_z[s - 1].start()

    def four(self):
        for copy in self.to_z:
            copy.wait_recv()
        total = self.acc[0, self.links.y, self.links.x].astype(F32)
        for s in range(self.n - 1):
            total = total + self.from_z[s].astype(F32)
        self.total[...] = total.astype(BF16)
        self.plane.start()


class GainSum(Steps):
    def __init__(self, links, gains, out, from_core, from_x, from_y, from_z, acc):
        self.gains, self.out, self.from_z, self.acc = gains, out, from_z, acc
        self.hops = [
            (from_core, links.plan(acc.at[0], from_core, links.core)),
            (from_x, links.plan(acc.at[1], from_x, links.xn)),
            (from_y, links.plan(acc.at[2], from_y, links.yn)),
        ]
        self.to_z = [links.plan(acc.at[3], from_z.at[r - 1], links.along(r)) for r in (1, 2, 3)]
        self.steps = [self.start] + [functools.partial(self.hop, i) for i in range(3)] + [self.end]

    def start(self):
        self.acc[0] = self.gains[...]
        self.hops[0][1].start()

    def hop(self, i):
        self.hops[i][1].wait_recv()
        self.acc[i + 1] = self.acc[i] + self.hops[i][0][...]
        for copy in [self.hops[i + 1][1]] if i < 2 else self.to_z:
            copy.start()

    def end(self):
        for copy in self.to_z:
            copy.wait_recv()
        self.out[...] = self.acc[3] + self.from_z[0] + self.from_z[1] + self.from_z[2]


def backward_kernel(
    len_ref, d_ref, x2, w2, q_ref, k_ref, v_ref, stat, cos_ref, sin_ref, resid, gains, out_part,
    normed, ffn_out, *refs,
):
    hidden, d_gates, d_ups = refs[0:4], refs[4:8], refs[8:12]
    in_grad, down_out, gate_out, up_out, out_out, qkv_out, gains_out = refs[12:19]
    send, recv, d2, bias, d_raw, dk_acc, dv_acc, qkv_part, in_send, in_recv = refs[19:29]
    down_part, gate_part, up_part = refs[29:32]
    gain_refs, rest = refs[32:37], refs[37:]
    links = Links(send, recv)
    rows, dim = resid.shape
    width = d2.shape[1]
    half = lax.rem(links.z, 2)
    mine = pl.ds(pl.multiple_of(half * rows, rows), rows)
    theirs = pl.ds(pl.multiple_of((1 - half) * rows, rows), rows)
    partner = links.along(1)
    length = len_ref[0]
    links.barrier()
    swaps = [
        links.plan(
            d_ref.at[:, pl.ds(width + p * 128, 128)], d2.at[mine, pl.ds(p * 128, 128)], partner
        )
        for p in range(3)
    ]
    swap_in = links.plan(in_send, in_recv, partner)
    qkv_parts = [qkv_part.at[s] for s in range(2)]
    down_parts, gate_parts, up_parts, out_parts = (
        [part.at[s] for s in range(4)] for part in (down_part, gate_part, up_part, out_part)
    )
    down, gate, up, out = (
        Reduction(links, ALL, parts, result, *rest[6 * i : 6 * i + 6])
        for i, (parts, result) in enumerate(
            [(down_parts, down_out), (gate_parts, gate_out), (up_parts, up_out),
             (out_parts, out_out)]
        )
    )
    qkv = Reduction(links, (0, 2), qkv_parts, qkv_out, *rest[24:30])
    gain = GainSum(links, gains, gains_out, *gain_refs)
    for copy in swaps:
        copy.start()

    def produce(job, part, left, right):
        for s in range(4):
            part[s] = dot_nn(left(s), right(s)).astype(BF16).reshape(part.shape[1:])
            job.core[s].start()
        job.steps.pop(0)

    named = {"d": down, "g": gate, "u": up, "o": out, "q": qkv, "n": gain}

    def advance(names):
        for name in names:
            named[name].step()

    turned_rows = normed[...].T
    advance("on")
    produce(down, down_part, lambda s: hidden[s][...].T, lambda s: ffn_out[...])
    advance(BACKWARD_PLAN[0])
    produce(gate, gate_part, lambda s: turned_rows, lambda s: d_gates[s][...])
    advance(BACKWARD_PLAN[1])
    produce(up, up_part, lambda s: turned_rows, lambda s: d_ups[s][...])
    d2[mine, :] = d_ref[:, :width]
    key_at = lax.broadcasted_iota(jnp.int32, (SLOT_LEN, QB), 0)
    bias[...] = jnp.where(key_at < length, 0.0, -1e30)
    advance(BACKWARD_PLAN[2])
    plan = [[named[name] for name in names] for names in BACKWARD_PLAN[3:15]]
    plan = [[job.steps.pop(0) for job in jobs] for jobs in plan]

    def pair_step(p, carry):
        lanes = pl.ds(pl.multiple_of(p * 128, 128), 128)
        for i in range(3):

            @pl.when(p == i)
            def _(i=i):
                swaps[i].wait_recv()

        k_pair, v_pair = k_ref[:, lanes], v_ref[:, lanes]
        k_turn = k_pair.T
        keys = [k_pair * head_mask(h) for h in range(2)]
        values = [v_pair * head_mask(h) for h in range(2)]
        for turn, qb in enumerate(reversed(range(SLOT_LEN // QB))):
            at = pl.ds(qb * QB, QB)
            span = (qb + 1) * QB
            query = q_ref[at, lanes]
            query_at = qb * QB + lax.broadcasted_iota(jnp.int32, (QB, 128), 0)
            present = jnp.where(query_at < length, 1.0, 0.0).astype(BF16)
            grad = d2[at, lanes] * present
            d_scores, probs_low, d_query = [], [], []
            for h in range(2):
                scores = dot_nt(keys[h][:span], query) + bias[:span, :]
                causal = lax.broadcasted_iota(jnp.int32, (QB, QB), 0) <= (
                    lax.broadcasted_iota(jnp.int32, (QB, QB), 1)
                )
                diag = jnp.where(causal, scores[span - QB :], -1e30)
                if qb:
                    scores = jnp.concatenate([scores[: span - QB], diag], axis=0)
                else:
                    scores = diag
                probs = jnp.exp(scores - stat[pl.ds(2 * p + h, 1), at])
                d_probs = dot_nt(values[h][:span], grad)
                total = jnp.sum(d_probs * probs, axis=0, keepdims=True)
                d_score = (probs * (d_probs - total)).astype(BF16)
                d_query.append(dot_nn(k_turn[h * HS : (h + 1) * HS, :span], d_score))
                d_scores.append(d_score)
                probs_low.append(probs.astype(BF16))
            d_key = dot_nn(
                jnp.concatenate(d_scores, axis=1),
                jnp.concatenate([query * head_mask(h) for h in range(2)], axis=0),
            )
            d_value = dot_nn(
                jnp.concatenate(probs_low, axis=1),
                jnp.concatenate([grad * head_mask(h) for h in range(2)], axis=0),
            )
            if turn == 0:
                dk_acc[...] = d_key
                dv_acc[...] = d_value
            else:
                dk_acc[:span, :] = dk_acc[:span, :] + d_key
                dv_acc[:span, :] = dv_acc[:span, :] + d_value
            part = jnp.concatenate(d_query, axis=0).T * 0.125
            part = part * cos_ref[at, :] - turned(part) * sin_ref[at, :]
            d_raw[at, lanes] = part.astype(BF16)
            for i in range(3):
                steps = plan[4 * i + turn]
                if steps:

                    @pl.when(p == i)
                    def _(steps=steps):
                        for step in steps:
                            step()

        part = dk_acc[...]
        part = part * cos_ref[...] - turned(part) * sin_ref[...]
        d_raw[:, pl.ds(pl.multiple_of(width + p * 128, 128), 128)] = part.astype(BF16)
        d_raw[:, pl.ds(pl.multiple_of(2 * width + p * 128, 128), 128)] = dv_acc[...].astype(BF16)
        return carry

    lax.fori_loop(0, 3, pair_step, 0)
    for t in range(3):
        grads = dot_nn(d_raw[:, t * width : (t + 1) * width].T, x2[...]).astype(BF16)
        qkv_part[:, :, :, :, t * dim : (t + 1) * dim] = grads.reshape(qkv_part.shape[:4] + (dim,))
    weights = [w2[:, :, t * dim : (t + 1) * dim].reshape(width, dim) for t in range(3)]

    def project(at):
        return sum(
            dot_nn(d_raw[at, t * width : (t + 1) * width], weights[t]) for t in range(3)
        )

    advance(BACKWARD_PLAN[15])
    in_send[...] = project(theirs).astype(BF16)
    advance(BACKWARD_PLAN[16])
    own = resid[...] + project(mine)
    advance(BACKWARD_PLAN[17])
    swap_in.start()
    while any(job.steps for job in named.values()):
        advance("ougdqn")
    swap_in.wait_recv()
    in_grad[...] = (own + in_recv[...].astype(F32)).astype(BF16)
    links.drain()


def backward(
    length, d_all, slot_in, qkv_all, queries, keys, values, stats, cosines, sines, d_resid, gains,
    out_part, normed, ffn_out, hidden, d_gates, d_ups,
):
    rows, dim = d_resid.shape
    width = queries.shape[1]
    units = hidden[0].shape[1]
    shape = jax.ShapeDtypeStruct
    shards = [(4, 2, 2, units // 4, dim)] + [(4, 2, 2, dim // 4, units)] * 2 + [out_part.shape]
    shards.append((2, 2, 2, width // 8, qkv_all.shape[2]))
    scratch = []
    copies = 4 + 6
    for n, _, _, height, cols in shards:
        half, cut = cols // 2, cut_of(4 * height)
        copies += 2 * n + 3 + 9
        scratch += [
            pltpu.VMEM((n, 2, 2, height, half), BF16),
            pltpu.VMEM((n, 2, cut, half), BF16),
            pltpu.VMEM((n, 2, height - cut, half), BF16),
            pltpu.VMEM((n, height - cut, half), BF16),
            pltpu.VMEM((n, cut, half), BF16),
            pltpu.VMEM((n - 1, height, half), BF16),
        ]
    vmem = pl.BlockSpec(memory_space=pltpu.VMEM)
    return pl.pallas_call(
        backward_kernel,
        out_shape=[shape((rows, dim), BF16)]
        + [shape((4 * s[3], s[4]), BF16) for s in shards]
        + [shape(gains.shape, F32)],
        in_specs=[pl.BlockSpec(memory_space=pltpu.SMEM)] + [vmem] * 26,
        out_specs=[vmem] * 7,
        scratch_shapes=[
            pltpu.SemaphoreType.DMA((copies,)),
            pltpu.SemaphoreType.DMA((copies,)),
            pltpu.VMEM((SLOT_LEN, width), BF16),
            pltpu.VMEM((SLOT_LEN, QB), F32),
            pltpu.VMEM((SLOT_LEN, 3 * width), BF16),
            pltpu.VMEM((SLOT_LEN, 128), F32),
            pltpu.VMEM((SLOT_LEN, 128), F32),
            pltpu.VMEM(shards[4], BF16),
            pltpu.VMEM((rows, dim), BF16),
            pltpu.VMEM((rows, dim), BF16),
            pltpu.VMEM(shards[0], BF16),
            pltpu.VMEM(shards[1], BF16),
            pltpu.VMEM(shards[2], BF16),
            pltpu.VMEM(gains.shape, F32),
            pltpu.VMEM(gains.shape, F32),
            pltpu.VMEM(gains.shape, F32),
            pltpu.VMEM((3,) + gains.shape, F32),
            pltpu.VMEM((4,) + gains.shape, F32),
        ]
        + scratch,
        compiler_params=pltpu.CompilerParams(
            collective_id=1, has_side_effects=True, vmem_limit_bytes=VMEM_LIMIT
        ),
        name="attention_backward",
    )(
        length, d_all, slot_in, qkv_all, queries, keys, values, stats, cosines, sines, d_resid,
        gains, out_part, normed, ffn_out, *hidden, *d_gates, *d_ups,
    )


ALL = (0, 2, 1, 3)


def body(
    dp_size,
    layer_in,
    query_proj,
    key_proj,
    value_proj,
    out_proj,
    gate_proj,
    up_proj,
    down_proj,
    first_gain,
    second_gain,
    seq_lengths,
    cotangent,
):
    z = lax.axis_index("mp")
    valid_len = lax.dynamic_index_in_dim(seq_lengths, lax.div(z, 2), keepdims=False)
    width = query_proj.shape[1]

    qkv_own = jnp.concatenate([query_proj.T, key_proj.T, value_proj.T], axis=1)
    cosines, sines = rotary_tables(SLOT_LEN)
    cos_wide = jnp.tile(cosines[:, 0, :], (1, 4))
    sin_wide = jnp.tile(jnp.concatenate([-sines[:, 0, :], sines[:, 0, :]], axis=1), (1, 2))
    (
        slot_in, qkv_all, out_all, rot_queries, rot_keys, values_low, mixed_all, stats,
        resid_one, gate_far, up_far, down_far,
    ) = attention(
        valid_len[None], layer_in, qkv_own, out_proj, cos_wide, sin_wide,
        gate_proj, up_proj, down_proj,
    )
    out_all = out_all.reshape(4 * width, -1)
    normed, first_pull = jax.vjp(rms_norm, resid_one, first_gain)
    normed_low = normed.astype(BF16)

    gates = [gate_proj] + [gate_far[i] for i in range(3)]
    ups = [up_proj] + [up_far[i] for i in range(3)]
    downs = [down_proj] + [down_far[i] for i in range(3)]
    gate_pre = [forward(normed_low, w) for w in gates]
    up_pre = [forward(normed_low, w) for w in ups]
    hidden = [swiglu(g, u).astype(BF16) for g, u in zip(gate_pre, up_pre)]
    ffn_branch = sum(forward(h, w) for h, w in zip(hidden, downs))
    resid_two = normed + ffn_branch
    result, second_pull = jax.vjp(rms_norm, resid_two, second_gain)
    layer_out = result.astype(BF16)
    d_resid_two, second_part = second_pull(cotangent.astype(F32))
    ffn_out = d_resid_two.astype(BF16)
    d_normed = d_resid_two
    d_gates, d_ups = [], []
    for r in range(4):
        d_hidden = against(ffn_out, downs[r])
        unused, glu_pull = jax.vjp(swiglu, gate_pre[r], up_pre[r])
        d_gate, d_up = (d.astype(BF16) for d in glu_pull(d_hidden))
        d_gates.append(d_gate)
        d_ups.append(d_up)
        d_normed = d_normed + against(d_gate, gates[r]) + against(d_up, ups[r])
    d_resid_one, first_part = first_pull(d_normed)
    attn_out = d_resid_one.astype(BF16)
    out_part = cross(mixed_all, attn_out).astype(BF16).reshape(4, 2, 2, width // 4, -1)
    d_all = against(attn_out, out_all).astype(BF16)
    gains = jnp.concatenate(
        [first_part[None], second_part[None], jnp.zeros((6, first_part.shape[0]), F32)], axis=0
    )
    input_grad, down_grad, gate_grad, up_grad, out_grad, qkv_grad, gains = backward(
        valid_len[None], d_all, slot_in, qkv_all, rot_queries, rot_keys, values_low, stats,
        cos_wide, sin_wide, d_resid_one, gains, out_part, normed_low, ffn_out, hidden, d_gates,
        d_ups,
    )
    dim = layer_in.shape[1]
    down_grad, gate_grad, up_grad, out_grad, qkv_grad = (
        g.astype(F32) for g in (down_grad, gate_grad, up_grad, out_grad, qkv_grad)
    )
    if dp_size > BLOCK:
        groups = [list(range(i, dp_size, BLOCK)) for i in range(BLOCK)]
        down_grad, gate_grad, up_grad, out_grad, qkv_grad, gains = lax.psum(
            (down_grad, gate_grad, up_grad, out_grad, qkv_grad, gains),
            "dp",
            axis_index_groups=groups,
        )
    qkv_grad = [qkv_grad[:, t * dim : (t + 1) * dim] for t in range(3)]
    return (
        layer_out,
        input_grad,
        qkv_grad[0].T,
        qkv_grad[1].T,
        qkv_grad[2].T,
        out_grad,
        gate_grad,
        up_grad,
        down_grad,
        gains[0],
        gains[1],
    )


def solution(mesh):
    rows = P(("dp", "mp"), None)
    cols, first = P(None, "mp"), P("mp", None)
    return jax.shard_map(
        functools.partial(body, mesh.shape["dp"]),
        mesh=mesh,
        in_specs=(rows, cols, cols, cols, first, cols, cols, first, P(), P(), P("dp"), rows),
        out_specs=(rows, rows, cols, cols, cols, first, cols, cols, first, P(), P()),
        check_vma=False,
    )
```

```python
import functools

import jax
import jax.numpy as jnp
from jax import lax
from jax.experimental import pallas as pl
from jax.experimental.pallas import tpu as pltpu
from jax.sharding import PartitionSpec as P

HS = 64
SLOT_LEN = 1024
BLOCK = 8
VMEM_LIMIT = 63 << 20
F32 = jnp.float32
BF16 = jnp.bfloat16


def rms_norm(resid, gain):
    return resid * lax.rsqrt(jnp.mean(resid * resid, axis=-1, keepdims=True) + 1e-05) * gain


def swiglu(gate_pre, up_pre):
    return jax.nn.silu(gate_pre) * up_pre


def rotary_tables(rows):
    half = HS // 2
    positions = (jnp.arange(rows, dtype=jnp.int32) % SLOT_LEN).astype(F32)
    freqs = 10000.0 ** (-jnp.arange(half, dtype=F32) * 2.0 / HS)
    angles = positions[:, None] * freqs[None, :]
    return (jnp.cos(angles)[:, None, :], jnp.sin(angles)[:, None, :])


def cross(left, right):
    return lax.dot_general(left, right, (((0,), (0,)), ((), ())), preferred_element_type=F32)


def against(left, right):
    return lax.dot_general(left, right, (((1,), (1,)), ((), ())), preferred_element_type=F32)


def forward(left, right):
    return jnp.dot(left, right, preferred_element_type=F32)


class Links:
    def __init__(self, send, recv):
        self.send, self.recv = send, recv
        self.count = 0
        self.sent = []
        self.d = lax.axis_index("dp")
        self.z = lax.axis_index("mp")
        self.core = (self.flip(1), self.z)
        self.xn = (self.flip(2), self.z)
        self.yn = (self.flip(4), self.z)
        self.c = lax.rem(self.d, 2)
        self.x = lax.rem(lax.div(self.d, 2), 2)
        self.y = lax.rem(lax.div(self.d, 4), 2)

    def flip(self, step):
        bit = lax.rem(lax.div(self.d, step), 2)
        return self.d + step * (1 - 2 * bit)

    def along(self, r):
        low, high = lax.rem(self.z, 2), lax.div(self.z, 2)
        low = 1 - low if r % 2 else low
        high = 1 - high if r // 2 else high
        return (self.d, 2 * high + low)

    def barrier(self):
        sem = pltpu.get_barrier_semaphore()
        targets = [self.core, self.xn, self.yn] + [self.along(r) for r in (1, 2, 3)]
        for target in targets:
            pl.semaphore_signal(
                sem, inc=1, device_id=target, device_id_type=pl.DeviceIdType.MESH
            )
        pl.semaphore_wait(sem, len(targets))

    def plan(self, src, dst, target):
        copy = pltpu.make_async_remote_copy(
            src_ref=src,
            dst_ref=dst,
            send_sem=self.send.at[self.count],
            recv_sem=self.recv.at[self.count],
            device_id=target,
            device_id_type=pl.DeviceIdType.MESH,
        )
        self.count += 1
        self.sent.append(copy)
        return copy

    def copy(self, src, dst, target):
        copy = self.plan(src, dst, target)
        copy.start()
        return copy

    def drain(self):
        for copy in self.sent:
            copy.wait_send()


def cut_of(rows):
    line = rows // 4
    return max(16, (line // 2 + 15) // 16 * 16)


def piece(ref, lead, line, c, part):
    rows, cols = ref.shape[-2], ref.shape[-1]
    height, width, cut = rows // 4, cols // 2, cut_of(rows)
    first, size = {"all": (0, height), "a": (0, cut), "b": (cut, height - cut)}[part]
    at_rows = pl.ds(pl.multiple_of(line * height + first, 16), size)
    at_cols = pl.ds(pl.multiple_of(c * width, 128), width)
    if lead is None:
        return ref.at[at_rows, at_cols]
    return ref.at[lead, at_rows, at_cols]


class Spread:
    def __init__(self, links, ref, lead):
        x, y, c = links.x, links.y, links.c
        own, off_x, off_y, far = 2 * y + x, 2 * y + 1 - x, 2 * (1 - y) + x, 3 - 2 * y - x

        def put(line, part, target):
            block = piece(ref, lead, line, c, part)
            return links.plan(block, block, target)

        self.to_x = put(own, "all", links.xn)
        self.to_y = put(own, "all", links.yn)
        self.far_a = put(off_x, "a", links.yn)
        self.far_b = put(off_y, "b", links.xn)
        self.cores = [
            put(own, "all", links.core),
            put(off_x, "all", links.core),
            put(off_y, "all", links.core),
            put(far, "a", links.core),
            put(far, "b", links.core),
        ]

    def start(self):
        self.to_x.start()
        self.to_y.start()
        self.cores[0].start()

    def relay(self):
        self.to_x.wait_recv()
        self.far_a.start()
        self.cores[1].start()
        self.to_y.wait_recv()
        self.far_b.start()
        self.cores[2].start()

    def last(self):
        self.far_a.wait_recv()
        self.cores[3].start()
        self.far_b.wait_recv()
        self.cores[4].start()

    def end(self):
        for copy in self.cores:
            copy.wait_recv()


class Gather:
    def __init__(self, links, shard, out, slot0, rels):
        line = 2 * links.y + links.x
        self.from_z = [
            links.plan(
                piece(shard, None, line, links.c, "all"),
                piece(out, slot0 + i, line, links.c, "all"),
                links.along(r),
            )
            for i, r in enumerate(rels)
        ]
        self.plane = Spread(links, out, pl.ds(slot0, len(rels)))
        self.steps = [self.arrive, self.plane.relay, self.plane.last, self.plane.end]

    def send(self):
        for copy in self.from_z:
            copy.start()

    def arrive(self):
        for copy in self.from_z:
            copy.wait_recv()
        self.plane.start()

    def step(self):
        if self.steps:
            self.steps.pop(0)()

    def finish(self):
        while self.steps:
            self.step()


def dot_nt(left, right):
    return lax.dot_general(left, right, (((1,), (1,)), ((), ())), preferred_element_type=F32)


def dot_tn(left, right):
    return lax.dot_general(left, right, (((0,), (0,)), ((), ())), preferred_element_type=F32)


def dot_nn(left, right):
    return lax.dot_general(left, right, (((1,), (0,)), ((), ())), preferred_element_type=F32)


def turned(values):
    lane = lax.broadcasted_iota(jnp.int32, values.shape, 1)
    return jnp.where(
        lax.rem(lane, HS) < HS // 2,
        pltpu.roll(values, 128 - HS // 2, 1),
        pltpu.roll(values, HS // 2, 1),
    )


def head_mask(head):
    lane = lax.broadcasted_iota(jnp.int32, (1, 128), 1)
    return jnp.where(lax.div(lane, HS) == head, 1.0, 0.0).astype(BF16)


QB = 256
FORWARD_PLAN = ["o", "", "o", "g", "o", "g", "u", "o", "g", "u", "", "d"]
BACKWARD_PLAN = [
    "o", "do", "go",
    "n", "d", "u", "n", "g", "o", "d", "n", "u", "o", "gn", "d",
    "quqo", "dgq", "qd",
]


def attention_kernel(
    len_ref, x_ref, qkv_ref, o_ref, cos_ref, sin_ref, gate_ref, up_ref, down_ref,
    x2, w2, wo, q_ref, k_ref, v_ref, m_all, stat, resid, gate_far, up_far, down_far,
    send, recv, m_ref, bias,
):
    links = Links(send, recv)
    rows = x_ref.shape[0]
    half = lax.rem(links.z, 2)
    mine = pl.ds(pl.multiple_of(half * rows, rows), rows)
    theirs = pl.ds(pl.multiple_of((1 - half) * rows, rows), rows)
    partner = links.along(1)
    length = len_ref[0]
    links.barrier()
    g_qkv = Gather(links, qkv_ref, w2, 1, (2,))
    g_out = Gather(links, o_ref, wo, 1, (2, 1, 3))
    g_gate = Gather(links, gate_ref, gate_far, 0, (2, 1, 3))
    g_up = Gather(links, up_ref, up_far, 0, (2, 1, 3))
    g_down = Gather(links, down_ref, down_far, 0, (2, 1, 3))
    swap_x = links.plan(x_ref, x2.at[mine], partner)
    width = m_ref.shape[1]
    swap_m = [
        links.plan(
            m_ref.at[theirs, pl.ds(p * 128, 128)], m_all.at[:, pl.ds(width + p * 128, 128)], partner
        )
        for p in range(3)
    ]
    g_qkv.send()
    swap_x.start()
    g_out.send()
    g_gate.send()
    g_up.send()
    x2[mine, :] = x_ref[...]
    w2[0] = qkv_ref[...]
    wo[0] = o_ref[...]
    key_at = lax.broadcasted_iota(jnp.int32, (SLOT_LEN, QB), 0)
    bias[...] = jnp.where(key_at < length, 0.0, -1e30)
    stat[...] = jnp.zeros_like(stat)
    g_qkv.finish()
    dim = x_ref.shape[1]
    w_rows = w2.shape[0] * w2.shape[1]
    def project_rows(i, carry):
        @pl.when(i == 1)
        def _():
            swap_x.wait_recv()

        at = pl.ds(pl.multiple_of((half + i * (1 - 2 * half)) * rows, rows), rows)
        for t, dst in enumerate((q_ref, k_ref, v_ref)):
            w = w2[:, :, t * dim : (t + 1) * dim].reshape(w_rows, dim)
            raw = dot_nt(x2[at, :], w)
            for p in range(3):
                part = raw[:, p * 128 : (p + 1) * 128]
                if t < 2:
                    part = part * cos_ref[at, :] + turned(part) * sin_ref[at, :]
                if t == 0:
                    part = part.astype(BF16) * 0.125
                dst[at, p * 128 : (p + 1) * 128] = part.astype(BF16)
        return carry

    lax.fori_loop(0, 2, project_rows, 0)
    plan = FORWARD_PLAN
    named = {"o": g_out, "g": g_gate, "u": g_up, "d": g_down}
    plan = [[named[name].steps.pop(0) for name in names] for names in plan]

    def pair_step(p, carry):
        lanes = pl.ds(pl.multiple_of(p * 128, 128), 128)
        k_pair, v_turn = k_ref[:, lanes], v_ref[:, lanes].T
        keys = [k_pair * head_mask(h) for h in range(2)]
        for qb in range(SLOT_LEN // QB):
            at = pl.ds(qb * QB, QB)
            span = (qb + 1) * QB
            query = q_ref[at, lanes]
            query_at = qb * QB + lax.broadcasted_iota(jnp.int32, (1, QB), 1)
            outs = []
            for h in range(2):
                scores = dot_nt(keys[h][:span], query) + bias[:span, :]
                causal = lax.broadcasted_iota(jnp.int32, (QB, QB), 0) <= (
                    lax.broadcasted_iota(jnp.int32, (QB, QB), 1)
                )
                diag = jnp.where(causal, scores[span - QB :], -1e30)
                if qb:
                    scores = jnp.concatenate([scores[: span - QB], diag], axis=0)
                else:
                    scores = diag
                top = jnp.max(scores, axis=0, keepdims=True)
                probs = jnp.exp(scores - top)
                total = jnp.sum(probs, axis=0, keepdims=True)
                out = dot_nn(v_turn[h * HS : (h + 1) * HS, :span], probs.astype(BF16))
                outs.append(out * jnp.where(query_at < length, 1.0 / total, 0.0))
                stat[pl.ds(2 * p + h, 1), at] = top + jnp.log(total)
            m_ref[at, lanes] = jnp.concatenate(outs, axis=0).T.astype(BF16)
            for i in range(3):
                steps = list(plan[4 * i + qb])
                if qb == 3:
                    steps.append(swap_m[i].start)
                    if i == 0:
                        steps.append(g_down.send)
                if steps:

                    @pl.when(p == i)
                    def _(steps=steps):
                        for step in steps:
                            step()

        return carry

    lax.fori_loop(0, 3, pair_step, 0)
    m_all[:, :width] = m_ref[mine, :]
    wo_rows = wo.shape[1]
    g_out.finish()
    g_up.step()
    first = dot_nn(m_all[:, :width], wo[0:2].reshape(2 * wo_rows, dim))
    g_down.step()
    for copy in swap_m:
        copy.wait_recv()
    g_gate.step()
    second = dot_nn(m_all[:, width:], wo[2:4].reshape(2 * wo_rows, dim))
    resid[...] = x_ref[...].astype(F32) + first + second
    gathers = [g_gate, g_up, g_down]
    while any(g.steps for g in gathers):
        for g in gathers:
            g.step()
    links.drain()


def attention(length, layer_in, qkv_own, out_proj, cosines, sines, gate_proj, up_proj, down_proj):
    rows, dim = layer_in.shape
    width = out_proj.shape[0]
    vmem, hbm = pl.BlockSpec(memory_space=pltpu.VMEM), pl.BlockSpec(memory_space=pl.ANY)
    shape = jax.ShapeDtypeStruct
    copies = 64
    heads = shape((SLOT_LEN, 2 * width), BF16)
    return pl.pallas_call(
        attention_kernel,
        out_shape=[
            shape((SLOT_LEN, dim), BF16),
            shape((2,) + qkv_own.shape, BF16),
            shape((4,) + out_proj.shape, BF16),
            heads,
            heads,
            heads,
            shape((rows, 4 * width), BF16),
            shape((8, SLOT_LEN), F32),
            shape((rows, dim), F32),
            shape((3,) + gate_proj.shape, BF16),
            shape((3,) + up_proj.shape, BF16),
            shape((3,) + down_proj.shape, BF16),
        ],
        in_specs=[pl.BlockSpec(memory_space=pltpu.SMEM)] + [vmem] * 5 + [hbm] * 3,
        out_specs=[vmem] * 9 + [hbm] * 3,
        scratch_shapes=[
            pltpu.SemaphoreType.DMA((copies,)),
            pltpu.SemaphoreType.DMA((copies,)),
            pltpu.VMEM((SLOT_LEN, 2 * width), BF16),
            pltpu.VMEM((SLOT_LEN, QB), F32),
        ],
        compiler_params=pltpu.CompilerParams(
            collective_id=0, has_side_effects=True, vmem_limit_bytes=VMEM_LIMIT
        ),
        name="attention_forward",
    )(length, layer_in, qkv_own, out_proj, cosines, sines, gate_proj, up_proj, down_proj)


class Steps:
    def step(self):
        if self.steps:
            self.steps.pop(0)()


class Reduction(Steps):
    def __init__(self, links, rel, parts, out, acc, x_one, y_one, x_two, y_two, from_z):
        self.links, self.parts, self.out, self.acc = links, parts, out, acc
        self.x_one, self.y_one, self.x_two, self.y_two = x_one, y_one, x_two, y_two
        self.from_z = from_z
        x, y, c = links.x, links.y, links.c
        height, width = acc.shape[3], acc.shape[4]
        cut = cut_of(4 * height)
        self.a, self.b = pl.ds(0, cut), pl.ds(cut, height - cut)
        self.mine = pl.ds(pl.multiple_of(c * width, 128), width)
        other = pl.ds(pl.multiple_of((1 - c) * width, 128), width)
        self.n = len(rel)
        self.core = [
            links.plan(parts.at[s, :, :, :, other], acc.at[s], links.core) for s in range(self.n)
        ]
        self.to_x = links.plan(acc.at[:, :, 1 - x, self.a], x_one, links.xn)
        self.to_y = links.plan(acc.at[:, 1 - y, :, self.b], y_one, links.yn)
        self.to_y2 = links.plan(acc.at[:, 1 - y, x, self.a], y_two, links.yn)
        self.to_x2 = links.plan(acc.at[:, y, 1 - x, self.b], x_two, links.xn)
        self.to_z = [
            links.plan(acc.at[s, y, x], from_z.at[s - 1], links.along(rel[s]))
            for s in range(1, self.n)
        ]
        self.plane = Spread(links, out, None)
        self.total = piece(out, None, 2 * y + x, c, "all")
        self.steps = [
            self.start, self.one, self.two, self.three, self.four,
            self.plane.relay, self.plane.last, self.plane.end,
        ]

    def start(self):
        for copy in self.core:
            copy.start()

    def one(self):
        acc, parts = self.acc, self.parts
        for copy in self.core:
            copy.wait_recv()

        def add(s, carry):
            acc[s] = acc[s] + parts[s, :, :, :, self.mine]
            return carry

        lax.fori_loop(0, self.n, add, 0)
        self.to_x.start()
        self.to_y.start()

    def two(self):
        acc, x, y = self.acc, self.links.x, self.links.y
        self.to_x.wait_recv()
        for s in range(self.n):
            for row in range(2):
                acc[s, row, x, self.a] = acc[s, row, x, self.a] + self.x_one[s, row]
        self.to_y2.start()
        self.to_y.wait_recv()
        for s in range(self.n):
            for col in range(2):
                acc[s, y, col, self.b] = acc[s, y, col, self.b] + self.y_one[s, col]
        self.to_x2.start()

    def three(self):
        acc, x, y = self.acc, self.links.x, self.links.y
        self.to_y2.wait_recv()
        self.to_x2.wait_recv()
        for s in list(range(1, self.n)) + [0]:
            acc[s, y, x, self.a] = acc[s, y, x, self.a] + self.y_two[s]
            acc[s, y, x, self.b] = acc[s, y, x, self.b] + self.x_two[s]
            if s:
                self.to_z[s - 1].start()

    def four(self):
        for copy in self.to_z:
            copy.wait_recv()
        total = self.acc[0, self.links.y, self.links.x].astype(F32)
        for s in range(self.n - 1):
            total = total + self.from_z[s].astype(F32)
        self.total[...] = total.astype(BF16)
        self.plane.start()


class GainSum(Steps):
    def __init__(self, links, gains, out, from_core, from_x, from_y, from_z, acc):
        self.gains, self.out, self.from_z, self.acc = gains, out, from_z, acc
        self.hops = [
            (from_core, links.plan(acc.at[0], from_core, links.core)),
            (from_x, links.plan(acc.at[1], from_x, links.xn)),
            (from_y, links.plan(acc.at[2], from_y, links.yn)),
        ]
        self.to_z = [links.plan(acc.at[3], from_z.at[r - 1], links.along(r)) for r in (1, 2, 3)]
        self.steps = [self.start] + [functools.partial(self.hop, i) for i in range(3)] + [self.end]

    def start(self):
        self.acc[0] = self.gains[...]
        self.hops[0][1].start()

    def hop(self, i):
        self.hops[i][1].wait_recv()
        self.acc[i + 1] = self.acc[i] + self.hops[i][0][...]
        for copy in [self.hops[i + 1][1]] if i < 2 else self.to_z:
            copy.start()

    def end(self):
        for copy in self.to_z:
            copy.wait_recv()
        self.out[...] = self.acc[3] + self.from_z[0] + self.from_z[1] + self.from_z[2]


def backward_kernel(
    len_ref, d_ref, x2, w2, q_ref, k_ref, v_ref, stat, cos_ref, sin_ref, resid, gains, out_part,
    normed, ffn_out, *refs,
):
    hidden, d_gates, d_ups = refs[0:4], refs[4:8], refs[8:12]
    in_grad, down_out, gate_out, up_out, out_out, qkv_out, gains_out = refs[12:19]
    send, recv, d2, bias, d_raw, dk_acc, dv_acc, qkv_part, in_send, in_recv = refs[19:29]
    down_part, gate_part, up_part = refs[29:32]
    gain_refs, rest = refs[32:37], refs[37:]
    links = Links(send, recv)
    rows, dim = resid.shape
    width = d2.shape[1]
    half = lax.rem(links.z, 2)
    mine = pl.ds(pl.multiple_of(half * rows, rows), rows)
    theirs = pl.ds(pl.multiple_of((1 - half) * rows, rows), rows)
    partner = links.along(1)
    length = len_ref[0]
    links.barrier()
    swaps = [
        links.plan(
            d_ref.at[:, pl.ds(width + p * 128, 128)], d2.at[mine, pl.ds(p * 128, 128)], partner
        )
        for p in range(3)
    ]
    swap_in = links.plan(in_send, in_recv, partner)
    down, gate, up, out = (
        Reduction(links, ALL, parts, result, *rest[6 * i : 6 * i + 6])
        for i, (parts, result) in enumerate(
            [(down_part, down_out), (gate_part, gate_out), (up_part, up_out),
             (out_part, out_out)]
        )
    )
    qkv = Reduction(links, (0, 2), qkv_part, qkv_out, *rest[24:30])
    gain = GainSum(links, gains, gains_out, *gain_refs)
    for copy in swaps:
        copy.start()

    def produce(job, part, left, right):
        for s in range(4):
            part[s] = dot_nn(left(s), right(s)).astype(BF16).reshape(part.shape[1:])
            job.core[s].start()
        job.steps.pop(0)

    named = {"d": down, "g": gate, "u": up, "o": out, "q": qkv, "n": gain}

    def advance(names):
        for name in names:
            named[name].step()

    turned_rows = normed[...].T
    advance("on")
    produce(down, down_part, lambda s: hidden[s][...].T, lambda s: ffn_out[...])
    advance(BACKWARD_PLAN[0])
    produce(gate, gate_part, lambda s: turned_rows, lambda s: d_gates[s][...])
    advance(BACKWARD_PLAN[1])
    produce(up, up_part, lambda s: turned_rows, lambda s: d_ups[s][...])
    d2[mine, :] = d_ref[:, :width]
    key_at = lax.broadcasted_iota(jnp.int32, (SLOT_LEN, QB), 0)
    bias[...] = jnp.where(key_at < length, 0.0, -1e30)
    advance(BACKWARD_PLAN[2])
    plan = [[named[name] for name in names] for names in BACKWARD_PLAN[3:15]]
    plan = [[job.steps.pop(0) for job in jobs] for jobs in plan]

    def pair_step(p, carry):
        lanes = pl.ds(pl.multiple_of(p * 128, 128), 128)
        for i in range(3):

            @pl.when(p == i)
            def _(i=i):
                swaps[i].wait_recv()

        k_pair, v_pair = k_ref[:, lanes], v_ref[:, lanes]
        k_turn = k_pair.T
        keys = [k_pair * head_mask(h) for h in range(2)]
        values = [v_pair * head_mask(h) for h in range(2)]
        for turn, qb in enumerate(reversed(range(SLOT_LEN // QB))):
            at = pl.ds(qb * QB, QB)
            span = (qb + 1) * QB
            query = q_ref[at, lanes]
            query_at = qb * QB + lax.broadcasted_iota(jnp.int32, (QB, 128), 0)
            present = jnp.where(query_at < length, 1.0, 0.0).astype(BF16)
            grad = d2[at, lanes] * present
            d_scores, probs_low, d_query = [], [], []
            for h in range(2):
                scores = dot_nt(keys[h][:span], query) + bias[:span, :]
                causal = lax.broadcasted_iota(jnp.int32, (QB, QB), 0) <= (
                    lax.broadcasted_iota(jnp.int32, (QB, QB), 1)
                )
                diag = jnp.where(causal, scores[span - QB :], -1e30)
                if qb:
                    scores = jnp.concatenate([scores[: span - QB], diag], axis=0)
                else:
                    scores = diag
                probs = jnp.exp(scores - stat[pl.ds(2 * p + h, 1), at])
                d_probs = dot_nt(values[h][:span], grad)
                total = jnp.sum(d_probs * probs, axis=0, keepdims=True)
                d_score = (probs * (d_probs - total)).astype(BF16)
                d_query.append(dot_nn(k_turn[h * HS : (h + 1) * HS, :span], d_score))
                d_scores.append(d_score)
                probs_low.append(probs.astype(BF16))
            d_key = dot_nn(
                jnp.concatenate(d_scores, axis=1),
                jnp.concatenate([query * head_mask(h) for h in range(2)], axis=0),
            )
            d_value = dot_nn(
                jnp.concatenate(probs_low, axis=1),
                jnp.concatenate([grad * head_mask(h) for h in range(2)], axis=0),
            )
            if turn == 0:
                dk_acc[...] = d_key
                dv_acc[...] = d_value
            else:
                dk_acc[:span, :] = dk_acc[:span, :] + d_key
                dv_acc[:span, :] = dv_acc[:span, :] + d_value
            part = jnp.concatenate(d_query, axis=0).T * 0.125
            part = part * cos_ref[at, :] - turned(part) * sin_ref[at, :]
            d_raw[at, lanes] = part.astype(BF16)
            for i in range(3):
                steps = plan[4 * i + turn]
                if steps:

                    @pl.when(p == i)
                    def _(steps=steps):
                        for step in steps:
                            step()

        part = dk_acc[...]
        part = part * cos_ref[...] - turned(part) * sin_ref[...]
        d_raw[:, pl.ds(pl.multiple_of(width + p * 128, 128), 128)] = part.astype(BF16)
        d_raw[:, pl.ds(pl.multiple_of(2 * width + p * 128, 128), 128)] = dv_acc[...].astype(BF16)
        return carry

    lax.fori_loop(0, 3, pair_step, 0)

    def qkv_step(t, carry):
        at = pl.ds(pl.multiple_of(t * width, 128), width)
        grads = dot_nn(d_raw[:, at].T, x2[...]).astype(BF16)
        qkv_part[:, :, :, :, pl.ds(pl.multiple_of(t * dim, 128), dim)] = grads.reshape(
            qkv_part.shape[:4] + (dim,)
        )
        return carry

    lax.fori_loop(0, 3, qkv_step, 0)
    weights = [w2[:, :, t * dim : (t + 1) * dim].reshape(width, dim) for t in range(3)]

    def project(at):
        return sum(
            dot_nn(d_raw[at, t * width : (t + 1) * width], weights[t]) for t in range(3)
        )

    advance(BACKWARD_PLAN[15])
    in_send[...] = project(theirs).astype(BF16)
    advance(BACKWARD_PLAN[16])
    own = resid[...] + project(mine)
    advance(BACKWARD_PLAN[17])
    swap_in.start()
    while any(job.steps for job in named.values()):
        advance("ougdqn")
    swap_in.wait_recv()
    in_grad[...] = (own + in_recv[...].astype(F32)).astype(BF16)
    links.drain()


def backward(
    length, d_all, slot_in, qkv_all, queries, keys, values, stats, cosines, sines, d_resid, gains,
    out_part, normed, ffn_out, hidden, d_gates, d_ups,
):
    rows, dim = d_resid.shape
    width = queries.shape[1]
    units = hidden[0].shape[1]
    shape = jax.ShapeDtypeStruct
    shards = [(4, 2, 2, units // 4, dim)] + [(4, 2, 2, dim // 4, units)] * 2 + [out_part.shape]
    shards.append((2, 2, 2, width // 8, qkv_all.shape[2]))
    scratch = []
    copies = 4 + 6
    for n, _, _, height, cols in shards:
        half, cut = cols // 2, cut_of(4 * height)
        copies += 2 * n + 3 + 9
        scratch += [
            pltpu.VMEM((n, 2, 2, height, half), BF16),
            pltpu.VMEM((n, 2, cut, half), BF16),
            pltpu.VMEM((n, 2, height - cut, half), BF16),
            pltpu.VMEM((n, height - cut, half), BF16),
            pltpu.VMEM((n, cut, half), BF16),
            pltpu.VMEM((n - 1, height, half), BF16),
        ]
    vmem = pl.BlockSpec(memory_space=pltpu.VMEM)
    return pl.pallas_call(
        backward_kernel,
        out_shape=[shape((rows, dim), BF16)]
        + [shape((4 * s[3], s[4]), BF16) for s in shards]
        + [shape(gains.shape, F32)],
        in_specs=[pl.BlockSpec(memory_space=pltpu.SMEM)] + [vmem] * 26,
        out_specs=[vmem] * 7,
        scratch_shapes=[
            pltpu.SemaphoreType.DMA((copies,)),
            pltpu.SemaphoreType.DMA((copies,)),
            pltpu.VMEM((SLOT_LEN, width), BF16),
            pltpu.VMEM((SLOT_LEN, QB), F32),
            pltpu.VMEM((SLOT_LEN, 3 * width), BF16),
            pltpu.VMEM((SLOT_LEN, 128), F32),
            pltpu.VMEM((SLOT_LEN, 128), F32),
            pltpu.VMEM(shards[4], BF16),
            pltpu.VMEM((rows, dim), BF16),
            pltpu.VMEM((rows, dim), BF16),
            pltpu.VMEM(shards[0], BF16),
            pltpu.VMEM(shards[1], BF16),
            pltpu.VMEM(shards[2], BF16),
            pltpu.VMEM(gains.shape, F32),
            pltpu.VMEM(gains.shape, F32),
            pltpu.VMEM(gains.shape, F32),
            pltpu.VMEM((3,) + gains.shape, F32),
            pltpu.VMEM((4,) + gains.shape, F32),
        ]
        + scratch,
        compiler_params=pltpu.CompilerParams(
            collective_id=1, has_side_effects=True, vmem_limit_bytes=VMEM_LIMIT
        ),
        name="attention_backward",
    )(
        length, d_all, slot_in, qkv_all, queries, keys, values, stats, cosines, sines, d_resid,
        gains, out_part, normed, ffn_out, *hidden, *d_gates, *d_ups,
    )


ALL = (0, 2, 1, 3)


def body(
    dp_size,
    layer_in,
    query_proj,
    key_proj,
    value_proj,
    out_proj,
    gate_proj,
    up_proj,
    down_proj,
    first_gain,
    second_gain,
    seq_lengths,
    cotangent,
):
    z = lax.axis_index("mp")
    valid_len = lax.dynamic_index_in_dim(seq_lengths, lax.div(z, 2), keepdims=False)
    width = query_proj.shape[1]

    qkv_own = jnp.concatenate([query_proj.T, key_proj.T, value_proj.T], axis=1)
    cosines, sines = rotary_tables(SLOT_LEN)
    cos_wide = jnp.tile(cosines[:, 0, :], (1, 4))
    sin_wide = jnp.tile(jnp.concatenate([-sines[:, 0, :], sines[:, 0, :]], axis=1), (1, 2))
    (
        slot_in, qkv_all, out_all, rot_queries, rot_keys, values_low, mixed_all, stats,
        resid_one, gate_far, up_far, down_far,
    ) = attention(
        valid_len[None], layer_in, qkv_own, out_proj, cos_wide, sin_wide,
        gate_proj, up_proj, down_proj,
    )
    out_all = out_all.reshape(4 * width, -1)
    normed, first_pull = jax.vjp(rms_norm, resid_one, first_gain)
    normed_low = normed.astype(BF16)

    gates = [gate_proj] + [gate_far[i] for i in range(3)]
    ups = [up_proj] + [up_far[i] for i in range(3)]
    downs = [down_proj] + [down_far[i] for i in range(3)]
    gate_pre = [forward(normed_low, w) for w in gates]
    up_pre = [forward(normed_low, w) for w in ups]
    hidden = [swiglu(g, u).astype(BF16) for g, u in zip(gate_pre, up_pre)]
    ffn_branch = sum(forward(h, w) for h, w in zip(hidden, downs))
    resid_two = normed + ffn_branch
    result, second_pull = jax.vjp(rms_norm, resid_two, second_gain)
    layer_out = result.astype(BF16)
    d_resid_two, second_part = second_pull(cotangent.astype(F32))
    ffn_out = d_resid_two.astype(BF16)
    d_normed = d_resid_two
    d_gates, d_ups = [], []
    for r in range(4):
        d_hidden = against(ffn_out, downs[r])
        unused, glu_pull = jax.vjp(swiglu, gate_pre[r], up_pre[r])
        d_gate, d_up = (d.astype(BF16) for d in glu_pull(d_hidden))
        d_gates.append(d_gate)
        d_ups.append(d_up)
        d_normed = d_normed + against(d_gate, gates[r]) + against(d_up, ups[r])
    d_resid_one, first_part = first_pull(d_normed)
    attn_out = d_resid_one.astype(BF16)
    out_part = cross(mixed_all, attn_out).astype(BF16).reshape(4, 2, 2, width // 4, -1)
    d_all = against(attn_out, out_all).astype(BF16)
    gains = jnp.concatenate(
        [first_part[None], second_part[None], jnp.zeros((6, first_part.shape[0]), F32)], axis=0
    )
    input_grad, down_grad, gate_grad, up_grad, out_grad, qkv_grad, gains = backward(
        valid_len[None], d_all, slot_in, qkv_all, rot_queries, rot_keys, values_low, stats,
        cos_wide, sin_wide, d_resid_one, gains, out_part, normed_low, ffn_out, hidden, d_gates,
        d_ups,
    )
    dim = layer_in.shape[1]
    down_grad, gate_grad, up_grad, out_grad, qkv_grad = (
        g.astype(F32) for g in (down_grad, gate_grad, up_grad, out_grad, qkv_grad)
    )
    if dp_size > BLOCK:
        groups = [list(range(i, dp_size, BLOCK)) for i in range(BLOCK)]
        down_grad, gate_grad, up_grad, out_grad, qkv_grad, gains = lax.psum(
            (down_grad, gate_grad, up_grad, out_grad, qkv_grad, gains),
            "dp",
            axis_index_groups=groups,
        )
    qkv_grad = [qkv_grad[:, t * dim : (t + 1) * dim] for t in range(3)]
    return (
        layer_out,
        input_grad,
        qkv_grad[0].T,
        qkv_grad[1].T,
        qkv_grad[2].T,
        out_grad,
        gate_grad,
        up_grad,
        down_grad,
        gains[0],
        gains[1],
    )


def solution(mesh):
    rows = P(("dp", "mp"), None)
    cols, first = P(None, "mp"), P("mp", None)
    return jax.shard_map(
        functools.partial(body, mesh.shape["dp"]),
        mesh=mesh,
        in_specs=(rows, cols, cols, cols, first, cols, cols, first, P(), P(), P("dp"), rows),
        out_specs=(rows, rows, cols, cols, cols, first, cols, cols, first, P(), P()),
        check_vma=False,
    )
```
